32 devices in a mesh: seq: 8 (over z, y), head: 4 (over x, core).
Axes of the slice: x: 2, y: 2, z: 4, core: 2. Of those that a mesh axis runs over, the one named last changes fastest.
Arguments:
- queries: bfloat16 [2048, 4096], P('seq', 'head'), may hold values from -80 to 80, as said below
- keys_in: bfloat16 [2048, 4096], P('seq', 'head'), may hold values from -4 to 4
- values_in: bfloat16 [2048, 4096], P('seq', 'head'), may hold values from -6 to 6
- out_weight: bfloat16 [4096, 4096], P('head'), may hold values from -0.09375 to 0.09375
- spans: int32 [32], P('head'), may hold values from 1024 to 4096
- full_ids: int32 [8], P('head'), may hold values from 0 to 31, as said below
Outputs:
- mixed: bfloat16 [2048, 4096], P('seq', 'head')
The draws below stay inside these ranges and needn't reach their ends.
Inputs may be any that keep to these rules, and one draw needn't show every extreme that they name: `queries`: unlike a plain normal draw, some rows may be far larger than the rest. `full_ids`: increasing and distinct; entries g * 2 to (g + 1) * 2 - 1 name heads of group g, that is heads g * 8 to (g + 1) * 8 - 1.
All inputs are finite; a program needn't handle non-finite values.
Results may differ from the reference program's by a relative error of at most 0.012.
Values may be sent and summed in bfloat16 or wider, within the bound.
No kernel may reach another device: no remote copies, remote signals or barrier semaphores. Data moves between devices by JAX's collectives and lax.ppermute only.
A program may use at most 128 MiB of HBM per device.

```python
import math
import jax
import jax.numpy as jnp
from jax import lax

HEADS = 32
FULL = 8
HEAD_DIM = 128
MODEL = 4096
SPAN_MAX = 4096
SPAN_MIN = 1024
SEQ = 2048
GROUP = 8
FULL_DEV = 2
N_HEAD = 4


def paired_draw(key):
    base_q = jnp.clip(jax.random.normal(jax.random.fold_in(key, 101), (SEQ, HEADS * HEAD_DIM), jnp.float32), -4.0, 4.0)
    base_k = jnp.clip(jax.random.normal(jax.random.fold_in(key, 202), (SEQ, HEADS * HEAD_DIM), jnp.float32), -4.0, 4.0)
    return (base_q, base_k)


def draw_queries(key, part):
    return paired_draw(key)[0].astype(jnp.bfloat16)


def draw_keys_in(key, part):
    return paired_draw(key)[1].astype(jnp.bfloat16)


def draw_full_ids(key, part):
    group_keys = jax.random.split(key, HEADS // GROUP)

    def pick_group(group_key):
        return jnp.sort(jax.random.permutation(group_key, GROUP)[:FULL_DEV])
    chosen = jax.vmap(pick_group)(group_keys)
    offsets = (jnp.arange(HEADS // GROUP) * GROUP)[:, None]
    return (chosen + offsets).reshape(FULL).astype(jnp.int32)


def touch_ends(values, rng, low, largest):
    dims = values.shape
    index_at = [jax.random.randint(jax.random.fold_in(rng, axis), (), 0, dims[axis]) for axis in range(len(dims))]
    values = values.at[tuple(index_at)].set(low)
    longest = dims.index(max(dims))
    index_at[longest] = (index_at[longest] + 1) % dims[longest]
    return values.at[tuple(index_at)].set(largest)


def shard_levels(rng, dims, pieces, smallest, largest):
    gain, own = 1.0, jax.random.fold_in(rng, 6)
    for axis_at, parts in pieces:
        steps = jnp.exp(jax.random.uniform(jax.random.fold_in(own, axis_at), (parts,), jnp.float32, smallest / len(pieces), largest / len(pieces)))
        gain = gain * jnp.repeat(steps, dims[axis_at] // parts).reshape([-1 if axis == axis_at else 1 for axis in range(len(dims))])
    return gain


def noise(stream_key, shape, spread, bound, cuts=(), kind=jnp.bfloat16):
    factor_of = shard_levels(stream_key, shape, cuts, -0.22, 0.18) if cuts else 1.0
    entries = jax.random.normal(stream_key, shape, jnp.float32) * spread * factor_of
    return jnp.minimum(jnp.maximum(entries, -bound), bound).astype(kind)


def setup_inputs(seed: int = 0) -> dict:
    key_list = jax.random.split(jax.random.key(seed), 7)
    return {
        "queries": draw_queries(jax.random.fold_in(key_list[6], 71), 0),
        "keys_in": draw_keys_in(jax.random.fold_in(key_list[6], 71), 0),
        "values_in": noise(key_list[2], (SEQ, HEADS * HEAD_DIM), 1.0, 6.0, ((0, 8), (1, 4))),
        "out_weight": noise(key_list[3], (HEADS * HEAD_DIM, MODEL), (HEADS * HEAD_DIM) ** -0.5, 0.09375, ((0, 4),)),
        "spans": touch_ends(jax.random.randint(key_list[4], (HEADS,), SPAN_MIN, SPAN_MAX + 1), jax.random.fold_in(key_list[4], 1), SPAN_MIN, SPAN_MAX).astype(jnp.int32),
        "full_ids": draw_full_ids(jax.random.fold_in(key_list[6], 71), 0),
    }


NEG_FILL = -1e30


def weigh(scores, allowed, value_rows):
    masked = jnp.where(allowed, scores, NEG_FILL)
    row_top = jnp.max(masked, axis=-1, keepdims=True)
    weights = jnp.where(allowed, jnp.exp(masked - row_top), 0.0)
    row_total = jnp.sum(weights, axis=-1, keepdims=True)
    rounded = lax.optimization_barrier(weights.astype(jnp.bfloat16)).astype(jnp.float32)
    numerator = jnp.dot(rounded, value_rows.astype(jnp.float32), precision=lax.Precision.HIGHEST)
    return numerator / row_total


def reference(queries, keys_in, values_in, out_weight, spans, full_ids):
    score_scale = HEAD_DIM ** -0.5
    block_rows = math.gcd(512, SEQ)
    block_starts = jnp.arange(SEQ // block_rows, dtype=jnp.int32) * block_rows
    positions = jnp.arange(SEQ, dtype=jnp.int32)
    head_range = jnp.arange(HEADS, dtype=jnp.int32)
    is_full = jnp.any(head_range[:, None] == full_ids[None, :], axis=1).astype(jnp.int32)
    ordering = jnp.argsort(is_full * HEADS + head_range).astype(jnp.int32)
    band_ids = ordering[: HEADS - FULL]
    full_list = ordering[HEADS - FULL:]

    def head_columns(array, head_id):
        return lax.dynamic_slice_in_dim(array, (head_id * HEAD_DIM).astype(jnp.int32), HEAD_DIM, 1)

    def banded_head(packed):
        head_id, reach = packed
        q_head = head_columns(queries, head_id).astype(jnp.float32)
        k_pad = jnp.pad(head_columns(keys_in, head_id).astype(jnp.float32), ((SPAN_MAX, 0), (0, 0)))
        v_pad = jnp.pad(head_columns(values_in, head_id).astype(jnp.float32), ((SPAN_MAX, 0), (0, 0)))

        def one_block(begin_row):
            q_rows = lax.dynamic_slice_in_dim(q_head, begin_row, block_rows, 0)
            k_rows = lax.dynamic_slice_in_dim(k_pad, begin_row, SPAN_MAX + block_rows, 0)
            v_rows = lax.dynamic_slice_in_dim(v_pad, begin_row, SPAN_MAX + block_rows, 0)
            scores = jnp.dot(q_rows, k_rows.T, precision=lax.Precision.HIGHEST) * score_scale
            q_pos = begin_row + jnp.arange(block_rows, dtype=jnp.int32)
            k_pos = begin_row - SPAN_MAX + jnp.arange(SPAN_MAX + block_rows, dtype=jnp.int32)
            gap_size = q_pos[:, None] - k_pos[None, :]
            allowed = (gap_size >= 0) & (gap_size < reach) & (k_pos >= 0)[None, :]
            return weigh(scores, allowed, v_rows)

        return lax.map(one_block, block_starts).reshape(SEQ, HEAD_DIM)

    def full_head(head_id):
        q_head = head_columns(queries, head_id).astype(jnp.float32)
        k_head = head_columns(keys_in, head_id).astype(jnp.float32)
        v_head = head_columns(values_in, head_id)

        def one_block(begin_row):
            q_rows = lax.dynamic_slice_in_dim(q_head, begin_row, block_rows, 0)
            scores = jnp.dot(q_rows, k_head.T, precision=lax.Precision.HIGHEST) * score_scale
            q_pos = begin_row + jnp.arange(block_rows, dtype=jnp.int32)
            allowed = positions[None, :] <= q_pos[:, None]
            return weigh(scores, allowed, v_head)

        return lax.map(one_block, block_starts).reshape(SEQ, HEAD_DIM)

    band_out = lax.map(banded_head, (band_ids, spans[band_ids]))
    full_out = lax.map(full_head, full_list)
    stacked = jnp.concatenate([band_out, full_out], axis=0).astype(jnp.bfloat16)
    inverse = jnp.argsort(ordering).astype(jnp.int32)
    per_head = jnp.take(stacked, inverse, axis=0)
    attended = per_head.transpose(1, 0, 2).reshape(SEQ, HEADS * HEAD_DIM)
    group_rows = HEADS * HEAD_DIM // N_HEAD
    summed = jnp.zeros((SEQ, MODEL), jnp.float32)
    for group_index in range(N_HEAD):
        lower = group_index * group_rows
        partial_value = jnp.dot(attended[:, lower:lower + group_rows], out_weight[lower:lower + group_rows], preferred_element_type=jnp.float32)
        summed = summed + lax.optimization_barrier(partial_value.astype(jnp.bfloat16)).astype(jnp.float32)
    return summed.astype(jnp.bfloat16)
```

```python
import math

import functools

import jax
import jax.numpy as jnp
from jax import lax
from jax.experimental import pallas as pl
from jax.experimental.pallas import tpu as pltpu
from jax.sharding import PartitionSpec as P

HEAD_DIM = 128
SPAN_MAX = 4096
SPAN_MIN = 1024
CHUNKS = 2


NEG_FILL = -1e30


def from_behind(block, axis, distance):
    devices = range(lax.axis_size(axis))
    route = [(i - distance, i) for i in devices if i - distance in devices]
    return lax.ppermute(block, axis, route)


def online_update(carry_state, scores, allowed, value_rows):
    old_peak, row_total, numerator = carry_state
    masked = jnp.where(allowed, scores, NEG_FILL)
    new_peak = jnp.maximum(old_peak, jnp.max(masked, axis=-1))
    weights = jnp.where(allowed, jnp.exp(masked - new_peak[..., None]), 0.0)
    rescale = jnp.exp(old_peak - new_peak)
    row_total = row_total * rescale + jnp.sum(weights, axis=-1)
    numerator = numerator * rescale[..., None] + jnp.einsum(
        "hqk,hkd->hqd", weights.astype(jnp.bfloat16), value_rows, preferred_element_type=jnp.float32
    )
    return (new_peak, row_total, numerator)


def empty_state(lead_count, row_count, head_width):
    return (
        jnp.full((lead_count, row_count), NEG_FILL, jnp.float32),
        jnp.zeros((lead_count, row_count), jnp.float32),
        jnp.zeros((lead_count, row_count, head_width), jnp.float32),
    )


def finish(carry_state):
    return (carry_state[2] / carry_state[1][..., None]).astype(jnp.bfloat16)


def ring_path(queries, keys_in, values_in, out_weight, spans, full_ids):
    score_scale = HEAD_DIM ** (-0.5)
    n_seq = lax.axis_size("seq")
    seq_index = lax.axis_index("seq")
    tok_rows = queries.shape[0]
    group_heads = queries.shape[1] // HEAD_DIM
    full_count = full_ids.shape[0]
    band_count = group_heads - full_count
    head_base = lax.axis_index("head") * group_heads
    local_range = jnp.arange(group_heads)
    marks = jnp.sum(
        (local_range[:, None] + head_base == full_ids[None, :]).astype(jnp.int32), axis=1
    )
    order_local = jnp.argsort(marks * group_heads + local_range)
    band_local = order_local[:band_count]
    full_local = order_local[band_count:]
    query_three = queries.reshape(tok_rows, group_heads, HEAD_DIM)
    key_three = keys_in.reshape(tok_rows, group_heads, HEAD_DIM)
    value_three = values_in.reshape(tok_rows, group_heads, HEAD_DIM)
    query_band = jnp.take(query_three, band_local, axis=1).transpose(1, 0, 2)
    kv_band = jnp.stack(
        [
            jnp.take(key_three, band_local, axis=1).transpose(1, 0, 2),
            jnp.take(value_three, band_local, axis=1).transpose(1, 0, 2),
        ]
    )
    band_reach = jnp.take(spans, band_local)
    query_pos = seq_index * tok_rows + jnp.arange(tok_rows)
    hop_count = min(max(1, SPAN_MAX // tok_rows), n_seq - 1)
    arrived = [(kv_band, 0)]
    moving = kv_band
    for distance in range(1, hop_count + 1):
        moving = from_behind(moving, "seq", 1)
        arrived.append((moving, distance))
    batch_size = max(1, 512 // tok_rows)
    band_state = empty_state(band_count, tok_rows, HEAD_DIM)
    for first_piece in range(0, len(arrived), batch_size):
        batch_pieces = arrived[first_piece : first_piece + batch_size]
        key_rows = jnp.concatenate([arrival[0][0] for arrival in batch_pieces], axis=1)
        value_rows = jnp.concatenate([arrival[0][1] for arrival in batch_pieces], axis=1)
        key_pos = jnp.concatenate(
            [(seq_index - arrival[1]) * tok_rows + jnp.arange(tok_rows) for arrival in batch_pieces]
        )
        scores = (
            jnp.einsum("hqd,hkd->hqk", query_band, key_rows, preferred_element_type=jnp.float32)
            * score_scale
        )
        gap_size = query_pos[None, :, None] - key_pos[None, None, :]
        allowed = (
            (gap_size >= 0) & (gap_size < band_reach[:, None, None]) & (key_pos >= 0)[None, None, :]
        )
        band_state = online_update(band_state, scores, allowed, value_rows)
    band_out = finish(band_state)
    query_full = jnp.take(query_three, full_local, axis=1).transpose(1, 0, 2)
    key_full = jnp.take(key_three, full_local, axis=1).transpose(1, 0, 2)
    value_full = jnp.take(value_three, full_local, axis=1).transpose(1, 0, 2)
    kv_full = jnp.stack([key_full, value_full])
    last_query = seq_index * tok_rows + tok_rows - 1
    key_piece = lax.all_gather(kv_full, "seq", axis=2, tiled=True)
    row_count = key_piece.shape[2]
    tile_rows = math.gcd(row_count, 512)

    def absorb_tile(tile_index, inner_state):
        key_tile = lax.dynamic_slice_in_dim(key_piece[0], tile_index * tile_rows, tile_rows, 1)
        value_tile = lax.dynamic_slice_in_dim(key_piece[1], tile_index * tile_rows, tile_rows, 1)
        key_pos = tile_index * tile_rows + jnp.arange(tile_rows)
        scores = (
            jnp.einsum("hqd,hkd->hqk", query_full, key_tile, preferred_element_type=jnp.float32)
            * score_scale
        )
        allowed = key_pos[None, None, :] <= query_pos[None, :, None]
        return online_update(inner_state, scores, allowed, value_tile)

    live_tiles = jnp.clip(last_query // tile_rows + 1, 0, row_count // tile_rows)
    full_state = lax.fori_loop(
        0, live_tiles, absorb_tile, empty_state(full_count, tok_rows, HEAD_DIM)
    )
    full_out = finish(full_state)
    combined = jnp.concatenate([band_out, full_out], axis=0)
    inverse = jnp.argsort(order_local)
    per_head = jnp.take(combined, inverse, axis=0)
    attended = per_head.transpose(1, 0, 2).reshape(tok_rows, group_heads * HEAD_DIM)
    projected = jnp.dot(attended, out_weight, preferred_element_type=jnp.float32)
    return lax.psum_scatter(projected.astype(jnp.bfloat16), "head", scatter_dimension=1, tiled=True)


def swap(block, axis, flip):
    devices = range(lax.axis_size(axis))
    return lax.ppermute(block, axis, [(i, i ^ flip) for i in devices])


def in_vmem(count):
    return [pl.BlockSpec(memory_space=pltpu.VMEM)] * count


def deal_heads(n_seq, seq_ref, q_ref, k_ref, v_ref, *out_refs):
    rows = q_ref.shape[0]
    for flip in range(n_seq):
        at = pl.multiple_of((seq_ref[0] ^ flip) * HEAD_DIM, HEAD_DIM)
        out_refs[flip][:rows] = q_ref[:, pl.ds(at, HEAD_DIM)]
        out_refs[flip][rows:] = k_ref[:, pl.ds(at, HEAD_DIM)]
        out_refs[n_seq + flip][...] = v_ref[:, pl.ds(at, HEAD_DIM)]


def attend(n_seq, chunk, meta_ref, *refs):
    qk_refs, v_refs = refs[:n_seq], refs[n_seq : 2 * n_seq]
    out_refs = refs[2 * n_seq : 3 * n_seq]
    q_all, k_all, v_all, o_all = refs[3 * n_seq :]
    me, reach = meta_ref[0], meta_ref[1]
    block = v_refs[0].shape[0]
    part = block // CHUNKS
    first = chunk * part
    factor = HEAD_DIM**-0.5 * math.log2(math.e)
    for flip in range(n_seq):
        source = me ^ flip
        q_all[pl.ds(pl.multiple_of(source * part, part), part)] = qk_refs[flip][
            first : first + part
        ]
        at = pl.multiple_of(source * block, block)
        k_all[pl.ds(at, block)] = qk_refs[flip][block:]
        v_all[pl.ds(at, block)] = v_refs[flip][...]
    tile = block
    span = tile // part
    row = lax.broadcasted_iota(jnp.int32, (tile, block), 0)
    column = lax.broadcasted_iota(jnp.int32, (tile, block), 1)
    gap_base = row // part * block + row % part + first - column
    for base in range(0, n_seq, span):
        q_tile = q_all[base * part : base * part + tile]
        last = base + span - 1
        pieces = []
        for j in range(last + 1):
            k_tile = k_all[j * block : (j + 1) * block]
            scores = lax.dot_general(
                q_tile, k_tile, (((1,), (1,)), ((), ())), preferred_element_type=jnp.float32
            )
            offset = (base - j) * block
            furthest = (last - j) * block + block - 1
            allowed = None
            if j >= base:
                allowed = gap_base >= -offset
            if furthest >= SPAN_MIN:
                near = gap_base < reach - offset
                allowed = near if allowed is None else allowed & near
            if allowed is not None:
                scores = jnp.where(allowed, scores, NEG_FILL)
            pieces.append(scores)
        peak = functools.reduce(jnp.maximum, pieces)
        peak = jnp.max(peak, axis=1, keepdims=True)
        total = jnp.zeros((tile, block), jnp.float32)
        numerator = jnp.zeros((tile, HEAD_DIM), jnp.float32)
        for j in range(last + 1):
            weights = jnp.exp2((pieces[j] - peak) * factor)
            total = total + weights
            numerator = numerator + jnp.dot(
                weights.astype(jnp.bfloat16),
                v_all[j * block : (j + 1) * block],
                preferred_element_type=jnp.float32,
            )
        row_total = jnp.sum(total, axis=1, keepdims=True)
        o_all[base * part : base * part + tile] = (numerator / row_total).astype(jnp.bfloat16)
    for flip in range(n_seq):
        at = pl.multiple_of((me ^ flip) * part, part)
        out_refs[flip][...] = o_all[pl.ds(at, part)]


def project(n_seq, wanted, meta_ref, *refs):
    o_refs, w_ref = refs[:n_seq], refs[n_seq]
    far_ref, near_ref, joined = refs[n_seq + 1 :]
    me, head = meta_ref[0], meta_ref[2]
    for flip in range(n_seq):
        at = pl.multiple_of((me ^ flip) * HEAD_DIM, HEAD_DIM)
        joined[:, pl.ds(at, HEAD_DIM)] = o_refs[flip][...]
    width = far_ref.shape[1]
    for out_ref, flip in ((far_ref, wanted ^ 2), (near_ref, wanted)):
        at = pl.multiple_of((head ^ flip) * width, width)
        out_ref[...] = jnp.dot(
            joined[...], w_ref[:, pl.ds(at, width)], preferred_element_type=jnp.float32
        ).astype(jnp.bfloat16)


def headwise_path(queries, keys_in, values_in, out_weight, spans, full_ids):
    n_seq = lax.axis_size("seq")
    me = lax.axis_index("seq")
    head = lax.axis_index("head")
    block = queries.shape[0]
    part = block // CHUNKS
    tokens = block * n_seq
    is_full = jnp.any(full_ids == head * n_seq + me)
    reach = jnp.where(is_full, tokens, jnp.sum(jnp.where(jnp.arange(n_seq) == me, spans, 0)))
    meta = jnp.stack([me, reach, head]).astype(jnp.int32)
    smem = pl.BlockSpec(memory_space=pltpu.SMEM)
    bf16 = jnp.bfloat16

    dealt = pl.pallas_call(
        functools.partial(deal_heads, n_seq),
        out_shape=[jax.ShapeDtypeStruct((2 * block, HEAD_DIM), bf16)] * n_seq
        + [jax.ShapeDtypeStruct((block, HEAD_DIM), bf16)] * n_seq,
        in_specs=[smem] + in_vmem(3),
        out_specs=in_vmem(2 * n_seq),
        cost_estimate=pl.CostEstimate(flops=10**8, bytes_accessed=12 * block * n_seq * HEAD_DIM, transcendentals=0),
    )(meta, queries, keys_in, values_in)
    flips = sorted(range(1, n_seq), key=lambda flip: -flip)
    qk = {0: dealt[0]}
    v = {0: dealt[n_seq]}
    for flip in flips:
        qk[flip] = swap(dealt[flip], "seq", flip)
    for flip in flips:
        v[flip] = swap(dealt[n_seq + flip], "seq", flip)
    qk = [qk[flip] for flip in range(n_seq)]
    v = [v[flip] for flip in range(n_seq)]

    width = out_weight.shape[1] // lax.axis_size("head")
    mixed = []
    for chunk in range(CHUNKS):
        sent = pl.pallas_call(
            functools.partial(attend, n_seq, chunk),
            out_shape=[jax.ShapeDtypeStruct((part, HEAD_DIM), bf16)] * n_seq,
            in_specs=[smem] + in_vmem(2 * n_seq),
            out_specs=in_vmem(n_seq),
            scratch_shapes=[
                pltpu.VMEM((tokens // CHUNKS, HEAD_DIM), bf16),
                pltpu.VMEM((tokens, HEAD_DIM), bf16),
                pltpu.VMEM((tokens, HEAD_DIM), bf16),
                pltpu.VMEM((tokens // CHUNKS, HEAD_DIM), bf16),
            ],
            cost_estimate=pl.CostEstimate(
                flops=2 * tokens * tokens * HEAD_DIM // CHUNKS,
                bytes_accessed=8 * tokens * HEAD_DIM,
                transcendentals=tokens * tokens // 2 // CHUNKS,
            ),
        )(meta, *qk, *v)
        came = {0: sent[0]}
        for flip in flips:
            came[flip] = swap(sent[flip], "seq", flip)
        came = [came[flip] for flip in range(n_seq)]
        halves = []
        for wanted in (1, 0):
            halves.append(
                pl.pallas_call(
                    functools.partial(project, n_seq, wanted),
                    out_shape=[jax.ShapeDtypeStruct((part, width), bf16)] * 2,
                    in_specs=[smem] + in_vmem(n_seq + 1),
                    out_specs=in_vmem(2),
                    scratch_shapes=[pltpu.VMEM((part, n_seq * HEAD_DIM), bf16)],
                    cost_estimate=pl.CostEstimate(
                        flops=4 * part * n_seq * HEAD_DIM * width,
                        bytes_accessed=4 * n_seq * HEAD_DIM * width,
                        transcendentals=0,
                    ),
                )(meta, *came, out_weight)
            )
        far = swap(halves[0][0], "head", 1)
        near = swap(halves[0][1], "head", 1)
        far = (far.astype(jnp.float32) + halves[1][0].astype(jnp.float32)).astype(bf16)
        far = swap(far, "head", 2)
        near = (near.astype(jnp.float32) + halves[1][1].astype(jnp.float32)).astype(bf16)
        mixed.append((near.astype(jnp.float32) + far.astype(jnp.float32)).astype(bf16))
    return jnp.concatenate(mixed, axis=0)


def on_device(queries, keys_in, values_in, out_weight, spans, full_ids):
    n_seq, n_head = lax.axis_size("seq"), lax.axis_size("head")
    one_head_each = queries.shape[1] == n_seq * HEAD_DIM
    if one_head_each and n_head == 4 and n_seq == 8 and queries.shape[0] % (16 * CHUNKS) == 0:
        return headwise_path(queries, keys_in, values_in, out_weight, spans, full_ids)
    return ring_path(queries, keys_in, values_in, out_weight, spans, full_ids)


def solution(mesh):
    placed = (
        P("seq", "head"),
        P("seq", "head"),
        P("seq", "head"),
        P("head", None),
        P("head"),
        P("head"),
    )
    return jax.shard_map(
        on_device, mesh=mesh, in_specs=placed, out_specs=P("seq", "head"), check_vma=False
    )
```

```python
import math

import functools

import jax
import jax.numpy as jnp
from jax import lax
from jax.experimental import pallas as pl
from jax.experimental.pallas import tpu as pltpu
from jax.sharding import PartitionSpec as P

HEAD_DIM = 128
SPAN_MAX = 4096
SPAN_MIN = 1024


NEG_FILL = -1e30


def from_behind(block, axis, distance):
    devices = range(lax.axis_size(axis))
    route = [(i - distance, i) for i in devices if i - distance in devices]
    return lax.ppermute(block, axis, route)


def online_update(carry_state, scores, allowed, value_rows):
    old_peak, row_total, numerator = carry_state
    masked = jnp.where(allowed, scores, NEG_FILL)
    new_peak = jnp.maximum(old_peak, jnp.max(masked, axis=-1))
    weights = jnp.where(allowed, jnp.exp(masked - new_peak[..., None]), 0.0)
    rescale = jnp.exp(old_peak - new_peak)
    row_total = row_total * rescale + jnp.sum(weights, axis=-1)
    numerator = numerator * rescale[..., None] + jnp.einsum(
        "hqk,hkd->hqd", weights.astype(jnp.bfloat16), value_rows, preferred_element_type=jnp.float32
    )
    return (new_peak, row_total, numerator)


def empty_state(lead_count, row_count, head_width):
    return (
        jnp.full((lead_count, row_count), NEG_FILL, jnp.float32),
        jnp.zeros((lead_count, row_count), jnp.float32),
        jnp.zeros((lead_count, row_count, head_width), jnp.float32),
    )


def finish(carry_state):
    return (carry_state[2] / carry_state[1][..., None]).astype(jnp.bfloat16)


def ring_path(queries, keys_in, values_in, out_weight, spans, full_ids):
    score_scale = HEAD_DIM ** (-0.5)
    n_seq = lax.axis_size("seq")
    seq_index = lax.axis_index("seq")
    tok_rows = queries.shape[0]
    group_heads = queries.shape[1] // HEAD_DIM
    full_count = full_ids.shape[0]
    band_count = group_heads - full_count
    head_base = lax.axis_index("head") * group_heads
    local_range = jnp.arange(group_heads)
    marks = jnp.sum(
        (local_range[:, None] + head_base == full_ids[None, :]).astype(jnp.int32), axis=1
    )
    order_local = jnp.argsort(marks * group_heads + local_range)
    band_local = order_local[:band_count]
    full_local = order_local[band_count:]
    query_three = queries.reshape(tok_rows, group_heads, HEAD_DIM)
    key_three = keys_in.reshape(tok_rows, group_heads, HEAD_DIM)
    value_three = values_in.reshape(tok_rows, group_heads, HEAD_DIM)
    query_band = jnp.take(query_three, band_local, axis=1).transpose(1, 0, 2)
    kv_band = jnp.stack(
        [
            jnp.take(key_three, band_local, axis=1).transpose(1, 0, 2),
            jnp.take(value_three, band_local, axis=1).transpose(1, 0, 2),
        ]
    )
    band_reach = jnp.take(spans, band_local)
    query_pos = seq_index * tok_rows + jnp.arange(tok_rows)
    hop_count = min(max(1, SPAN_MAX // tok_rows), n_seq - 1)
    arrived = [(kv_band, 0)]
    moving = kv_band
    for distance in range(1, hop_count + 1):
        moving = from_behind(moving, "seq", 1)
        arrived.append((moving, distance))
    batch_size = max(1, 512 // tok_rows)
    band_state = empty_state(band_count, tok_rows, HEAD_DIM)
    for first_piece in range(0, len(arrived), batch_size):
        batch_pieces = arrived[first_piece : first_piece + batch_size]
        key_rows = jnp.concatenate([arrival[0][0] for arrival in batch_pieces], axis=1)
        value_rows = jnp.concatenate([arrival[0][1] for arrival in batch_pieces], axis=1)
        key_pos = jnp.concatenate(
            [(seq_index - arrival[1]) * tok_rows + jnp.arange(tok_rows) for arrival in batch_pieces]
        )
        scores = (
            jnp.einsum("hqd,hkd->hqk", query_band, key_rows, preferred_element_type=jnp.float32)
            * score_scale
        )
        gap_size = query_pos[None, :, None] - key_pos[None, None, :]
        allowed = (
            (gap_size >= 0) & (gap_size < band_reach[:, None, None]) & (key_pos >= 0)[None, None, :]
        )
        band_state = online_update(band_state, scores, allowed, value_rows)
    band_out = finish(band_state)
    query_full = jnp.take(query_three, full_local, axis=1).transpose(1, 0, 2)
    key_full = jnp.take(key_three, full_local, axis=1).transpose(1, 0, 2)
    value_full = jnp.take(value_three, full_local, axis=1).transpose(1, 0, 2)
    kv_full = jnp.stack([key_full, value_full])
    last_query = seq_index * tok_rows + tok_rows - 1
    key_piece = lax.all_gather(kv_full, "seq", axis=2, tiled=True)
    row_count = key_piece.shape[2]
    tile_rows = math.gcd(row_count, 512)

    def absorb_tile(tile_index, inner_state):
        key_tile = lax.dynamic_slice_in_dim(key_piece[0], tile_index * tile_rows, tile_rows, 1)
        value_tile = lax.dynamic_slice_in_dim(key_piece[1], tile_index * tile_rows, tile_rows, 1)
        key_pos = tile_index * tile_rows + jnp.arange(tile_rows)
        scores = (
            jnp.einsum("hqd,hkd->hqk", query_full, key_tile, preferred_element_type=jnp.float32)
            * score_scale
        )
        allowed = key_pos[None, None, :] <= query_pos[None, :, None]
        return online_update(inner_state, scores, allowed, value_tile)

    live_tiles = jnp.clip(last_query // tile_rows + 1, 0, row_count // tile_rows)
    full_state = lax.fori_loop(
        0, live_tiles, absorb_tile, empty_state(full_count, tok_rows, HEAD_DIM)
    )
    full_out = finish(full_state)
    combined = jnp.concatenate([band_out, full_out], axis=0)
    inverse = jnp.argsort(order_local)
    per_head = jnp.take(combined, inverse, axis=0)
    attended = per_head.transpose(1, 0, 2).reshape(tok_rows, group_heads * HEAD_DIM)
    projected = jnp.dot(attended, out_weight, preferred_element_type=jnp.float32)
    return lax.psum_scatter(projected.astype(jnp.bfloat16), "head", scatter_dimension=1, tiled=True)


def swap(block, axis, flip):
    devices = range(lax.axis_size(axis))
    return lax.ppermute(block, axis, [(i, i ^ flip) for i in devices])


def in_vmem(count):
    return [pl.BlockSpec(memory_space=pltpu.VMEM)] * count


def held(array):
    return pltpu.with_memory_space_constraint(array, pltpu.VMEM)


SMEM = pl.BlockSpec(memory_space=pltpu.SMEM)


def own_kernel(body, out_shapes, in_specs, scratch=(), flops=10**8, limit=20 * 2**20):
    return pl.pallas_call(
        body,
        out_shape=out_shapes,
        in_specs=in_specs,
        out_specs=in_vmem(len(out_shapes)),
        scratch_shapes=list(scratch),
        compiler_params=pltpu.CompilerParams(vmem_limit_bytes=limit),
        cost_estimate=pl.CostEstimate(flops=flops, bytes_accessed=10**6, transcendentals=0),
    )


def deal_heads(n_seq, me_ref, *refs):
    in_refs, out_refs = refs[:-n_seq], refs[-n_seq:]
    rows = in_refs[0].shape[0]
    for flip in range(n_seq):
        at = pl.multiple_of((me_ref[0] ^ flip) * HEAD_DIM, HEAD_DIM)
        for place, in_ref in enumerate(in_refs):
            out_refs[flip][place * rows : (place + 1) * rows] = in_ref[:, pl.ds(at, HEAD_DIM)]


def weigh(n_seq, me_ref, spans_ref, full_ref, *refs):
    qk_refs, (weight_ref, total_ref, q_all, k_all) = refs[:n_seq], refs[n_seq:]
    me, head = me_ref[0], me_ref[1]
    block = q_all.shape[0] // n_seq
    reach = spans_ref[me]
    for place in range(full_ref.shape[0]):
        reach = jnp.where(full_ref[place] == head * n_seq + me, n_seq * block, reach)
    factor = HEAD_DIM**-0.5 * math.log2(math.e)
    for flip in range(n_seq):
        at = pl.multiple_of((me ^ flip) * block, block)
        q_all[pl.ds(at, block)] = qk_refs[flip][:block]
        k_all[pl.ds(at, block)] = qk_refs[flip][block:]
    row = lax.broadcasted_iota(jnp.int32, (block, block), 0)
    column = lax.broadcasted_iota(jnp.int32, (block, block), 1)
    gap_base = row - column
    for i in range(n_seq):
        q_tile = q_all[i * block : (i + 1) * block]
        pieces = []
        for j in range(i + 1):
            scores = lax.dot_general(
                q_tile,
                k_all[j * block : (j + 1) * block],
                (((1,), (1,)), ((), ())),
                preferred_element_type=jnp.float32,
            )
            offset = (i - j) * block
            if j == i:
                scores = jnp.where(gap_base >= 0, scores, NEG_FILL)
            if offset + block - 1 >= SPAN_MIN:
                scores = jnp.where(gap_base < reach - offset, scores, NEG_FILL)
            pieces.append(scores)
        peak = jnp.max(functools.reduce(jnp.maximum, pieces), axis=1, keepdims=True)
        total = None
        for j in range(i + 1):
            weights = jnp.exp2((pieces[j] - peak) * factor)
            weight_ref[i, :, j * block : (j + 1) * block] = weights.astype(jnp.bfloat16)
            total = weights if total is None else total + weights
        total_ref[i] = jnp.sum(total, axis=1, keepdims=True)


def attend(n_seq, flip, me_ref, weight_ref, total_ref, *refs):
    v_refs, (near_ref, far_ref, v_all) = refs[:n_seq], refs[n_seq:]
    me = me_ref[0]
    block = near_ref.shape[0]
    for other in range(n_seq):
        v_all[pl.ds(pl.multiple_of((me ^ other) * block, block), block)] = v_refs[other][...]
    chosen = me ^ flip

    def rows_of(i):
        width = (i + 1) * block
        numerator = jnp.dot(
            weight_ref[i, :, :width], v_all[:width], preferred_element_type=jnp.float32
        )
        return (numerator / total_ref[i]).astype(jnp.bfloat16)

    for i in range(n_seq):

        @pl.when(chosen == i)
        def _():
            near_ref[...] = rows_of(i)
            far_ref[...] = rows_of(n_seq - 1 - i)


def project(n_seq, wanted, me_ref, *refs):
    o_refs, w_ref = refs[:n_seq], refs[n_seq]
    far_ref, near_ref, joined = refs[n_seq + 1 :]
    me, head = me_ref[0], me_ref[1]
    for flip in range(n_seq):
        at = pl.multiple_of((me ^ flip) * HEAD_DIM, HEAD_DIM)
        joined[:, pl.ds(at, HEAD_DIM)] = o_refs[flip][...]
    width = far_ref.shape[1]
    for out_ref, flip in ((far_ref, wanted ^ 2), (near_ref, wanted)):
        at = pl.multiple_of((head ^ flip) * width, width)
        out_ref[...] = jnp.dot(
            joined[...], w_ref[:, pl.ds(at, width)], preferred_element_type=jnp.float32
        ).astype(jnp.bfloat16)


def headwise_path(queries, keys_in, values_in, out_weight, spans, full_ids):
    n_seq = lax.axis_size("seq")
    bf16, f32 = jnp.bfloat16, jnp.float32
    where = jnp.stack([lax.axis_index("seq"), lax.axis_index("head")]).astype(jnp.int32)
    block = queries.shape[0]
    tokens = block * n_seq
    head_block = jax.ShapeDtypeStruct((block, HEAD_DIM), bf16)
    pair_block = jax.ShapeDtypeStruct((2 * block, HEAD_DIM), bf16)
    flips = sorted(range(1, n_seq), key=lambda flip: -flip)

    qk = own_kernel(
        functools.partial(deal_heads, n_seq), [pair_block] * n_seq, [SMEM] + in_vmem(2)
    )(where, queries, keys_in)
    v = own_kernel(functools.partial(deal_heads, n_seq), [head_block] * n_seq, [SMEM] + in_vmem(1))(
        where, values_in
    )
    qk, v = list(qk), list(v)
    for flip in flips:
        qk[flip] = swap(qk[flip], "seq", flip)
    for flip in flips:
        v[flip] = swap(v[flip], "seq", flip)
    w_held = held(out_weight)
    qk = [held(a) for a in qk]
    v = [held(a) for a in v]

    weights, totals = own_kernel(
        functools.partial(weigh, n_seq),
        [
            jax.ShapeDtypeStruct((n_seq, block, tokens), bf16),
            jax.ShapeDtypeStruct((n_seq, block, 1), f32),
        ],
        [SMEM] * 3 + in_vmem(n_seq),
        [pltpu.VMEM((tokens, HEAD_DIM), bf16)] * 2,
        flops=4 * 10**9,
    )(where, spans, full_ids, *qk)
    came = [None] * n_seq
    for flip in range(n_seq // 2):
        near, far = own_kernel(
            functools.partial(attend, n_seq, flip),
            [head_block] * 2,
            [SMEM] + in_vmem(2 + n_seq),
            [pltpu.VMEM((tokens, HEAD_DIM), bf16)],
            flops=10**9,
        )(where, held(weights), held(totals), *v)
        mirror = n_seq - 1 - flip
        came[mirror] = swap(far, "seq", mirror)
        came[flip] = swap(near, "seq", flip) if flip else near
    came = [held(a) for a in came]
    width = out_weight.shape[1] // lax.axis_size("head")
    halves = [
        own_kernel(
            functools.partial(project, n_seq, wanted),
            [jax.ShapeDtypeStruct((block, width), bf16)] * 2,
            [SMEM] + in_vmem(n_seq + 1),
            [pltpu.VMEM((block, n_seq * HEAD_DIM), bf16)],
            flops=10**9,
        )(where, *came, w_held)
        for wanted in (1, 0)
    ]
    far = swap(halves[0][0], "head", 1)
    near = swap(halves[0][1], "head", 1)
    far = (far.astype(f32) + halves[1][0].astype(f32)).astype(bf16)
    far = swap(far, "head", 2)
    near = (near.astype(f32) + halves[1][1].astype(f32)).astype(bf16)
    return (near.astype(f32) + far.astype(f32)).astype(bf16)


def on_device(queries, keys_in, values_in, out_weight, spans, full_ids):
    n_seq, n_head = lax.axis_size("seq"), lax.axis_size("head")
    one_head_each = queries.shape[1] == n_seq * HEAD_DIM
    if one_head_each and n_head == 4 and n_seq == 8 and queries.shape[0] % 128 == 0:
        return headwise_path(queries, keys_in, values_in, out_weight, spans, full_ids)
    return ring_path(queries, keys_in, values_in, out_weight, spans, full_ids)


def solution(mesh):
    placed = (
        P("seq", "head"),
        P("seq", "head"),
        P("seq", "head"),
        P("head", None),
        P("head"),
        P("head"),
    )
    return jax.shard_map(
        on_device, mesh=mesh, in_specs=placed, out_specs=P("seq", "head"), check_vma=False
    )
```

```python
import math

import functools

import jax
import jax.numpy as jnp
from jax import lax
from jax.experimental import pallas as pl
from jax.experimental.pallas import tpu as pltpu
from jax.sharding import PartitionSpec as P

HEAD_DIM = 128
SPAN_MAX = 4096
SPAN_MIN = 1024


NEG_FILL = -1e30


def from_behind(block, axis, distance):
    devices = range(lax.axis_size(axis))
    route = [(i - distance, i) for i in devices if i - distance in devices]
    return lax.ppermute(block, axis, route)


def online_update(carry_state, scores, allowed, value_rows):
    old_peak, row_total, numerator = carry_state
    masked = jnp.where(allowed, scores, NEG_FILL)
    new_peak = jnp.maximum(old_peak, jnp.max(masked, axis=-1))
    weights = jnp.where(allowed, jnp.exp(masked - new_peak[..., None]), 0.0)
    rescale = jnp.exp(old_peak - new_peak)
    row_total = row_total * rescale + jnp.sum(weights, axis=-1)
    numerator = numerator * rescale[..., None] + jnp.einsum(
        "hqk,hkd->hqd", weights.astype(jnp.bfloat16), value_rows, preferred_element_type=jnp.float32
    )
    return (new_peak, row_total, numerator)


def empty_state(lead_count, row_count, head_width):
    return (
        jnp.full((lead_count, row_count), NEG_FILL, jnp.float32),
        jnp.zeros((lead_count, row_count), jnp.float32),
        jnp.zeros((lead_count, row_count, head_width), jnp.float32),
    )


def finish(carry_state):
    return (carry_state[2] / carry_state[1][..., None]).astype(jnp.bfloat16)


def ring_path(queries, keys_in, values_in, out_weight, spans, full_ids):
    score_scale = HEAD_DIM ** (-0.5)
    n_seq = lax.axis_size("seq")
    seq_index = lax.axis_index("seq")
    tok_rows = queries.shape[0]
    group_heads = queries.shape[1] // HEAD_DIM
    full_count = full_ids.shape[0]
    band_count = group_heads - full_count
    head_base = lax.axis_index("head") * group_heads
    local_range = jnp.arange(group_heads)
    marks = jnp.sum(
        (local_range[:, None] + head_base == full_ids[None, :]).astype(jnp.int32), axis=1
    )
    order_local = jnp.argsort(marks * group_heads + local_range)
    band_local = order_local[:band_count]
    full_local = order_local[band_count:]
    query_three = queries.reshape(tok_rows, group_heads, HEAD_DIM)
    key_three = keys_in.reshape(tok_rows, group_heads, HEAD_DIM)
    value_three = values_in.reshape(tok_rows, group_heads, HEAD_DIM)
    query_band = jnp.take(query_three, band_local, axis=1).transpose(1, 0, 2)
    kv_band = jnp.stack(
        [
            jnp.take(key_three, band_local, axis=1).transpose(1, 0, 2),
            jnp.take(value_three, band_local, axis=1).transpose(1, 0, 2),
        ]
    )
    band_reach = jnp.take(spans, band_local)
    query_pos = seq_index * tok_rows + jnp.arange(tok_rows)
    hop_count = min(max(1, SPAN_MAX // tok_rows), n_seq - 1)
    arrived = [(kv_band, 0)]
    moving = kv_band
    for distance in range(1, hop_count + 1):
        moving = from_behind(moving, "seq", 1)
        arrived.append((moving, distance))
    batch_size = max(1, 512 // tok_rows)
    band_state = empty_state(band_count, tok_rows, HEAD_DIM)
    for first_piece in range(0, len(arrived), batch_size):
        batch_pieces = arrived[first_piece : first_piece + batch_size]
        key_rows = jnp.concatenate([arrival[0][0] for arrival in batch_pieces], axis=1)
        value_rows = jnp.concatenate([arrival[0][1] for arrival in batch_pieces], axis=1)
        key_pos = jnp.concatenate(
            [(seq_index - arrival[1]) * tok_rows + jnp.arange(tok_rows) for arrival in batch_pieces]
        )
        scores = (
            jnp.einsum("hqd,hkd->hqk", query_band, key_rows, preferred_element_type=jnp.float32)
            * score_scale
        )
        gap_size = query_pos[None, :, None] - key_pos[None, None, :]
        allowed = (
            (gap_size >= 0) & (gap_size < band_reach[:, None, None]) & (key_pos >= 0)[None, None, :]
        )
        band_state = online_update(band_state, scores, allowed, value_rows)
    band_out = finish(band_state)
    query_full = jnp.take(query_three, full_local, axis=1).transpose(1, 0, 2)
    key_full = jnp.take(key_three, full_local, axis=1).transpose(1, 0, 2)
    value_full = jnp.take(value_three, full_local, axis=1).transpose(1, 0, 2)
    kv_full = jnp.stack([key_full, value_full])
    last_query = seq_index * tok_rows + tok_rows - 1
    key_piece = lax.all_gather(kv_full, "seq", axis=2, tiled=True)
    row_count = key_piece.shape[2]
    tile_rows = math.gcd(row_count, 512)

    def absorb_tile(tile_index, inner_state):
        key_tile = lax.dynamic_slice_in_dim(key_piece[0], tile_index * tile_rows, tile_rows, 1)
        value_tile = lax.dynamic_slice_in_dim(key_piece[1], tile_index * tile_rows, tile_rows, 1)
        key_pos = tile_index * tile_rows + jnp.arange(tile_rows)
        scores = (
            jnp.einsum("hqd,hkd->hqk", query_full, key_tile, preferred_element_type=jnp.float32)
            * score_scale
        )
        allowed = key_pos[None, None, :] <= query_pos[None, :, None]
        return online_update(inner_state, scores, allowed, value_tile)

    live_tiles = jnp.clip(last_query // tile_rows + 1, 0, row_count // tile_rows)
    full_state = lax.fori_loop(
        0, live_tiles, absorb_tile, empty_state(full_count, tok_rows, HEAD_DIM)
    )
    full_out = finish(full_state)
    combined = jnp.concatenate([band_out, full_out], axis=0)
    inverse = jnp.argsort(order_local)
    per_head = jnp.take(combined, inverse, axis=0)
    attended = per_head.transpose(1, 0, 2).reshape(tok_rows, group_heads * HEAD_DIM)
    projected = jnp.dot(attended, out_weight, preferred_element_type=jnp.float32)
    return lax.psum_scatter(projected.astype(jnp.bfloat16), "head", scatter_dimension=1, tiled=True)


def move(block, axis, pairs):
    return lax.ppermute(block, axis, pairs)


def swap(block, axis, flip):
    return move(block, axis, [(i, i ^ flip) for i in range(lax.axis_size(axis))])


def in_vmem(count):
    return [pl.BlockSpec(memory_space=pltpu.VMEM)] * count


def held(array):
    return pltpu.with_memory_space_constraint(array, pltpu.VMEM)


SMEM = pl.BlockSpec(memory_space=pltpu.SMEM)
FACTOR = HEAD_DIM**-0.5 * math.log2(math.e)
STAT_ROWS = 16


def own_kernel(body, out_shapes, in_specs, scratch=(), flops=10**8, limit=20 * 2**20):
    return pl.pallas_call(
        body,
        out_shape=out_shapes,
        in_specs=in_specs,
        out_specs=in_vmem(len(out_shapes)),
        scratch_shapes=list(scratch),
        compiler_params=pltpu.CompilerParams(vmem_limit_bytes=limit),
        cost_estimate=pl.CostEstimate(flops=flops, bytes_accessed=10**6, transcendentals=0),
    )


def deal(half, me_ref, q_ref, k_ref, v_ref, *refs):
    inner, cross, sems = refs[:half], refs[half : 2 * half], refs[2 * half]
    me = me_ref[0]
    low = me % half
    rows = q_ref.shape[0]
    copies = []

    def fetch(source, head, out_ref, place):
        at = pl.multiple_of(head * HEAD_DIM, HEAD_DIM)
        copies.append(
            pltpu.make_async_copy(
                source.at[:, pl.ds(at, HEAD_DIM)],
                out_ref.at[pl.ds(place * rows, rows)],
                sems.at[len(copies)],
            )
        )
        return copies[-1]

    for flip in range(half):
        target = low ^ flip
        for place in range(6):
            source = (q_ref, k_ref, v_ref)[place % 3]
            fetch(source, target + place // 3 * half, inner[flip], place).start()
    for flip in range(half):
        target = low ^ flip
        fetch(v_ref, target + half, cross[flip], 1).start()
        below = fetch(k_ref, target + half, cross[flip], 0)
        copies.pop()
        above = fetch(q_ref, target, cross[flip], 0)

        @pl.when(me < half)
        def _():
            below.start()

        @pl.when(me >= half)
        def _():
            above.start()

    for copy in copies:
        copy.wait()


def square_eye(size):
    row = lax.broadcasted_iota(jnp.int32, (size, size), 0)
    return row == lax.broadcasted_iota(jnp.int32, (size, size), 1)


def pack_stat(stat):
    eye = square_eye(HEAD_DIM)
    rows = []
    for first in range(0, stat.shape[0], HEAD_DIM):
        piece = jnp.where(eye, stat[first : first + HEAD_DIM], 0.0)
        left = jnp.sum(piece, axis=0, keepdims=True)
        for _ in range(3):
            part = left.astype(jnp.bfloat16).astype(jnp.float32)
            rows.append(part)
            left = left - part
    rows.append(jnp.zeros((STAT_ROWS - len(rows), HEAD_DIM), jnp.float32))
    return jnp.concatenate(rows, axis=0).astype(jnp.bfloat16)


def unpack_stat(packed, size):
    eye = square_eye(HEAD_DIM)
    columns = []
    packed = packed.astype(jnp.float32)
    for index in range(size // HEAD_DIM):
        row = packed[3 * index : 3 * index + 1]
        for more in (1, 2):
            row = row + packed[3 * index + more : 3 * index + more + 1]
        columns.append(jnp.sum(jnp.where(eye, row, 0.0), axis=1, keepdims=True))
    return jnp.concatenate(columns, axis=0)


def softmax_rows(pieces, value_tiles):
    peak = jnp.max(functools.reduce(jnp.maximum, pieces), axis=1, keepdims=True)
    total, numerator = None, None
    for scores, value_tile in zip(pieces, value_tiles):
        weights = jnp.exp2((scores - peak) * FACTOR)
        total = weights if total is None else total + weights
        product = jnp.dot(
            weights.astype(jnp.bfloat16), value_tile, preferred_element_type=jnp.float32
        )
        numerator = product if numerator is None else numerator + product
    return numerator, jnp.sum(total, axis=1, keepdims=True), peak


def score_tile(q_tile, k_tile):
    return lax.dot_general(
        q_tile, k_tile, (((1,), (1,)), ((), ())), preferred_element_type=jnp.float32
    )


def attend_own_half(half, me_ref, *refs):
    inner, out_refs = refs[:half], refs[half : 2 * half]
    num_ref, total_ref, peak_ref, qkv, o_low, o_up, stats = refs[2 * half :]
    low = me_ref[0] % half
    block = out_refs[0].shape[0] // 2
    for flip in range(half):
        at = pl.multiple_of((low ^ flip) * block, block)
        for place in range(6):
            qkv[place, pl.ds(at, block)] = inner[flip][place * block : (place + 1) * block]
    row = lax.broadcasted_iota(jnp.int32, (block, block), 0)
    causal = row >= lax.broadcasted_iota(jnp.int32, (block, block), 1)
    for head in range(2):
        for i in range(half):
            q_tile = qkv[3 * head, i * block : (i + 1) * block]
            pieces, value_tiles = [], []
            for j in range(i + 1):
                scores = score_tile(q_tile, qkv[3 * head + 1, j * block : (j + 1) * block])
                pieces.append(jnp.where(causal, scores, NEG_FILL) if i == j else scores)
                value_tiles.append(qkv[3 * head + 2, j * block : (j + 1) * block])
            numerator, total, peak = softmax_rows(pieces, value_tiles)
            result = (numerator / total).astype(jnp.bfloat16)
            if head == 0:
                o_low[i] = result
                stats[i] = pack_stat(peak * FACTOR + jnp.log2(total))
            else:
                o_up[i] = result
                num_ref[i] = numerator
                total_ref[i] = total
                peak_ref[i] = peak
    for flip in range(half):
        out_refs[flip][:block] = o_low[low ^ flip]

        @pl.when(me_ref[0] < half)
        def _():
            out_refs[flip][block:] = o_up[low ^ flip]

        @pl.when(me_ref[0] >= half)
        def _():
            out_refs[flip][block : block + STAT_ROWS] = stats[low ^ flip]


def attend_across(half, flip, me_ref, spans_ref, full_ref, num_ref, total_ref, peak_ref, *refs):
    inner, cross = refs[:half], refs[half : 2 * half]
    out_ref, q_tile, k_tiles, v_tiles = refs[2 * half :]
    me, head = me_ref[0], me_ref[1]
    low = me % half
    block = q_tile.shape[0]
    below = me < half

    @pl.when(below)
    def _():
        q_tile[...] = cross[flip][:block]
        for other in range(half):
            k_tiles[other] = inner[other][block : 2 * block]
            v_tiles[other] = inner[other][2 * block : 3 * block]

    @pl.when(jnp.logical_not(below))
    def _():
        q_tile[...] = inner[flip][3 * block : 4 * block]
        for other in range(half):
            k_tiles[other] = cross[other][:block]
            v_tiles[other] = cross[other][block:]

    local = jnp.where(below, low, low + half)
    reach = spans_ref[local]
    for place in range(full_ref.shape[0]):
        reach = jnp.where(full_ref[place] == head * 2 * half + local, 2 * half * block, reach)
    row_block = low ^ flip
    row = lax.broadcasted_iota(jnp.int32, (block, block), 0)
    gap = row - lax.broadcasted_iota(jnp.int32, (block, block), 1)
    pieces = []
    for other in range(half):
        offset = (half + row_block - (low ^ other)) * block
        scores = score_tile(q_tile[...], k_tiles[other])
        pieces.append(jnp.where(gap < reach - offset, scores, NEG_FILL))
    numerator, total, peak = softmax_rows(pieces, [v_tiles[other] for other in range(half)])
    own_peak = jnp.where(below, NEG_FILL, peak_ref[row_block])
    joint = jnp.maximum(peak, own_peak)
    scale = jnp.exp2((peak - joint) * FACTOR)
    own_scale = jnp.where(below, 0.0, jnp.exp2((own_peak - joint) * FACTOR))
    numerator = numerator * scale + num_ref[row_block] * own_scale
    total = total * scale + total_ref[row_block] * own_scale
    out_ref[:block] = (numerator / total).astype(jnp.bfloat16)
    out_ref[block:] = pack_stat(joint * FACTOR + jnp.log2(total))


def join_heads(half, me_ref, *refs):
    own, across, upper = refs[:half], refs[half : 2 * half], refs[2 * half : 3 * half]
    joined = refs[3 * half]
    me = me_ref[0]
    low = me % half
    block = joined.shape[0]
    for flip in range(half):
        at = pl.multiple_of((low ^ flip) * HEAD_DIM, HEAD_DIM)
        up_at = pl.multiple_of((low ^ flip) * HEAD_DIM + half * HEAD_DIM, HEAD_DIM)

        @pl.when(me < half)
        def _():
            joined[:, pl.ds(at, HEAD_DIM)] = own[flip][:block]
            joined[:, pl.ds(up_at, HEAD_DIM)] = own[flip][block:]

        @pl.when(me >= half)
        def _():
            here = unpack_stat(own[flip][block : block + STAT_ROWS], block)
            there = unpack_stat(across[flip][block:], block)
            joint = jnp.maximum(here, there)
            here, there = jnp.exp2(here - joint), jnp.exp2(there - joint)
            total = here + there
            mixed = own[flip][:block].astype(jnp.float32) * (here / total)
            mixed = mixed + across[flip][:block].astype(jnp.float32) * (there / total)
            joined[:, pl.ds(at, HEAD_DIM)] = mixed.astype(jnp.bfloat16)
            joined[:, pl.ds(up_at, HEAD_DIM)] = upper[flip][:block]


def project(flip, me_ref, joined, w_ref, out_ref):
    width = out_ref.shape[1]
    at = pl.multiple_of((me_ref[1] ^ flip) * width, width)
    out_ref[...] = jnp.dot(
        joined[...], w_ref[:, pl.ds(at, width)], preferred_element_type=jnp.float32
    ).astype(jnp.bfloat16)


def half_path(queries, keys_in, values_in, out_weight, spans, full_ids):
    n_seq = lax.axis_size("seq")
    half = n_seq // 2
    bf16, f32 = jnp.bfloat16, jnp.float32
    shape = jax.ShapeDtypeStruct
    where = jnp.stack([lax.axis_index("seq"), lax.axis_index("head")]).astype(jnp.int32)
    block = queries.shape[0]
    hbm = pl.BlockSpec(memory_space=pltpu.HBM)

    dealt = own_kernel(
        functools.partial(deal, half),
        [shape((6 * block, HEAD_DIM), bf16)] * half + [shape((2 * block, HEAD_DIM), bf16)] * half,
        [SMEM] + [hbm] * 3,
        [pltpu.SemaphoreType.DMA((8 * half,))],
    )(where, queries, keys_in, values_in)
    inner, cross = list(dealt[:half]), list(dealt[half:])
    for flip in range(half - 1, 0, -1):
        inner[flip] = swap(inner[flip], "seq", flip)
    for flip in range(half - 1, -1, -1):
        cross[flip] = swap(cross[flip], "seq", half + flip)
    w_held = held(out_weight)
    inner = [held(a) for a in inner]
    cross = [held(a) for a in cross]

    *own, numerator, total, peak = own_kernel(
        functools.partial(attend_own_half, half),
        [shape((2 * block, HEAD_DIM), bf16)] * half
        + [shape((half, block, HEAD_DIM), f32)]
        + [shape((half, block, 1), f32)] * 2,
        [SMEM] + in_vmem(half),
        [
            pltpu.VMEM((6, half * block, HEAD_DIM), bf16),
            pltpu.VMEM((half, block, HEAD_DIM), bf16),
            pltpu.VMEM((half, block, HEAD_DIM), bf16),
            pltpu.VMEM((half, STAT_ROWS, HEAD_DIM), bf16),
        ],
        flops=2 * 10**9,
    )(where, *inner)
    for flip in range(half - 1, 0, -1):
        own[flip] = swap(own[flip], "seq", flip)
    across, upper = [None] * half, [None] * half
    for flip in range(half - 1, -1, -1):
        (sent,) = own_kernel(
            functools.partial(attend_across, half, flip),
            [shape((block + STAT_ROWS, HEAD_DIM), bf16)],
            [SMEM] * 3 + in_vmem(3 + 2 * half),
            [
                pltpu.VMEM((block, HEAD_DIM), bf16),
                pltpu.VMEM((half, block, HEAD_DIM), bf16),
                pltpu.VMEM((half, block, HEAD_DIM), bf16),
            ],
            flops=10**9,
        )(where, spans, full_ids, held(numerator), held(total), held(peak), *inner, *cross)
        across[flip] = move(sent, "seq", [(i, half + (i ^ flip)) for i in range(half)])
        upper[flip] = sent
        if flip:
            upper[flip] = move(sent, "seq", [(half + i, half + (i ^ flip)) for i in range(half)])
    (joined,) = own_kernel(
        functools.partial(join_heads, half),
        [shape((block, n_seq * HEAD_DIM), bf16)],
        [SMEM] + in_vmem(3 * half),
    )(where, *[held(a) for a in own + across + upper])
    joined = held(joined)
    width = out_weight.shape[1] // lax.axis_size("head")

    def columns_of(flip):
        return own_kernel(
            functools.partial(project, flip),
            [shape((block, width), bf16)],
            [SMEM] + in_vmem(2),
            flops=10**9,
        )(where, joined, w_held)[0]

    far = swap(columns_of(3), "head", 1)
    far = (far.astype(f32) + columns_of(2).astype(f32)).astype(bf16)
    far = swap(far, "head", 2)
    near = swap(columns_of(1), "head", 1)
    near = (near.astype(f32) + columns_of(0).astype(f32)).astype(bf16)
    return (near.astype(f32) + far.astype(f32)).astype(bf16)


def on_device(queries, keys_in, values_in, out_weight, spans, full_ids):
    n_seq, n_head = lax.axis_size("seq"), lax.axis_size("head")
    block = queries.shape[0]
    one_head_each = queries.shape[1] == n_seq * HEAD_DIM
    if one_head_each and n_head == 4 and n_seq == 8 and block == 256:
        return half_path(queries, keys_in, values_in, out_weight, spans, full_ids)
    return ring_path(queries, keys_in, values_in, out_weight, spans, full_ids)


def solution(mesh):
    placed = (
        P("seq", "head"),
        P("seq", "head"),
        P("seq", "head"),
        P("head", None),
        P("head"),
        P("head"),
    )
    return jax.shard_map(
        on_device, mesh=mesh, in_specs=placed, out_specs=P("seq", "head"), check_vma=False
    )
```

```python
import math

import functools

import jax
import jax.numpy as jnp
from jax import lax
from jax.experimental import pallas as pl
from jax.experimental.pallas import tpu as pltpu
from jax.sharding import PartitionSpec as P

HEAD_DIM = 128
SPAN_MAX = 4096


NEG_FILL = -1e30


def from_behind(block, axis, distance):
    devices = range(lax.axis_size(axis))
    route = [(i - distance, i) for i in devices if i - distance in devices]
    return lax.ppermute(block, axis, route)


def online_update(carry_state, scores, allowed, value_rows):
    old_peak, row_total, numerator = carry_state
    masked = jnp.where(allowed, scores, NEG_FILL)
    new_peak = jnp.maximum(old_peak, jnp.max(masked, axis=-1))
    weights = jnp.where(allowed, jnp.exp(masked - new_peak[..., None]), 0.0)
    rescale = jnp.exp(old_peak - new_peak)
    row_total = row_total * rescale + jnp.sum(weights, axis=-1)
    numerator = numerator * rescale[..., None] + jnp.einsum(
        "hqk,hkd->hqd", weights.astype(jnp.bfloat16), value_rows, preferred_element_type=jnp.float32
    )
    return (new_peak, row_total, numerator)


def empty_state(lead_count, row_count, head_width):
    return (
        jnp.full((lead_count, row_count), NEG_FILL, jnp.float32),
        jnp.zeros((lead_count, row_count), jnp.float32),
        jnp.zeros((lead_count, row_count, head_width), jnp.float32),
    )


def finish(carry_state):
    return (carry_state[2] / carry_state[1][..., None]).astype(jnp.bfloat16)


def ring_path(queries, keys_in, values_in, out_weight, spans, full_ids):
    score_scale = HEAD_DIM ** (-0.5)
    n_seq = lax.axis_size("seq")
    seq_index = lax.axis_index("seq")
    tok_rows = queries.shape[0]
    group_heads = queries.shape[1] // HEAD_DIM
    full_count = full_ids.shape[0]
    band_count = group_heads - full_count
    head_base = lax.axis_index("head") * group_heads
    local_range = jnp.arange(group_heads)
    marks = jnp.sum(
        (local_range[:, None] + head_base == full_ids[None, :]).astype(jnp.int32), axis=1
    )
    order_local = jnp.argsort(marks * group_heads + local_range)
    band_local = order_local[:band_count]
    full_local = order_local[band_count:]
    query_three = queries.reshape(tok_rows, group_heads, HEAD_DIM)
    key_three = keys_in.reshape(tok_rows, group_heads, HEAD_DIM)
    value_three = values_in.reshape(tok_rows, group_heads, HEAD_DIM)
    query_band = jnp.take(query_three, band_local, axis=1).transpose(1, 0, 2)
    kv_band = jnp.stack(
        [
            jnp.take(key_three, band_local, axis=1).transpose(1, 0, 2),
            jnp.take(value_three, band_local, axis=1).transpose(1, 0, 2),
        ]
    )
    band_reach = jnp.take(spans, band_local)
    query_pos = seq_index * tok_rows + jnp.arange(tok_rows)
    hop_count = min(max(1, SPAN_MAX // tok_rows), n_seq - 1)
    arrived = [(kv_band, 0)]
    moving = kv_band
    for distance in range(1, hop_count + 1):
        moving = from_behind(moving, "seq", 1)
        arrived.append((moving, distance))
    batch_size = max(1, 512 // tok_rows)
    band_state = empty_state(band_count, tok_rows, HEAD_DIM)
    for first_piece in range(0, len(arrived), batch_size):
        batch_pieces = arrived[first_piece : first_piece + batch_size]
        key_rows = jnp.concatenate([arrival[0][0] for arrival in batch_pieces], axis=1)
        value_rows = jnp.concatenate([arrival[0][1] for arrival in batch_pieces], axis=1)
        key_pos = jnp.concatenate(
            [(seq_index - arrival[1]) * tok_rows + jnp.arange(tok_rows) for arrival in batch_pieces]
        )
        scores = (
            jnp.einsum("hqd,hkd->hqk", query_band, key_rows, preferred_element_type=jnp.float32)
            * score_scale
        )
        gap_size = query_pos[None, :, None] - key_pos[None, None, :]
        allowed = (
            (gap_size >= 0) & (gap_size < band_reach[:, None, None]) & (key_pos >= 0)[None, None, :]
        )
        band_state = online_update(band_state, scores, allowed, value_rows)
    band_out = finish(band_state)
    query_full = jnp.take(query_three, full_local, axis=1).transpose(1, 0, 2)
    key_full = jnp.take(key_three, full_local, axis=1).transpose(1, 0, 2)
    value_full = jnp.take(value_three, full_local, axis=1).transpose(1, 0, 2)
    kv_full = jnp.stack([key_full, value_full])
    last_query = seq_index * tok_rows + tok_rows - 1
    key_piece = lax.all_gather(kv_full, "seq", axis=2, tiled=True)
    row_count = key_piece.shape[2]
    tile_rows = math.gcd(row_count, 512)

    def absorb_tile(tile_index, inner_state):
        key_tile = lax.dynamic_slice_in_dim(key_piece[0], tile_index * tile_rows, tile_rows, 1)
        value_tile = lax.dynamic_slice_in_dim(key_piece[1], tile_index * tile_rows, tile_rows, 1)
        key_pos = tile_index * tile_rows + jnp.arange(tile_rows)
        scores = (
            jnp.einsum("hqd,hkd->hqk", query_full, key_tile, preferred_element_type=jnp.float32)
            * score_scale
        )
        allowed = key_pos[None, None, :] <= query_pos[None, :, None]
        return online_update(inner_state, scores, allowed, value_tile)

    live_tiles = jnp.clip(last_query // tile_rows + 1, 0, row_count // tile_rows)
    full_state = lax.fori_loop(
        0, live_tiles, absorb_tile, empty_state(full_count, tok_rows, HEAD_DIM)
    )
    full_out = finish(full_state)
    combined = jnp.concatenate([band_out, full_out], axis=0)
    inverse = jnp.argsort(order_local)
    per_head = jnp.take(combined, inverse, axis=0)
    attended = per_head.transpose(1, 0, 2).reshape(tok_rows, group_heads * HEAD_DIM)
    projected = jnp.dot(attended, out_weight, preferred_element_type=jnp.float32)
    return lax.psum_scatter(projected.astype(jnp.bfloat16), "head", scatter_dimension=1, tiled=True)


def move(block, axis, pairs):
    return lax.ppermute(block, axis, pairs)


def swap(block, axis, flip):
    return move(block, axis, [(i, i ^ flip) for i in range(lax.axis_size(axis))])


def in_vmem(count):
    return [pl.BlockSpec(memory_space=pltpu.VMEM)] * count


def held(array):
    return pltpu.with_memory_space_constraint(array, pltpu.VMEM)


SMEM = pl.BlockSpec(memory_space=pltpu.SMEM)
FACTOR = HEAD_DIM**-0.5 * math.log2(math.e)
STAT_ROWS = 16


def own_kernel(body, out_shapes, in_specs, scratch=(), flops=10**8, limit=20 * 2**20):
    return pl.pallas_call(
        body,
        out_shape=out_shapes,
        in_specs=in_specs,
        out_specs=in_vmem(len(out_shapes)),
        scratch_shapes=list(scratch),
        compiler_params=pltpu.CompilerParams(vmem_limit_bytes=limit),
        cost_estimate=pl.CostEstimate(flops=flops, bytes_accessed=10**6, transcendentals=0),
    )


def deal(half, me_ref, q_ref, k_ref, v_ref, *refs):
    inner, cross, cross_v = refs[:half], refs[half : 2 * half], refs[2 * half : 3 * half]
    sems = refs[3 * half]
    me = me_ref[0]
    low = me % half
    rows = q_ref.shape[0]
    waits = []

    def fetch(source, head, out_ref, place):
        at = pl.multiple_of(head * HEAD_DIM, HEAD_DIM)
        return pltpu.make_async_copy(
            source.at[:, pl.ds(at, HEAD_DIM)],
            out_ref.at[pl.ds(place * rows, rows)],
            sems.at[len(waits)],
        )

    for flip in range(half - 1, -1, -1):
        target = low ^ flip
        for place in range(6):
            source = (q_ref, k_ref, v_ref)[place % 3]
            copy = fetch(source, target + place // 3 * half, inner[flip], place)
            copy.start()
            waits.append(copy)
    for flip in range(half - 1, -1, -1):
        target = low ^ flip
        below = fetch(k_ref, target + half, cross[flip], 0)
        above = fetch(q_ref, target, cross[flip], 0)
        pl.when(me < half)(below.start)
        pl.when(me >= half)(above.start)
        waits.append(above)
        copy = fetch(v_ref, target + half, cross_v[flip], 0)
        copy.start()
        waits.append(copy)
    for copy in waits:
        copy.wait()


def square_eye(size):
    row = lax.broadcasted_iota(jnp.int32, (size, size), 0)
    return row == lax.broadcasted_iota(jnp.int32, (size, size), 1)


def pack_stat(stat):
    eye = square_eye(HEAD_DIM)
    rows = []
    for first in range(0, stat.shape[0], HEAD_DIM):
        piece = jnp.where(eye, stat[first : first + HEAD_DIM], 0.0)
        left = jnp.sum(piece, axis=0, keepdims=True)
        for _ in range(3):
            part = left.astype(jnp.bfloat16).astype(jnp.float32)
            rows.append(part)
            left = left - part
    rows.append(jnp.zeros((STAT_ROWS - len(rows), HEAD_DIM), jnp.float32))
    return jnp.concatenate(rows, axis=0).astype(jnp.bfloat16)


def unpack_stat(packed, size):
    eye = square_eye(HEAD_DIM)
    columns = []
    packed = packed.astype(jnp.float32)
    for index in range(size // HEAD_DIM):
        row = packed[3 * index : 3 * index + 1]
        for more in (1, 2):
            row = row + packed[3 * index + more : 3 * index + more + 1]
        columns.append(jnp.sum(jnp.where(eye, row, 0.0), axis=1, keepdims=True))
    return jnp.concatenate(columns, axis=0)


def softmax_rows(pieces, value_tiles):
    peak = jnp.max(functools.reduce(jnp.maximum, pieces), axis=1, keepdims=True)
    total, numerator = None, None
    for scores, value_tile in zip(pieces, value_tiles):
        weights = jnp.exp2((scores - peak) * FACTOR)
        total = weights if total is None else total + weights
        product = jnp.dot(
            weights.astype(jnp.bfloat16), value_tile, preferred_element_type=jnp.float32
        )
        numerator = product if numerator is None else numerator + product
    return numerator, jnp.sum(total, axis=1, keepdims=True), peak


def score_tile(q_tile, k_tile):
    return lax.dot_general(
        q_tile, k_tile, (((1,), (1,)), ((), ())), preferred_element_type=jnp.float32
    )


def attend_own_half(half, me_ref, *refs):
    inner, out_refs = refs[:half], refs[half : 2 * half]
    num_ref, total_ref, peak_ref, qkv, o_low, o_up, stats = refs[2 * half :]
    low = me_ref[0] % half
    block = out_refs[0].shape[0] // 2
    for flip in range(half):
        at = pl.multiple_of((low ^ flip) * block, block)
        for place in range(6):
            qkv[place, pl.ds(at, block)] = inner[flip][place * block : (place + 1) * block]
    row = lax.broadcasted_iota(jnp.int32, (block, block), 0)
    causal = row >= lax.broadcasted_iota(jnp.int32, (block, block), 1)
    for head in range(2):
        for i in range(half):
            q_tile = qkv[3 * head, i * block : (i + 1) * block]
            pieces, value_tiles = [], []
            for j in range(i + 1):
                scores = score_tile(q_tile, qkv[3 * head + 1, j * block : (j + 1) * block])
                pieces.append(jnp.where(causal, scores, NEG_FILL) if i == j else scores)
                value_tiles.append(qkv[3 * head + 2, j * block : (j + 1) * block])
            numerator, total, peak = softmax_rows(pieces, value_tiles)
            result = (numerator / total).astype(jnp.bfloat16)
            if head == 0:
                o_low[i] = result
                stats[i] = pack_stat(peak * FACTOR + jnp.log2(total))
            else:
                o_up[i] = result
                num_ref[i] = numerator
                total_ref[i] = total
                peak_ref[i] = peak
    for flip in range(half):
        out_refs[flip][:block] = o_low[low ^ flip]

        @pl.when(me_ref[0] < half)
        def _():
            out_refs[flip][block:] = o_up[low ^ flip]

        @pl.when(me_ref[0] >= half)
        def _():
            out_refs[flip][block : block + STAT_ROWS] = stats[low ^ flip]


def weigh_across(half, me_ref, spans_ref, full_ref, *refs):
    inner, cross = refs[:half], refs[half : 2 * half]
    weight_ref, total_ref, peak_ref, q_tiles, k_tiles = refs[2 * half :]
    me, head = me_ref[0], me_ref[1]
    low = me % half
    block = q_tiles.shape[1]
    below = me < half

    @pl.when(below)
    def _():
        for other in range(half):
            q_tiles[other] = cross[other][...]
            k_tiles[other] = inner[other][block : 2 * block]

    @pl.when(jnp.logical_not(below))
    def _():
        for other in range(half):
            q_tiles[other] = inner[other][3 * block : 4 * block]
            k_tiles[other] = cross[other][...]

    local = jnp.where(below, low, low + half)
    reach = spans_ref[local]
    for place in range(full_ref.shape[0]):
        reach = jnp.where(full_ref[place] == head * 2 * half + local, 2 * half * block, reach)
    row = lax.broadcasted_iota(jnp.int32, (block, block), 0)
    gap = row - lax.broadcasted_iota(jnp.int32, (block, block), 1)
    for flip in range(half):
        pieces = []
        for other in range(half):
            offset = (half + (low ^ flip) - (low ^ other)) * block
            scores = score_tile(q_tiles[flip], k_tiles[other])
            pieces.append(jnp.where(gap < reach - offset, scores, NEG_FILL))
        peak = jnp.max(functools.reduce(jnp.maximum, pieces), axis=1, keepdims=True)
        total = None
        for other in range(half):
            weights = jnp.exp2((pieces[other] - peak) * FACTOR)
            weight_ref[flip, :, other * block : (other + 1) * block] = weights.astype(jnp.bfloat16)
            total = weights if total is None else total + weights
        total_ref[flip] = jnp.sum(total, axis=1, keepdims=True)
        peak_ref[flip] = peak


def attend_across(half, flip, me_ref, num_ref, total_ref, peak_ref, *refs):
    weight_ref, far_total_ref, far_peak_ref = refs[:3]
    inner, cross_v = refs[3 : 3 + half], refs[3 + half : 3 + 2 * half]
    out_ref, values = refs[3 + 2 * half :]
    me = me_ref[0]
    block = out_ref.shape[0] - STAT_ROWS
    below = me < half

    @pl.when(below)
    def _():
        for other in range(half):
            values[other * block : (other + 1) * block] = inner[other][2 * block : 3 * block]

    @pl.when(jnp.logical_not(below))
    def _():
        for other in range(half):
            values[other * block : (other + 1) * block] = cross_v[other][...]

    numerator = jnp.dot(weight_ref[flip], values[...], preferred_element_type=jnp.float32)
    row_block = me % half ^ flip
    total, peak = far_total_ref[flip], far_peak_ref[flip]
    own_peak = jnp.where(below, NEG_FILL, peak_ref[row_block])
    joint = jnp.maximum(peak, own_peak)
    scale = jnp.exp2((peak - joint) * FACTOR)
    own_scale = jnp.where(below, 0.0, jnp.exp2((own_peak - joint) * FACTOR))
    numerator = numerator * scale + num_ref[row_block] * own_scale
    total = total * scale + total_ref[row_block] * own_scale
    out_ref[:block] = (numerator / total).astype(jnp.bfloat16)
    out_ref[block:] = pack_stat(joint * FACTOR + jnp.log2(total))


def join_heads(half, me_ref, *refs):
    own, across, upper = refs[:half], refs[half : 2 * half], refs[2 * half : 3 * half]
    joined = refs[3 * half]
    me = me_ref[0]
    low = me % half
    block = joined.shape[0]
    for flip in range(half):
        at = pl.multiple_of((low ^ flip) * HEAD_DIM, HEAD_DIM)
        up_at = pl.multiple_of((low ^ flip) * HEAD_DIM + half * HEAD_DIM, HEAD_DIM)

        @pl.when(me < half)
        def _():
            joined[:, pl.ds(at, HEAD_DIM)] = own[flip][:block]
            joined[:, pl.ds(up_at, HEAD_DIM)] = own[flip][block:]

        @pl.when(me >= half)
        def _():
            here = unpack_stat(own[flip][block : block + STAT_ROWS], block)
            there = unpack_stat(across[flip][block:], block)
            joint = jnp.maximum(here, there)
            here, there = jnp.exp2(here - joint), jnp.exp2(there - joint)
            total = here + there
            mixed = own[flip][:block].astype(jnp.float32) * (here / total)
            mixed = mixed + across[flip][:block].astype(jnp.float32) * (there / total)
            joined[:, pl.ds(at, HEAD_DIM)] = mixed.astype(jnp.bfloat16)
            joined[:, pl.ds(up_at, HEAD_DIM)] = upper[flip][:block]


def project(flip, part, parts, me_ref, joined, w_ref, out_ref):
    width = out_ref.shape[1]
    at = pl.multiple_of(((me_ref[1] ^ flip) * parts + part) * width, width)
    out_ref[...] = jnp.dot(
        joined[...], w_ref[:, pl.ds(at, width)], preferred_element_type=jnp.float32
    ).astype(jnp.bfloat16)


def half_path(queries, keys_in, values_in, out_weight, spans, full_ids):
    n_seq = lax.axis_size("seq")
    half = n_seq // 2
    bf16, f32 = jnp.bfloat16, jnp.float32
    shape = jax.ShapeDtypeStruct
    where = jnp.stack([lax.axis_index("seq"), lax.axis_index("head")]).astype(jnp.int32)
    block = queries.shape[0]
    down = range(half - 1, -1, -1)
    piece = shape((block, HEAD_DIM), bf16)

    dealt = own_kernel(
        functools.partial(deal, half),
        [shape((6 * block, HEAD_DIM), bf16)] * half + [piece] * (2 * half),
        [SMEM] + [pl.BlockSpec(memory_space=pltpu.HBM)] * 3,
        [pltpu.SemaphoreType.DMA((8 * half,))],
    )(where, *[pltpu.with_memory_space_constraint(a, pltpu.HBM) for a in (queries, keys_in, values_in)])
    inner, cross, cross_v = dealt[:half], dealt[half : 2 * half], dealt[2 * half :]
    inner, cross, cross_v = list(inner), list(cross), list(cross_v)
    for flip in range(half - 1, 0, -1):
        inner[flip] = swap(inner[flip], "seq", flip)
    for flip in down:
        cross[flip] = swap(cross[flip], "seq", half + flip)
    for flip in down:
        cross_v[flip] = move(cross_v[flip], "seq", [(i, half + (i ^ flip)) for i in range(half)])
    w_held = held(out_weight)
    inner = [held(a) for a in inner]
    cross = [held(a) for a in cross]
    cross_v = [held(a) for a in cross_v]

    *own, numerator, total, peak = own_kernel(
        functools.partial(attend_own_half, half),
        [shape((2 * block, HEAD_DIM), bf16)] * half
        + [shape((half, block, HEAD_DIM), f32)]
        + [shape((half, block, 1), f32)] * 2,
        [SMEM] + in_vmem(half),
        [
            pltpu.VMEM((6, half * block, HEAD_DIM), bf16),
            pltpu.VMEM((half, block, HEAD_DIM), bf16),
            pltpu.VMEM((half, block, HEAD_DIM), bf16),
            pltpu.VMEM((half, STAT_ROWS, HEAD_DIM), bf16),
        ],
        flops=2 * 10**9,
    )(where, *inner)
    for flip in range(half - 1, 0, -1):
        own[flip] = swap(own[flip], "seq", flip)
    weights = own_kernel(
        functools.partial(weigh_across, half),
        [shape((half, block, half * block), bf16)] + [shape((half, block, 1), f32)] * 2,
        [SMEM] * 3 + in_vmem(2 * half),
        [pltpu.VMEM((half, block, HEAD_DIM), bf16)] * 2,
        flops=2 * 10**9,
    )(where, spans, full_ids, *inner, *cross)
    state = [held(a) for a in (numerator, total, peak, *weights)]
    across, upper = [None] * half, [None] * half
    for flip in down:
        (sent,) = own_kernel(
            functools.partial(attend_across, half, flip),
            [shape((block + STAT_ROWS, HEAD_DIM), bf16)],
            [SMEM] + in_vmem(6 + 2 * half),
            [pltpu.VMEM((half * block, HEAD_DIM), bf16)],
            flops=5 * 10**8,
        )(where, *state, *inner, *cross_v)
        across[flip] = move(sent, "seq", [(i, half + (i ^ flip)) for i in range(half)])
        upper[flip] = sent
        if flip:
            upper[flip] = move(sent, "seq", [(half + i, half + (i ^ flip)) for i in range(half)])
    (joined,) = own_kernel(
        functools.partial(join_heads, half),
        [shape((block, n_seq * HEAD_DIM), bf16)],
        [SMEM] + in_vmem(3 * half),
    )(where, *[held(a) for a in own + across + upper])
    joined = held(joined)

    width = out_weight.shape[1] // lax.axis_size("head")

    def columns_of(flip, part, parts, rows):
        return own_kernel(
            functools.partial(project, flip, part, parts),
            [shape((block, width // parts), bf16)],
            [SMEM] + in_vmem(2),
            flops=10**9 // parts,
        )(where, rows, w_held)[0]

    def summed(came, kept):
        return (came.astype(f32) + kept.astype(f32)).astype(bf16)

    parts = 2
    sent = [columns_of(3, part, parts, joined) for part in range(parts)]
    came = [swap(a, "head", 1) for a in sent]
    rows, _ = lax.optimization_barrier((joined, sent[-1]))
    kept = [columns_of(2, part, parts, held(rows)) for part in range(parts)]
    far = [summed(a, b) for a, b in zip(came, kept)]
    rows, *far = lax.optimization_barrier((joined, *far))
    far = [swap(a, "head", 2) for a in far]
    near = columns_of(1, 0, 1, held(rows))
    near = swap(near, "head", 1)
    near = summed(near, columns_of(0, 0, 1, held(rows)))
    return (near.astype(f32) + jnp.concatenate(far, axis=1).astype(f32)).astype(bf16)


def on_device(queries, keys_in, values_in, out_weight, spans, full_ids):
    n_seq, n_head = lax.axis_size("seq"), lax.axis_size("head")
    block = queries.shape[0]
    one_head_each = queries.shape[1] == n_seq * HEAD_DIM
    if one_head_each and n_head == 4 and n_seq == 8 and block == 256:
        return half_path(queries, keys_in, values_in, out_weight, spans, full_ids)
    return ring_path(queries, keys_in, values_in, out_weight, spans, full_ids)


def solution(mesh):
    placed = (
        P("seq", "head"),
        P("seq", "head"),
        P("seq", "head"),
        P("head", None),
        P("head"),
        P("head"),
    )
    return jax.shard_map(
        on_device, mesh=mesh, in_specs=placed, out_specs=P("seq", "head"), check_vma=False
    )
```

```python
import math

import functools

import jax
import jax.numpy as jnp
from jax import lax
from jax.experimental import pallas as pl
from jax.experimental.pallas import tpu as pltpu
from jax.sharding import PartitionSpec as P

HEAD_DIM = 128
SPAN_MAX = 4096


NEG_FILL = -1e30


def from_behind(block, axis, distance):
    devices = range(lax.axis_size(axis))
    route = [(i - distance, i) for i in devices if i - distance in devices]
    return lax.ppermute(block, axis, route)


def online_update(carry_state, scores, allowed, value_rows):
    old_peak, row_total, numerator = carry_state
    masked = jnp.where(allowed, scores, NEG_FILL)
    new_peak = jnp.maximum(old_peak, jnp.max(masked, axis=-1))
    weights = jnp.where(allowed, jnp.exp(masked - new_peak[..., None]), 0.0)
    rescale = jnp.exp(old_peak - new_peak)
    row_total = row_total * rescale + jnp.sum(weights, axis=-1)
    numerator = numerator * rescale[..., None] + jnp.einsum(
        "hqk,hkd->hqd", weights.astype(jnp.bfloat16), value_rows, preferred_element_type=jnp.float32
    )
    return (new_peak, row_total, numerator)


def empty_state(lead_count, row_count, head_width):
    return (
        jnp.full((lead_count, row_count), NEG_FILL, jnp.float32),
        jnp.zeros((lead_count, row_count), jnp.float32),
        jnp.zeros((lead_count, row_count, head_width), jnp.float32),
    )


def finish(carry_state):
    return (carry_state[2] / carry_state[1][..., None]).astype(jnp.bfloat16)


def ring_path(queries, keys_in, values_in, out_weight, spans, full_ids):
    score_scale = HEAD_DIM ** (-0.5)
    n_seq = lax.axis_size("seq")
    seq_index = lax.axis_index("seq")
    tok_rows = queries.shape[0]
    group_heads = queries.shape[1] // HEAD_DIM
    full_count = full_ids.shape[0]
    band_count = group_heads - full_count
    head_base = lax.axis_index("head") * group_heads
    local_range = jnp.arange(group_heads)
    marks = jnp.sum(
        (local_range[:, None] + head_base == full_ids[None, :]).astype(jnp.int32), axis=1
    )
    order_local = jnp.argsort(marks * group_heads + local_range)
    band_local = order_local[:band_count]
    full_local = order_local[band_count:]
    query_three = queries.reshape(tok_rows, group_heads, HEAD_DIM)
    key_three = keys_in.reshape(tok_rows, group_heads, HEAD_DIM)
    value_three = values_in.reshape(tok_rows, group_heads, HEAD_DIM)
    query_band = jnp.take(query_three, band_local, axis=1).transpose(1, 0, 2)
    kv_band = jnp.stack(
        [
            jnp.take(key_three, band_local, axis=1).transpose(1, 0, 2),
            jnp.take(value_three, band_local, axis=1).transpose(1, 0, 2),
        ]
    )
    band_reach = jnp.take(spans, band_local)
    query_pos = seq_index * tok_rows + jnp.arange(tok_rows)
    hop_count = min(max(1, SPAN_MAX // tok_rows), n_seq - 1)
    arrived = [(kv_band, 0)]
    moving = kv_band
    for distance in range(1, hop_count + 1):
        moving = from_behind(moving, "seq", 1)
        arrived.append((moving, distance))
    batch_size = max(1, 512 // tok_rows)
    band_state = empty_state(band_count, tok_rows, HEAD_DIM)
    for first_piece in range(0, len(arrived), batch_size):
        batch_pieces = arrived[first_piece : first_piece + batch_size]
        key_rows = jnp.concatenate([arrival[0][0] for arrival in batch_pieces], axis=1)
        value_rows = jnp.concatenate([arrival[0][1] for arrival in batch_pieces], axis=1)
        key_pos = jnp.concatenate(
            [(seq_index - arrival[1]) * tok_rows + jnp.arange(tok_rows) for arrival in batch_pieces]
        )
        scores = (
            jnp.einsum("hqd,hkd->hqk", query_band, key_rows, preferred_element_type=jnp.float32)
            * score_scale
        )
        gap_size = query_pos[None, :, None] - key_pos[None, None, :]
        allowed = (
            (gap_size >= 0) & (gap_size < band_reach[:, None, None]) & (key_pos >= 0)[None, None, :]
        )
        band_state = online_update(band_state, scores, allowed, value_rows)
    band_out = finish(band_state)
    query_full = jnp.take(query_three, full_local, axis=1).transpose(1, 0, 2)
    key_full = jnp.take(key_three, full_local, axis=1).transpose(1, 0, 2)
    value_full = jnp.take(value_three, full_local, axis=1).transpose(1, 0, 2)
    kv_full = jnp.stack([key_full, value_full])
    last_query = seq_index * tok_rows + tok_rows - 1
    key_piece = lax.all_gather(kv_full, "seq", axis=2, tiled=True)
    row_count = key_piece.shape[2]
    tile_rows = math.gcd(row_count, 512)

    def absorb_tile(tile_index, inner_state):
        key_tile = lax.dynamic_slice_in_dim(key_piece[0], tile_index * tile_rows, tile_rows, 1)
        value_tile = lax.dynamic_slice_in_dim(key_piece[1], tile_index * tile_rows, tile_rows, 1)
        key_pos = tile_index * tile_rows + jnp.arange(tile_rows)
        scores = (
            jnp.einsum("hqd,hkd->hqk", query_full, key_tile, preferred_element_type=jnp.float32)
            * score_scale
        )
        allowed = key_pos[None, None, :] <= query_pos[None, :, None]
        return online_update(inner_state, scores, allowed, value_tile)

    live_tiles = jnp.clip(last_query // tile_rows + 1, 0, row_count // tile_rows)
    full_state = lax.fori_loop(
        0, live_tiles, absorb_tile, empty_state(full_count, tok_rows, HEAD_DIM)
    )
    full_out = finish(full_state)
    combined = jnp.concatenate([band_out, full_out], axis=0)
    inverse = jnp.argsort(order_local)
    per_head = jnp.take(combined, inverse, axis=0)
    attended = per_head.transpose(1, 0, 2).reshape(tok_rows, group_heads * HEAD_DIM)
    projected = jnp.dot(attended, out_weight, preferred_element_type=jnp.float32)
    return lax.psum_scatter(projected.astype(jnp.bfloat16), "head", scatter_dimension=1, tiled=True)


def move(block, axis, pairs):
    return lax.ppermute(block, axis, pairs)


def swap(block, axis, flip):
    return move(block, axis, [(i, i ^ flip) for i in range(lax.axis_size(axis))])


def in_vmem(count):
    return [pl.BlockSpec(memory_space=pltpu.VMEM)] * count


def held(array):
    return pltpu.with_memory_space_constraint(array, pltpu.VMEM)


SMEM = pl.BlockSpec(memory_space=pltpu.SMEM)
FACTOR = HEAD_DIM**-0.5 * math.log2(math.e)
STAT_ROWS = 16


def own_kernel(body, out_shapes, in_specs, scratch=(), flops=10**8, limit=20 * 2**20):
    return pl.pallas_call(
        body,
        out_shape=out_shapes,
        in_specs=in_specs,
        out_specs=in_vmem(len(out_shapes)),
        scratch_shapes=list(scratch),
        compiler_params=pltpu.CompilerParams(vmem_limit_bytes=limit),
        cost_estimate=pl.CostEstimate(flops=flops, bytes_accessed=10**6, transcendentals=0),
    )


def deal(half, me_ref, q_ref, k_ref, v_ref, *refs):
    inner, cross, cross_v = refs[:half], refs[half : 2 * half], refs[2 * half : 3 * half]
    sems = refs[3 * half]
    me = me_ref[0]
    low = me % half
    rows = q_ref.shape[0]
    waits = []

    def fetch(source, head, out_ref, place):
        at = pl.multiple_of(head * HEAD_DIM, HEAD_DIM)
        return pltpu.make_async_copy(
            source.at[:, pl.ds(at, HEAD_DIM)],
            out_ref.at[pl.ds(place * rows, rows)],
            sems.at[len(waits)],
        )

    for flip in range(half - 1, -1, -1):
        target = low ^ flip
        for place in range(6):
            source = (q_ref, k_ref, v_ref)[place % 3]
            copy = fetch(source, target + place // 3 * half, inner[flip], place)
            copy.start()
            waits.append(copy)
    for flip in range(half - 1, -1, -1):
        target = low ^ flip
        below = fetch(k_ref, target + half, cross[flip], 0)
        above = fetch(q_ref, target, cross[flip], 0)
        pl.when(me < half)(below.start)
        pl.when(me >= half)(above.start)
        waits.append(above)
        copy = fetch(v_ref, target + half, cross_v[flip], 0)
        copy.start()
        waits.append(copy)
    for copy in waits:
        copy.wait()


def square_eye(size):
    row = lax.broadcasted_iota(jnp.int32, (size, size), 0)
    return row == lax.broadcasted_iota(jnp.int32, (size, size), 1)


def pack_stat(stat):
    eye = square_eye(HEAD_DIM)
    rows = []
    for first in range(0, stat.shape[0], HEAD_DIM):
        piece = jnp.where(eye, stat[first : first + HEAD_DIM], 0.0)
        left = jnp.sum(piece, axis=0, keepdims=True)
        for _ in range(3):
            part = left.astype(jnp.bfloat16).astype(jnp.float32)
            rows.append(part)
            left = left - part
    rows.append(jnp.zeros((STAT_ROWS - len(rows), HEAD_DIM), jnp.float32))
    return jnp.concatenate(rows, axis=0).astype(jnp.bfloat16)


def unpack_stat(packed, size):
    eye = square_eye(HEAD_DIM)
    columns = []
    packed = packed.astype(jnp.float32)
    for index in range(size // HEAD_DIM):
        row = packed[3 * index : 3 * index + 1]
        for more in (1, 2):
            row = row + packed[3 * index + more : 3 * index + more + 1]
        columns.append(jnp.sum(jnp.where(eye, row, 0.0), axis=1, keepdims=True))
    return jnp.concatenate(columns, axis=0)


def softmax_rows(pieces, value_tiles):
    peak = jnp.max(functools.reduce(jnp.maximum, pieces), axis=1, keepdims=True)
    total, numerator = None, None
    for scores, value_tile in zip(pieces, value_tiles):
        weights = jnp.exp2((scores - peak) * FACTOR)
        total = weights if total is None else total + weights
        product = jnp.dot(
            weights.astype(jnp.bfloat16), value_tile, preferred_element_type=jnp.float32
        )
        numerator = product if numerator is None else numerator + product
    return numerator, jnp.sum(total, axis=1, keepdims=True), peak


def score_tile(q_tile, k_tile):
    return lax.dot_general(
        q_tile, k_tile, (((1,), (1,)), ((), ())), preferred_element_type=jnp.float32
    )


def attend_own_half(half, me_ref, *refs):
    inner, (o_low, o_up, stat_ref, num_ref, total_ref, peak_ref, qkv) = refs[:half], refs[half:]
    low = me_ref[0] % half
    block = o_low.shape[1]
    for flip in range(half):
        at = pl.multiple_of((low ^ flip) * block, block)
        for place in range(6):
            qkv[place, pl.ds(at, block)] = inner[flip][place * block : (place + 1) * block]
    row = lax.broadcasted_iota(jnp.int32, (block, block), 0)
    causal = row >= lax.broadcasted_iota(jnp.int32, (block, block), 1)
    for head in range(2):
        for i in range(half):
            q_tile = qkv[3 * head, i * block : (i + 1) * block]
            pieces, value_tiles = [], []
            for j in range(i + 1):
                scores = score_tile(q_tile, qkv[3 * head + 1, j * block : (j + 1) * block])
                pieces.append(jnp.where(causal, scores, NEG_FILL) if i == j else scores)
                value_tiles.append(qkv[3 * head + 2, j * block : (j + 1) * block])
            numerator, total, peak = softmax_rows(pieces, value_tiles)
            result = (numerator / total).astype(jnp.bfloat16)
            if head == 0:
                o_low[i] = result
                stat_ref[i] = pack_stat(peak * FACTOR + jnp.log2(total))
            else:
                o_up[i] = result
                num_ref[i] = numerator
                total_ref[i] = total
                peak_ref[i] = peak


def weigh_across(half, me_ref, spans_ref, full_ref, *refs):
    inner, cross = refs[:half], refs[half : 2 * half]
    weight_ref, total_ref, peak_ref, q_tiles, k_tiles = refs[2 * half :]
    me, head = me_ref[0], me_ref[1]
    low = me % half
    block = q_tiles.shape[1]
    below = me < half

    @pl.when(below)
    def _():
        for other in range(half):
            q_tiles[other] = cross[other][...]
            k_tiles[other] = inner[other][block : 2 * block]

    @pl.when(jnp.logical_not(below))
    def _():
        for other in range(half):
            q_tiles[other] = inner[other][3 * block : 4 * block]
            k_tiles[other] = cross[other][...]

    local = jnp.where(below, low, low + half)
    reach = spans_ref[local]
    for place in range(full_ref.shape[0]):
        reach = jnp.where(full_ref[place] == head * 2 * half + local, 2 * half * block, reach)
    row = lax.broadcasted_iota(jnp.int32, (block, block), 0)
    gap = row - lax.broadcasted_iota(jnp.int32, (block, block), 1)
    for flip in range(half):
        pieces = []
        for other in range(half):
            offset = (half + (low ^ flip) - (low ^ other)) * block
            scores = score_tile(q_tiles[flip], k_tiles[other])
            pieces.append(jnp.where(gap < reach - offset, scores, NEG_FILL))
        peak = jnp.max(functools.reduce(jnp.maximum, pieces), axis=1, keepdims=True)
        total = None
        for other in range(half):
            weights = jnp.exp2((pieces[other] - peak) * FACTOR)
            weight_ref[flip, :, other * block : (other + 1) * block] = weights.astype(jnp.bfloat16)
            total = weights if total is None else total + weights
        total_ref[flip] = jnp.sum(total, axis=1, keepdims=True)
        peak_ref[flip] = peak


def attend_across(half, flip, me_ref, *refs):
    o_low, o_up, stat_ref, num_ref, total_ref, peak_ref = refs[:6]
    weight_ref, far_total_ref, far_peak_ref = refs[6:9]
    inner, cross_v = refs[9 : 9 + half], refs[9 + half : 9 + 2 * half]
    across_ref, inner_ref, values = refs[9 + 2 * half :]
    me = me_ref[0]
    block = o_low.shape[1]
    below = me < half
    row_block = me % half ^ flip
    inner_ref[:block] = o_low[row_block]
    inner_ref[2 * block :] = stat_ref[row_block]

    @pl.when(below)
    def _():
        for other in range(half):
            values[other * block : (other + 1) * block] = inner[other][2 * block : 3 * block]

    @pl.when(jnp.logical_not(below))
    def _():
        for other in range(half):
            values[other * block : (other + 1) * block] = cross_v[other][...]

    numerator = jnp.dot(weight_ref[flip], values[...], preferred_element_type=jnp.float32)
    total, peak = far_total_ref[flip], far_peak_ref[flip]

    @pl.when(below)
    def _():
        across_ref[:block] = (numerator / total).astype(jnp.bfloat16)
        across_ref[block:] = pack_stat(peak * FACTOR + jnp.log2(total))
        inner_ref[block : 2 * block] = o_up[row_block]

    @pl.when(jnp.logical_not(below))
    def _():
        own_peak = peak_ref[row_block]
        joint = jnp.maximum(peak, own_peak)
        scale = jnp.exp2((peak - joint) * FACTOR)
        own_scale = jnp.exp2((own_peak - joint) * FACTOR)
        both = numerator * scale + num_ref[row_block] * own_scale
        both_total = total * scale + total_ref[row_block] * own_scale
        inner_ref[block : 2 * block] = (both / both_total).astype(jnp.bfloat16)


def join_heads(half, me_ref, inner, across, joined):
    me = me_ref[0]
    low = me % half
    block = joined.shape[0]
    for flip in range(half):
        at = pl.multiple_of((low ^ flip) * HEAD_DIM, HEAD_DIM)
        up_at = pl.multiple_of((low ^ flip) * HEAD_DIM + half * HEAD_DIM, HEAD_DIM)
        joined[:, pl.ds(up_at, HEAD_DIM)] = inner[flip][block : 2 * block]

        @pl.when(me < half)
        def _():
            joined[:, pl.ds(at, HEAD_DIM)] = inner[flip][:block]

        @pl.when(me >= half)
        def _():
            here = unpack_stat(inner[flip][2 * block :], block)
            there = unpack_stat(across[flip][block:], block)
            share = 1.0 / (1.0 + jnp.exp2(there - here))
            mixed = inner[flip][:block].astype(jnp.float32) * share
            mixed = mixed + across[flip][:block].astype(jnp.float32) * (1.0 - share)
            joined[:, pl.ds(at, HEAD_DIM)] = mixed.astype(jnp.bfloat16)


def join_and_project(half, flip, me_ref, *refs):
    inner, across, (w_ref, out_ref, joined) = refs[:half], refs[half : 2 * half], refs[2 * half :]
    join_heads(half, me_ref, inner, across, joined)
    project(flip, me_ref, joined, w_ref, out_ref)


def project(flip, me_ref, joined, w_ref, out_ref):
    width = out_ref.shape[1]
    at = pl.multiple_of((me_ref[1] ^ flip) * width, width)
    out_ref[...] = jnp.dot(
        joined[...], w_ref[:, pl.ds(at, width)], preferred_element_type=jnp.float32
    ).astype(jnp.bfloat16)


def half_path(queries, keys_in, values_in, out_weight, spans, full_ids):
    n_seq = lax.axis_size("seq")
    half = n_seq // 2
    bf16, f32 = jnp.bfloat16, jnp.float32
    shape = jax.ShapeDtypeStruct
    where = jnp.stack([lax.axis_index("seq"), lax.axis_index("head")]).astype(jnp.int32)
    block = queries.shape[0]
    down = range(half - 1, -1, -1)
    piece = shape((block, HEAD_DIM), bf16)

    dealt = own_kernel(
        functools.partial(deal, half),
        [shape((6 * block, HEAD_DIM), bf16)] * half + [piece] * (2 * half),
        [SMEM] + [pl.BlockSpec(memory_space=pltpu.HBM)] * 3,
        [pltpu.SemaphoreType.DMA((8 * half,))],
    )(where, *[pltpu.with_memory_space_constraint(a, pltpu.HBM) for a in (queries, keys_in, values_in)])
    inner, cross, cross_v = dealt[:half], dealt[half : 2 * half], dealt[2 * half :]
    inner, cross, cross_v = list(inner), list(cross), list(cross_v)
    for flip in range(half - 1, 0, -1):
        inner[flip] = swap(inner[flip], "seq", flip)
    for flip in down:
        cross[flip] = swap(cross[flip], "seq", half + flip)
    for flip in down:
        cross_v[flip] = move(cross_v[flip], "seq", [(i, half + (i ^ flip)) for i in range(half)])
    w_held = held(out_weight)
    inner = [held(a) for a in inner]
    cross = [held(a) for a in cross]
    cross_v = [held(a) for a in cross_v]

    own = own_kernel(
        functools.partial(attend_own_half, half),
        [shape((half, block, HEAD_DIM), bf16)] * 2
        + [shape((half, STAT_ROWS, HEAD_DIM), bf16), shape((half, block, HEAD_DIM), f32)]
        + [shape((half, block, 1), f32)] * 2,
        [SMEM] + in_vmem(half),
        [pltpu.VMEM((6, half * block, HEAD_DIM), bf16)],
        flops=2 * 10**9,
    )(where, *inner)
    weights = own_kernel(
        functools.partial(weigh_across, half),
        [shape((half, block, half * block), bf16)] + [shape((half, block, 1), f32)] * 2,
        [SMEM] * 3 + in_vmem(2 * half),
        [pltpu.VMEM((half, block, HEAD_DIM), bf16)] * 2,
        flops=2 * 10**9,
    )(where, spans, full_ids, *inner, *cross)
    state = [held(a) for a in (*own, *weights)]
    across, own_half = [None] * half, [None] * half
    for flip in range(half):
        far, near = own_kernel(
            functools.partial(attend_across, half, flip),
            [
                shape((block + STAT_ROWS, HEAD_DIM), bf16),
                shape((2 * block + STAT_ROWS, HEAD_DIM), bf16),
            ],
            [SMEM] + in_vmem(len(state) + 2 * half),
            [pltpu.VMEM((half * block, HEAD_DIM), bf16)],
            flops=5 * 10**8,
        )(where, *state, *inner, *cross_v)
        across[flip] = move(far, "seq", [(i, half + (i ^ flip)) for i in range(half)])
        own_half[flip] = swap(near, "seq", flip) if flip else near
    came = [held(a) for a in own_half + across]
    width = out_weight.shape[1] // lax.axis_size("head")
    part = shape((block, width), bf16)
    sent, joined = own_kernel(
        functools.partial(join_and_project, half, 3),
        [part, shape((block, n_seq * HEAD_DIM), bf16)],
        [SMEM] + in_vmem(2 * half + 1),
        flops=10**9,
    )(where, *came, w_held)

    def columns_of(flip, rows):
        return own_kernel(
            functools.partial(project, flip), [part], [SMEM] + in_vmem(2), flops=10**9
        )(where, held(rows), w_held)[0]

    def summed(one, other):
        return (one.astype(f32) + other.astype(f32)).astype(bf16)

    far = summed(swap(sent, "head", 1), columns_of(2, joined))
    rows, far = lax.optimization_barrier((joined, far))
    far = swap(far, "head", 2)
    near = columns_of(1, rows)
    near = summed(swap(near, "head", 1), columns_of(0, rows))
    return summed(near, far)


def on_device(queries, keys_in, values_in, out_weight, spans, full_ids):
    n_seq, n_head = lax.axis_size("seq"), lax.axis_size("head")
    block = queries.shape[0]
    one_head_each = queries.shape[1] == n_seq * HEAD_DIM
    if one_head_each and n_head == 4 and n_seq == 8 and block == 256:
        return half_path(queries, keys_in, values_in, out_weight, spans, full_ids)
    return ring_path(queries, keys_in, values_in, out_weight, spans, full_ids)


def solution(mesh):
    placed = (
        P("seq", "head"),
        P("seq", "head"),
        P("seq", "head"),
        P("head", None),
        P("head"),
        P("head"),
    )
    return jax.shard_map(
        on_device, mesh=mesh, in_specs=placed, out_specs=P("seq", "head"), check_vma=False
    )
```

```python
import math

import functools

import jax
import jax.numpy as jnp
from jax import lax
from jax.experimental import pallas as pl
from jax.experimental.pallas import tpu as pltpu
from jax.sharding import PartitionSpec as P

HEAD_DIM = 128
SPAN_MAX = 4096


NEG_FILL = -1e30


def from_behind(block, axis, distance):
    devices = range(lax.axis_size(axis))
    route = [(i - distance, i) for i in devices if i - distance in devices]
    return lax.ppermute(block, axis, route)


def online_update(carry_state, scores, allowed, value_rows):
    old_peak, row_total, numerator = carry_state
    masked = jnp.where(allowed, scores, NEG_FILL)
    new_peak = jnp.maximum(old_peak, jnp.max(masked, axis=-1))
    weights = jnp.where(allowed, jnp.exp(masked - new_peak[..., None]), 0.0)
    rescale = jnp.exp(old_peak - new_peak)
    row_total = row_total * rescale + jnp.sum(weights, axis=-1)
    numerator = numerator * rescale[..., None] + jnp.einsum(
        "hqk,hkd->hqd", weights.astype(jnp.bfloat16), value_rows, preferred_element_type=jnp.float32
    )
    return (new_peak, row_total, numerator)


def empty_state(lead_count, row_count, head_width):
    return (
        jnp.full((lead_count, row_count), NEG_FILL, jnp.float32),
        jnp.zeros((lead_count, row_count), jnp.float32),
        jnp.zeros((lead_count, row_count, head_width), jnp.float32),
    )


def finish(carry_state):
    return (carry_state[2] / carry_state[1][..., None]).astype(jnp.bfloat16)


def ring_path(queries, keys_in, values_in, out_weight, spans, full_ids):
    score_scale = HEAD_DIM ** (-0.5)
    n_seq = lax.axis_size("seq")
    seq_index = lax.axis_index("seq")
    tok_rows = queries.shape[0]
    group_heads = queries.shape[1] // HEAD_DIM
    full_count = full_ids.shape[0]
    band_count = group_heads - full_count
    head_base = lax.axis_index("head") * group_heads
    local_range = jnp.arange(group_heads)
    marks = jnp.sum(
        (local_range[:, None] + head_base == full_ids[None, :]).astype(jnp.int32), axis=1
    )
    order_local = jnp.argsort(marks * group_heads + local_range)
    band_local = order_local[:band_count]
    full_local = order_local[band_count:]
    query_three = queries.reshape(tok_rows, group_heads, HEAD_DIM)
    key_three = keys_in.reshape(tok_rows, group_heads, HEAD_DIM)
    value_three = values_in.reshape(tok_rows, group_heads, HEAD_DIM)
    query_band = jnp.take(query_three, band_local, axis=1).transpose(1, 0, 2)
    kv_band = jnp.stack(
        [
            jnp.take(key_three, band_local, axis=1).transpose(1, 0, 2),
            jnp.take(value_three, band_local, axis=1).transpose(1, 0, 2),
        ]
    )
    band_reach = jnp.take(spans, band_local)
    query_pos = seq_index * tok_rows + jnp.arange(tok_rows)
    hop_count = min(max(1, SPAN_MAX // tok_rows), n_seq - 1)
    arrived = [(kv_band, 0)]
    moving = kv_band
    for distance in range(1, hop_count + 1):
        moving = from_behind(moving, "seq", 1)
        arrived.append((moving, distance))
    batch_size = max(1, 512 // tok_rows)
    band_state = empty_state(band_count, tok_rows, HEAD_DIM)
    for first_piece in range(0, len(arrived), batch_size):
        batch_pieces = arrived[first_piece : first_piece + batch_size]
        key_rows = jnp.concatenate([arrival[0][0] for arrival in batch_pieces], axis=1)
        value_rows = jnp.concatenate([arrival[0][1] for arrival in batch_pieces], axis=1)
        key_pos = jnp.concatenate(
            [(seq_index - arrival[1]) * tok_rows + jnp.arange(tok_rows) for arrival in batch_pieces]
        )
        scores = (
            jnp.einsum("hqd,hkd->hqk", query_band, key_rows, preferred_element_type=jnp.float32)
            * score_scale
        )
        gap_size = query_pos[None, :, None] - key_pos[None, None, :]
        allowed = (
            (gap_size >= 0) & (gap_size < band_reach[:, None, None]) & (key_pos >= 0)[None, None, :]
        )
        band_state = online_update(band_state, scores, allowed, value_rows)
    band_out = finish(band_state)
    query_full = jnp.take(query_three, full_local, axis=1).transpose(1, 0, 2)
    key_full = jnp.take(key_three, full_local, axis=1).transpose(1, 0, 2)
    value_full = jnp.take(value_three, full_local, axis=1).transpose(1, 0, 2)
    kv_full = jnp.stack([key_full, value_full])
    last_query = seq_index * tok_rows + tok_rows - 1
    key_piece = lax.all_gather(kv_full, "seq", axis=2, tiled=True)
    row_count = key_piece.shape[2]
    tile_rows = math.gcd(row_count, 512)

    def absorb_tile(tile_index, inner_state):
        key_tile = lax.dynamic_slice_in_dim(key_piece[0], tile_index * tile_rows, tile_rows, 1)
        value_tile = lax.dynamic_slice_in_dim(key_piece[1], tile_index * tile_rows, tile_rows, 1)
        key_pos = tile_index * tile_rows + jnp.arange(tile_rows)
        scores = (
            jnp.einsum("hqd,hkd->hqk", query_full, key_tile, preferred_element_type=jnp.float32)
            * score_scale
        )
        allowed = key_pos[None, None, :] <= query_pos[None, :, None]
        return online_update(inner_state, scores, allowed, value_tile)

    live_tiles = jnp.clip(last_query // tile_rows + 1, 0, row_count // tile_rows)
    full_state = lax.fori_loop(
        0, live_tiles, absorb_tile, empty_state(full_count, tok_rows, HEAD_DIM)
    )
    full_out = finish(full_state)
    combined = jnp.concatenate([band_out, full_out], axis=0)
    inverse = jnp.argsort(order_local)
    per_head = jnp.take(combined, inverse, axis=0)
    attended = per_head.transpose(1, 0, 2).reshape(tok_rows, group_heads * HEAD_DIM)
    projected = jnp.dot(attended, out_weight, preferred_element_type=jnp.float32)
    return lax.psum_scatter(projected.astype(jnp.bfloat16), "head", scatter_dimension=1, tiled=True)


def move(block, axis, pairs):
    return lax.ppermute(block, axis, pairs)


def swap(block, axis, flip):
    return move(block, axis, [(i, i ^ flip) for i in range(lax.axis_size(axis))])


def in_vmem(count):
    return [pl.BlockSpec(memory_space=pltpu.VMEM)] * count


def held(array):
    return pltpu.with_memory_space_constraint(array, pltpu.VMEM)


SMEM = pl.BlockSpec(memory_space=pltpu.SMEM)
FACTOR = HEAD_DIM**-0.5 * math.log2(math.e)
STAT_ROWS = 16


def own_kernel(body, out_shapes, in_specs, scratch=(), flops=10**8, limit=20 * 2**20):
    return pl.pallas_call(
        body,
        out_shape=out_shapes,
        in_specs=in_specs,
        out_specs=in_vmem(len(out_shapes)),
        scratch_shapes=list(scratch),
        compiler_params=pltpu.CompilerParams(vmem_limit_bytes=limit),
        cost_estimate=pl.CostEstimate(flops=flops, bytes_accessed=10**6, transcendentals=0),
    )


def deal(half, me_ref, q_ref, k_ref, v_ref, *refs):
    inner, cross, cross_v = refs[:half], refs[half : 2 * half], refs[2 * half : 3 * half]
    sems = refs[3 * half]
    me = me_ref[0]
    low = me % half
    rows = q_ref.shape[0]
    waits = []

    def fetch(source, head, out_ref, place):
        at = pl.multiple_of(head * HEAD_DIM, HEAD_DIM)
        return pltpu.make_async_copy(
            source.at[:, pl.ds(at, HEAD_DIM)],
            out_ref.at[pl.ds(place * rows, rows)],
            sems.at[len(waits)],
        )

    for flip in range(half - 1, -1, -1):
        target = low ^ flip
        for place in range(6):
            source = (q_ref, k_ref, v_ref)[place % 3]
            copy = fetch(source, target + place // 3 * half, inner[flip], place)
            copy.start()
            waits.append(copy)
    for flip in range(half - 1, -1, -1):
        target = low ^ flip
        below = fetch(k_ref, target + half, cross[flip], 0)
        above = fetch(q_ref, target, cross[flip], 0)
        pl.when(me < half)(below.start)
        pl.when(me >= half)(above.start)
        waits.append(above)
        copy = fetch(v_ref, target + half, cross_v[flip], 0)
        copy.start()
        waits.append(copy)
    for copy in waits:
        copy.wait()


def square_eye(size):
    row = lax.broadcasted_iota(jnp.int32, (size, size), 0)
    return row == lax.broadcasted_iota(jnp.int32, (size, size), 1)


def pack_stat(stat):
    eye = square_eye(HEAD_DIM)
    rows = []
    for first in range(0, stat.shape[0], HEAD_DIM):
        piece = jnp.where(eye, stat[first : first + HEAD_DIM], 0.0)
        left = jnp.sum(piece, axis=0, keepdims=True)
        for _ in range(3):
            part = left.astype(jnp.bfloat16).astype(jnp.float32)
            rows.append(part)
            left = left - part
    rows.append(jnp.zeros((STAT_ROWS - len(rows), HEAD_DIM), jnp.float32))
    return jnp.concatenate(rows, axis=0).astype(jnp.bfloat16)


def share_column(here, there, size):
    eye = square_eye(HEAD_DIM)
    apart = there.astype(jnp.float32) - here.astype(jnp.float32)
    columns = []
    for index in range(size // HEAD_DIM):
        row = apart[3 * index : 3 * index + 1]
        for more in (1, 2):
            row = row + apart[3 * index + more : 3 * index + more + 1]
        share = 1.0 / (1.0 + jnp.exp2(row))
        columns.append(jnp.sum(jnp.where(eye, share, 0.0), axis=1, keepdims=True))
    return jnp.concatenate(columns, axis=0)


def softmax_rows(pieces, value_tiles):
    peak = jnp.max(functools.reduce(jnp.maximum, pieces), axis=1, keepdims=True)
    total, numerator = None, None
    for scores, value_tile in zip(pieces, value_tiles):
        weights = jnp.exp2((scores - peak) * FACTOR)
        total = weights if total is None else total + weights
        product = jnp.dot(
            weights.astype(jnp.bfloat16), value_tile, preferred_element_type=jnp.float32
        )
        numerator = product if numerator is None else numerator + product
    return numerator, jnp.sum(total, axis=1, keepdims=True), peak


def score_tile(q_tile, k_tile):
    return lax.dot_general(
        q_tile, k_tile, (((1,), (1,)), ((), ())), preferred_element_type=jnp.float32
    )


def attend_own_half(half, me_ref, *refs):
    inner, (o_low, o_up, stat_ref, num_ref, total_ref, peak_ref, qkv) = refs[:half], refs[half:]
    low = me_ref[0] % half
    block = o_low.shape[1]
    for flip in range(half):
        at = pl.multiple_of((low ^ flip) * block, block)
        for place in range(6):
            qkv[place, pl.ds(at, block)] = inner[flip][place * block : (place + 1) * block]
    row = lax.broadcasted_iota(jnp.int32, (block, block), 0)
    causal = row >= lax.broadcasted_iota(jnp.int32, (block, block), 1)
    for head in range(2):
        for i in range(half):
            q_tile = qkv[3 * head, i * block : (i + 1) * block]
            pieces, value_tiles = [], []
            for j in range(i + 1):
                scores = score_tile(q_tile, qkv[3 * head + 1, j * block : (j + 1) * block])
                pieces.append(jnp.where(causal, scores, NEG_FILL) if i == j else scores)
                value_tiles.append(qkv[3 * head + 2, j * block : (j + 1) * block])
            numerator, total, peak = softmax_rows(pieces, value_tiles)
            result = (numerator / total).astype(jnp.bfloat16)
            if head == 0:
                o_low[i] = result
                stat_ref[i] = pack_stat(peak * FACTOR + jnp.log2(total))
            else:
                o_up[i] = result
                num_ref[i] = numerator
                total_ref[i] = total
                peak_ref[i] = peak


def weigh_across(half, me_ref, spans_ref, full_ref, *refs):
    inner, cross = refs[:half], refs[half : 2 * half]
    weight_ref, total_ref, peak_ref, q_tiles, k_tiles = refs[2 * half :]
    me, head = me_ref[0], me_ref[1]
    low = me % half
    block = q_tiles.shape[1]
    below = me < half

    @pl.when(below)
    def _():
        for other in range(half):
            q_tiles[other] = cross[other][...]
            k_tiles[other] = inner[other][block : 2 * block]

    @pl.when(jnp.logical_not(below))
    def _():
        for other in range(half):
            q_tiles[other] = inner[other][3 * block : 4 * block]
            k_tiles[other] = cross[other][...]

    local = jnp.where(below, low, low + half)
    reach = spans_ref[local]
    for place in range(full_ref.shape[0]):
        reach = jnp.where(full_ref[place] == head * 2 * half + local, 2 * half * block, reach)
    row = lax.broadcasted_iota(jnp.int32, (block, block), 0)
    gap = row - lax.broadcasted_iota(jnp.int32, (block, block), 1)
    for flip in range(half):
        pieces = []
        for other in range(half):
            offset = (half + (low ^ flip) - (low ^ other)) * block
            scores = score_tile(q_tiles[flip], k_tiles[other])
            pieces.append(jnp.where(gap < reach - offset, scores, NEG_FILL))
        peak = jnp.max(functools.reduce(jnp.maximum, pieces), axis=1, keepdims=True)
        total = None
        for other in range(half):
            weights = jnp.exp2((pieces[other] - peak) * FACTOR)
            weight_ref[flip, :, other * block : (other + 1) * block] = weights.astype(jnp.bfloat16)
            total = weights if total is None else total + weights
        total_ref[flip] = jnp.sum(total, axis=1, keepdims=True)
        peak_ref[flip] = peak


def attend_low(half, flips, me_ref, *refs):
    weight_ref, total_ref, peak_ref = refs[:3]
    inner, out_refs = refs[3 : 3 + half], refs[3 + half : -1]
    values = refs[-1]
    block = values.shape[0] // half

    @pl.when(me_ref[0] < half)
    def _():
        for other in range(half):
            values[other * block : (other + 1) * block] = inner[other][2 * block : 3 * block]
        for flip, out_ref in zip(flips, out_refs):
            numerator = jnp.dot(weight_ref[flip], values[...], preferred_element_type=jnp.float32)
            total = total_ref[flip]
            out_ref[:block] = (numerator / total).astype(jnp.bfloat16)
            out_ref[block:] = pack_stat(peak_ref[flip] * FACTOR + jnp.log2(total))


def attend_up(half, flips, me_ref, *refs):
    o_low, o_up, stat_ref, num_ref, total_ref, peak_ref = refs[:6]
    weight_ref, far_total_ref, far_peak_ref = refs[6:9]
    cross_v, out_refs, values = refs[9 : 9 + half], refs[9 + half : -1], refs[-1]
    me = me_ref[0]
    block = o_low.shape[1]
    for flip, out_ref in zip(flips, out_refs):
        row_block = me % half ^ flip
        out_ref[:block] = o_low[row_block]
        out_ref[2 * block :] = stat_ref[row_block]

    @pl.when(me < half)
    def _():
        for flip, out_ref in zip(flips, out_refs):
            out_ref[block : 2 * block] = o_up[me % half ^ flip]

    @pl.when(me >= half)
    def _():
        for other in range(half):
            values[other * block : (other + 1) * block] = cross_v[other][...]
        for flip, out_ref in zip(flips, out_refs):
            row_block = me % half ^ flip
            numerator = jnp.dot(weight_ref[flip], values[...], preferred_element_type=jnp.float32)
            total, peak, own_peak = far_total_ref[flip], far_peak_ref[flip], peak_ref[row_block]
            joint = jnp.maximum(peak, own_peak)
            scale = jnp.exp2((peak - joint) * FACTOR)
            own_scale = jnp.exp2((own_peak - joint) * FACTOR)
            both = numerator * scale + num_ref[row_block] * own_scale
            both_total = total * scale + total_ref[row_block] * own_scale
            out_ref[block : 2 * block] = (both / both_total).astype(jnp.bfloat16)


def join_heads(half, me_ref, inner, across, joined):
    me = me_ref[0]
    low = me % half
    block = joined.shape[0]
    for flip in range(half):
        at = pl.multiple_of((low ^ flip) * HEAD_DIM, HEAD_DIM)
        up_at = pl.multiple_of((low ^ flip) * HEAD_DIM + half * HEAD_DIM, HEAD_DIM)
        joined[:, pl.ds(up_at, HEAD_DIM)] = inner[flip][block : 2 * block]

        @pl.when(me < half)
        def _():
            joined[:, pl.ds(at, HEAD_DIM)] = inner[flip][:block]

        @pl.when(me >= half)
        def _():
            share = share_column(inner[flip][2 * block :], across[flip][block:], block)
            mixed = inner[flip][:block].astype(jnp.float32) * share
            mixed = mixed + across[flip][:block].astype(jnp.float32) * (1.0 - share)
            joined[:, pl.ds(at, HEAD_DIM)] = mixed.astype(jnp.bfloat16)


def join_and_project(half, flip, me_ref, *refs):
    inner, across, (w_ref, out_ref, joined) = refs[:half], refs[half : 2 * half], refs[2 * half :]
    join_heads(half, me_ref, inner, across, joined)
    project(flip, me_ref, joined, w_ref, out_ref)


def project(flip, me_ref, joined, w_ref, out_ref):
    width = out_ref.shape[1]
    at = pl.multiple_of((me_ref[1] ^ flip) * width, width)
    out_ref[...] = jnp.dot(
        joined[...], w_ref[:, pl.ds(at, width)], preferred_element_type=jnp.float32
    ).astype(jnp.bfloat16)


def half_path(queries, keys_in, values_in, out_weight, spans, full_ids):
    n_seq = lax.axis_size("seq")
    half = n_seq // 2
    bf16, f32 = jnp.bfloat16, jnp.float32
    shape = jax.ShapeDtypeStruct
    where = jnp.stack([lax.axis_index("seq"), lax.axis_index("head")]).astype(jnp.int32)
    block = queries.shape[0]
    down = range(half - 1, -1, -1)
    piece = shape((block, HEAD_DIM), bf16)

    dealt = own_kernel(
        functools.partial(deal, half),
        [shape((6 * block, HEAD_DIM), bf16)] * half + [piece] * (2 * half),
        [SMEM] + [pl.BlockSpec(memory_space=pltpu.HBM)] * 3,
        [pltpu.SemaphoreType.DMA((8 * half,))],
    )(where, *[pltpu.with_memory_space_constraint(a, pltpu.HBM) for a in (queries, keys_in, values_in)])
    inner, cross, cross_v = dealt[:half], dealt[half : 2 * half], dealt[2 * half :]
    inner, cross, cross_v = list(inner), list(cross), list(cross_v)
    for flip in range(half - 1, 0, -1):
        inner[flip] = swap(inner[flip], "seq", flip)
    for flip in down:
        cross[flip] = swap(cross[flip], "seq", half + flip)
        cross_v[flip] = move(cross_v[flip], "seq", [(i, half + (i ^ flip)) for i in range(half)])
    w_held = held(out_weight)
    inner = [held(a) for a in inner]
    cross = [held(a) for a in cross]
    cross_v = [held(a) for a in cross_v]

    own = own_kernel(
        functools.partial(attend_own_half, half),
        [shape((half, block, HEAD_DIM), bf16)] * 2
        + [shape((half, STAT_ROWS, HEAD_DIM), bf16), shape((half, block, HEAD_DIM), f32)]
        + [shape((half, block, 1), f32)] * 2,
        [SMEM] + in_vmem(half),
        [pltpu.VMEM((6, half * block, HEAD_DIM), bf16)],
        flops=2 * 10**9,
    )(where, *inner)
    weights = own_kernel(
        functools.partial(weigh_across, half),
        [shape((half, block, half * block), bf16)] + [shape((half, block, 1), f32)] * 2,
        [SMEM] * 3 + in_vmem(2 * half),
        [pltpu.VMEM((half, block, HEAD_DIM), bf16)] * 2,
        flops=2 * 10**9,
    )(where, spans, full_ids, *inner, *cross)
    weights = [held(a) for a in weights]
    own = [held(a) for a in own]
    across, own_half = [None] * half, [None] * half
    pairs = [(flip, flip - 1) for flip in range(half - 1, 0, -2)]
    for flips in pairs:
        lows = own_kernel(
            functools.partial(attend_low, half, flips),
            [shape((block + STAT_ROWS, HEAD_DIM), bf16)] * len(flips),
            [SMEM] + in_vmem(3 + half),
            [pltpu.VMEM((half * block, HEAD_DIM), bf16)],
            flops=5 * 10**8,
        )(where, *weights, *inner)
        for flip, low in zip(flips, lows):
            across[flip] = move(low, "seq", [(i, half + (i ^ flip)) for i in range(half)])
    for flips in pairs:
        ups = own_kernel(
            functools.partial(attend_up, half, flips),
            [shape((2 * block + STAT_ROWS, HEAD_DIM), bf16)] * len(flips),
            [SMEM] + in_vmem(9 + half),
            [pltpu.VMEM((half * block, HEAD_DIM), bf16)],
            flops=5 * 10**8,
        )(where, *own, *weights, *cross_v)
        for flip, up in zip(flips, ups):
            own_half[flip] = swap(up, "seq", flip) if flip else up
    came = [held(a) for a in own_half + across]
    width = out_weight.shape[1] // lax.axis_size("head")
    part = shape((block, width), bf16)
    sent, joined = own_kernel(
        functools.partial(join_and_project, half, 3),
        [part, shape((block, n_seq * HEAD_DIM), bf16)],
        [SMEM] + in_vmem(2 * half + 1),
        flops=10**9,
    )(where, *came, w_held)

    def columns_of(flip, rows):
        return own_kernel(
            functools.partial(project, flip), [part], [SMEM] + in_vmem(2), flops=10**9
        )(where, held(rows), w_held)[0]

    def summed(one, other):
        return (one.astype(f32) + other.astype(f32)).astype(bf16)

    far = summed(swap(sent, "head", 1), columns_of(2, joined))
    rows, far = lax.optimization_barrier((joined, far))
    far = swap(far, "head", 2)
    near = columns_of(1, rows)
    near = summed(swap(near, "head", 1), columns_of(0, rows))
    return summed(near, far)


def on_device(queries, keys_in, values_in, out_weight, spans, full_ids):
    n_seq, n_head = lax.axis_size("seq"), lax.axis_size("head")
    block = queries.shape[0]
    one_head_each = queries.shape[1] == n_seq * HEAD_DIM
    if one_head_each and n_head == 4 and n_seq == 8 and block == 256:
        return half_path(queries, keys_in, values_in, out_weight, spans, full_ids)
    return ring_path(queries, keys_in, values_in, out_weight, spans, full_ids)


def solution(mesh):
    placed = (
        P("seq", "head"),
        P("seq", "head"),
        P("seq", "head"),
        P("head", None),
        P("head"),
        P("head"),
    )
    return jax.shard_map(
        on_device, mesh=mesh, in_specs=placed, out_specs=P("seq", "head"), check_vma=False
    )
```

```python
import math

import functools

import jax
import jax.numpy as jnp
from jax import lax
from jax.experimental import pallas as pl
from jax.experimental.pallas import tpu as pltpu
from jax.sharding import PartitionSpec as P

HEAD_DIM = 128
SPAN_MAX = 4096


NEG_FILL = -1e30


def from_behind(block, axis, distance):
    devices = range(lax.axis_size(axis))
    route = [(i - distance, i) for i in devices if i - distance in devices]
    return lax.ppermute(block, axis, route)


def online_update(carry_state, scores, allowed, value_rows):
    old_peak, row_total, numerator = carry_state
    masked = jnp.where(allowed, scores, NEG_FILL)
    new_peak = jnp.maximum(old_peak, jnp.max(masked, axis=-1))
    weights = jnp.where(allowed, jnp.exp(masked - new_peak[..., None]), 0.0)
    rescale = jnp.exp(old_peak - new_peak)
    row_total = row_total * rescale + jnp.sum(weights, axis=-1)
    numerator = numerator * rescale[..., None] + jnp.einsum(
        "hqk,hkd->hqd", weights.astype(jnp.bfloat16), value_rows, preferred_element_type=jnp.float32
    )
    return (new_peak, row_total, numerator)


def empty_state(lead_count, row_count, head_width):
    return (
        jnp.full((lead_count, row_count), NEG_FILL, jnp.float32),
        jnp.zeros((lead_count, row_count), jnp.float32),
        jnp.zeros((lead_count, row_count, head_width), jnp.float32),
    )


def finish(carry_state):
    return (carry_state[2] / carry_state[1][..., None]).astype(jnp.bfloat16)


def ring_path(queries, keys_in, values_in, out_weight, spans, full_ids):
    score_scale = HEAD_DIM ** (-0.5)
    n_seq = lax.axis_size("seq")
    seq_index = lax.axis_index("seq")
    tok_rows = queries.shape[0]
    group_heads = queries.shape[1] // HEAD_DIM
    full_count = full_ids.shape[0]
    band_count = group_heads - full_count
    head_base = lax.axis_index("head") * group_heads
    local_range = jnp.arange(group_heads)
    marks = jnp.sum(
        (local_range[:, None] + head_base == full_ids[None, :]).astype(jnp.int32), axis=1
    )
    order_local = jnp.argsort(marks * group_heads + local_range)
    band_local = order_local[:band_count]
    full_local = order_local[band_count:]
    query_three = queries.reshape(tok_rows, group_heads, HEAD_DIM)
    key_three = keys_in.reshape(tok_rows, group_heads, HEAD_DIM)
    value_three = values_in.reshape(tok_rows, group_heads, HEAD_DIM)
    query_band = jnp.take(query_three, band_local, axis=1).transpose(1, 0, 2)
    kv_band = jnp.stack(
        [
            jnp.take(key_three, band_local, axis=1).transpose(1, 0, 2),
            jnp.take(value_three, band_local, axis=1).transpose(1, 0, 2),
        ]
    )
    band_reach = jnp.take(spans, band_local)
    query_pos = seq_index * tok_rows + jnp.arange(tok_rows)
    hop_count = min(max(1, SPAN_MAX // tok_rows), n_seq - 1)
    arrived = [(kv_band, 0)]
    moving = kv_band
    for distance in range(1, hop_count + 1):
        moving = from_behind(moving, "seq", 1)
        arrived.append((moving, distance))
    batch_size = max(1, 512 // tok_rows)
    band_state = empty_state(band_count, tok_rows, HEAD_DIM)
    for first_piece in range(0, len(arrived), batch_size):
        batch_pieces = arrived[first_piece : first_piece + batch_size]
        key_rows = jnp.concatenate([arrival[0][0] for arrival in batch_pieces], axis=1)
        value_rows = jnp.concatenate([arrival[0][1] for arrival in batch_pieces], axis=1)
        key_pos = jnp.concatenate(
            [(seq_index - arrival[1]) * tok_rows + jnp.arange(tok_rows) for arrival in batch_pieces]
        )
        scores = (
            jnp.einsum("hqd,hkd->hqk", query_band, key_rows, preferred_element_type=jnp.float32)
            * score_scale
        )
        gap_size = query_pos[None, :, None] - key_pos[None, None, :]
        allowed = (
            (gap_size >= 0) & (gap_size < band_reach[:, None, None]) & (key_pos >= 0)[None, None, :]
        )
        band_state = online_update(band_state, scores, allowed, value_rows)
    band_out = finish(band_state)
    query_full = jnp.take(query_three, full_local, axis=1).transpose(1, 0, 2)
    key_full = jnp.take(key_three, full_local, axis=1).transpose(1, 0, 2)
    value_full = jnp.take(value_three, full_local, axis=1).transpose(1, 0, 2)
    kv_full = jnp.stack([key_full, value_full])
    last_query = seq_index * tok_rows + tok_rows - 1
    key_piece = lax.all_gather(kv_full, "seq", axis=2, tiled=True)
    row_count = key_piece.shape[2]
    tile_rows = math.gcd(row_count, 512)

    def absorb_tile(tile_index, inner_state):
        key_tile = lax.dynamic_slice_in_dim(key_piece[0], tile_index * tile_rows, tile_rows, 1)
        value_tile = lax.dynamic_slice_in_dim(key_piece[1], tile_index * tile_rows, tile_rows, 1)
        key_pos = tile_index * tile_rows + jnp.arange(tile_rows)
        scores = (
            jnp.einsum("hqd,hkd->hqk", query_full, key_tile, preferred_element_type=jnp.float32)
            * score_scale
        )
        allowed = key_pos[None, None, :] <= query_pos[None, :, None]
        return online_update(inner_state, scores, allowed, value_tile)

    live_tiles = jnp.clip(last_query // tile_rows + 1, 0, row_count // tile_rows)
    full_state = lax.fori_loop(
        0, live_tiles, absorb_tile, empty_state(full_count, tok_rows, HEAD_DIM)
    )
    full_out = finish(full_state)
    combined = jnp.concatenate([band_out, full_out], axis=0)
    inverse = jnp.argsort(order_local)
    per_head = jnp.take(combined, inverse, axis=0)
    attended = per_head.transpose(1, 0, 2).reshape(tok_rows, group_heads * HEAD_DIM)
    projected = jnp.dot(attended, out_weight, preferred_element_type=jnp.float32)
    return lax.psum_scatter(projected.astype(jnp.bfloat16), "head", scatter_dimension=1, tiled=True)


def move(block, axis, pairs):
    return lax.ppermute(block, axis, pairs)


def swap(block, axis, flip):
    return move(block, axis, [(i, i ^ flip) for i in range(lax.axis_size(axis))])


def in_vmem(count):
    return [pl.BlockSpec(memory_space=pltpu.VMEM)] * count


def held(array):
    return pltpu.with_memory_space_constraint(array, pltpu.VMEM)


SMEM = pl.BlockSpec(memory_space=pltpu.SMEM)
FACTOR = HEAD_DIM**-0.5 * math.log2(math.e)
STAT_ROWS = 16


def own_kernel(body, out_shapes, in_specs, scratch=(), flops=10**8, limit=20 * 2**20):
    return pl.pallas_call(
        body,
        out_shape=out_shapes,
        in_specs=in_specs,
        out_specs=in_vmem(len(out_shapes)),
        scratch_shapes=list(scratch),
        compiler_params=pltpu.CompilerParams(vmem_limit_bytes=limit),
        cost_estimate=pl.CostEstimate(flops=flops, bytes_accessed=10**6, transcendentals=0),
    )


def deal(half, upper, me_ref, q_ref, k_ref, v_ref, *refs):
    inner, cross, sems = refs[:half], refs[half : 2 * half], refs[2 * half]
    me = me_ref[0]
    low = me % half
    rows = q_ref.shape[0]
    waits = []

    def fetch(source, head, out_ref, place):
        at = pl.multiple_of(head * HEAD_DIM, HEAD_DIM)
        return pltpu.make_async_copy(
            source.at[:, pl.ds(at, HEAD_DIM)],
            out_ref.at[pl.ds(place * rows, rows)],
            sems.at[len(waits)],
        )

    for flip in range(half - 1, -1, -1):
        for place, source in enumerate((q_ref, k_ref, v_ref)):
            copy = fetch(source, (low ^ flip) + upper * half, inner[flip], place)
            copy.start()
            waits.append(copy)
    for flip in range(half - 1, -1, -1):
        target = low ^ flip
        if upper:
            copy = fetch(v_ref, target + half, cross[flip], 0)
            copy.start()
        else:
            below = fetch(k_ref, target + half, cross[flip], 0)
            copy = fetch(q_ref, target, cross[flip], 0)
            pl.when(me < half)(below.start)
            pl.when(me >= half)(copy.start)
        waits.append(copy)
    for copy in waits:
        copy.wait()


def square_eye(size):
    row = lax.broadcasted_iota(jnp.int32, (size, size), 0)
    return row == lax.broadcasted_iota(jnp.int32, (size, size), 1)


def pack_stat(stat):
    eye = square_eye(HEAD_DIM)
    rows = []
    for first in range(0, stat.shape[0], HEAD_DIM):
        piece = jnp.where(eye, stat[first : first + HEAD_DIM], 0.0)
        left = jnp.sum(piece, axis=0, keepdims=True)
        for _ in range(3):
            part = left.astype(jnp.bfloat16).astype(jnp.float32)
            rows.append(part)
            left = left - part
    rows.append(jnp.zeros((STAT_ROWS - len(rows), HEAD_DIM), jnp.float32))
    return jnp.concatenate(rows, axis=0).astype(jnp.bfloat16)


def share_column(here, there, size):
    eye = square_eye(HEAD_DIM)
    apart = there.astype(jnp.float32) - here.astype(jnp.float32)
    columns = []
    for index in range(size // HEAD_DIM):
        row = apart[3 * index : 3 * index + 1]
        for more in (1, 2):
            row = row + apart[3 * index + more : 3 * index + more + 1]
        share = 1.0 / (1.0 + jnp.exp2(row))
        columns.append(jnp.sum(jnp.where(eye, share, 0.0), axis=1, keepdims=True))
    return jnp.concatenate(columns, axis=0)


def softmax_rows(pieces, value_tiles):
    peak = jnp.max(functools.reduce(jnp.maximum, pieces), axis=1, keepdims=True)
    total, numerator = None, None
    for scores, value_tile in zip(pieces, value_tiles):
        weights = jnp.exp2((scores - peak) * FACTOR)
        total = weights if total is None else total + weights
        product = jnp.dot(
            weights.astype(jnp.bfloat16), value_tile, preferred_element_type=jnp.float32
        )
        numerator = product if numerator is None else numerator + product
    return numerator, jnp.sum(total, axis=1, keepdims=True), peak


def score_tile(q_tile, k_tile):
    return lax.dot_general(
        q_tile, k_tile, (((1,), (1,)), ((), ())), preferred_element_type=jnp.float32
    )


def attend_own_half(half, upper, me_ref, *refs):
    inner, (out_ref, *state_refs, qkv) = refs[:half], refs[half:]
    low = me_ref[0] % half
    block = out_ref.shape[1]
    for flip in range(half):
        at = pl.multiple_of((low ^ flip) * block, block)
        for place in range(3):
            qkv[place, pl.ds(at, block)] = inner[flip][place * block : (place + 1) * block]
    row = lax.broadcasted_iota(jnp.int32, (block, block), 0)
    causal = row >= lax.broadcasted_iota(jnp.int32, (block, block), 1)
    for i in range(half):
        q_tile = qkv[0, i * block : (i + 1) * block]
        pieces, value_tiles = [], []
        for j in range(i + 1):
            scores = score_tile(q_tile, qkv[1, j * block : (j + 1) * block])
            pieces.append(jnp.where(causal, scores, NEG_FILL) if i == j else scores)
            value_tiles.append(qkv[2, j * block : (j + 1) * block])
        numerator, total, peak = softmax_rows(pieces, value_tiles)
        out_ref[i] = (numerator / total).astype(jnp.bfloat16)
        if upper:
            for state_ref, value in zip(state_refs, (numerator, total, peak)):
                state_ref[i] = value
        else:
            state_refs[0][i] = pack_stat(peak * FACTOR + jnp.log2(total))


def weigh_across(half, upper, me_ref, spans_ref, full_ref, *refs):
    inner, cross = refs[:half], refs[half : 2 * half]
    weight_ref, total_ref, peak_ref = refs[2 * half :]
    me, head = me_ref[0], me_ref[1]
    low = me % half
    block = cross[0].shape[0]

    @pl.when(me >= half if upper else me < half)
    def _():
        local = low + upper * half
        reach = spans_ref[local]
        for place in range(full_ref.shape[0]):
            reach = jnp.where(full_ref[place] == head * 2 * half + local, 2 * half * block, reach)
        row = lax.broadcasted_iota(jnp.int32, (block, block), 0)
        gap = row - lax.broadcasted_iota(jnp.int32, (block, block), 1)
        for flip in range(half):
            q_tile = inner[flip][:block] if upper else cross[flip][...]
            pieces = []
            for other in range(half):
                k_tile = cross[other][...] if upper else inner[other][block : 2 * block]
                offset = (half + (low ^ flip) - (low ^ other)) * block
                scores = score_tile(q_tile, k_tile)
                pieces.append(jnp.where(gap < reach - offset, scores, NEG_FILL))
            peak = jnp.max(functools.reduce(jnp.maximum, pieces), axis=1, keepdims=True)
            total = None
            for other in range(half):
                weights = jnp.exp2((pieces[other] - peak) * FACTOR)
                weight_ref[flip, :, other * block : (other + 1) * block] = weights.astype(
                    jnp.bfloat16
                )
                total = weights if total is None else total + weights
            total_ref[flip] = jnp.sum(total, axis=1, keepdims=True)
            peak_ref[flip] = peak


def attend_low(half, flips, me_ref, *refs):
    weight_ref, total_ref, peak_ref = refs[:3]
    inner, out_refs = refs[3 : 3 + half], refs[3 + half : -1]
    values = refs[-1]
    block = values.shape[0] // half

    @pl.when(me_ref[0] < half)
    def _():
        for other in range(half):
            values[other * block : (other + 1) * block] = inner[other][2 * block : 3 * block]
        for flip, out_ref in zip(flips, out_refs):
            numerator = jnp.dot(weight_ref[flip], values[...], preferred_element_type=jnp.float32)
            total = total_ref[flip]
            out_ref[:block] = (numerator / total).astype(jnp.bfloat16)
            out_ref[block:] = pack_stat(peak_ref[flip] * FACTOR + jnp.log2(total))


def attend_up(half, flips, me_ref, *refs):
    o_low, stat_ref, o_up, num_ref, total_ref, peak_ref = refs[:6]
    weight_ref, far_total_ref, far_peak_ref = refs[6:9]
    cross_v, out_refs, values = refs[9 : 9 + half], refs[9 + half : -1], refs[-1]
    me = me_ref[0]
    block = o_low.shape[1]
    for flip, out_ref in zip(flips, out_refs):
        row_block = me % half ^ flip
        out_ref[:block] = o_low[row_block]
        out_ref[2 * block :] = stat_ref[row_block]

    @pl.when(me < half)
    def _():
        for flip, out_ref in zip(flips, out_refs):
            out_ref[block : 2 * block] = o_up[me % half ^ flip]

    @pl.when(me >= half)
    def _():
        for other in range(half):
            values[other * block : (other + 1) * block] = cross_v[other][...]
        for flip, out_ref in zip(flips, out_refs):
            row_block = me % half ^ flip
            numerator = jnp.dot(weight_ref[flip], values[...], preferred_element_type=jnp.float32)
            total, peak, own_peak = far_total_ref[flip], far_peak_ref[flip], peak_ref[row_block]
            joint = jnp.maximum(peak, own_peak)
            scale = jnp.exp2((peak - joint) * FACTOR)
            own_scale = jnp.exp2((own_peak - joint) * FACTOR)
            both = numerator * scale + num_ref[row_block] * own_scale
            both_total = total * scale + total_ref[row_block] * own_scale
            out_ref[block : 2 * block] = (both / both_total).astype(jnp.bfloat16)


def join_heads(half, me_ref, inner, across, joined):
    me = me_ref[0]
    low = me % half
    block = joined.shape[0]
    for flip in range(half):
        at = pl.multiple_of((low ^ flip) * HEAD_DIM, HEAD_DIM)
        up_at = pl.multiple_of((low ^ flip) * HEAD_DIM + half * HEAD_DIM, HEAD_DIM)
        joined[:, pl.ds(up_at, HEAD_DIM)] = inner[flip][block : 2 * block]

        @pl.when(me < half)
        def _():
            joined[:, pl.ds(at, HEAD_DIM)] = inner[flip][:block]

        @pl.when(me >= half)
        def _():
            share = share_column(inner[flip][2 * block :], across[flip][block:], block)
            mixed = inner[flip][:block].astype(jnp.float32) * share
            mixed = mixed + across[flip][:block].astype(jnp.float32) * (1.0 - share)
            joined[:, pl.ds(at, HEAD_DIM)] = mixed.astype(jnp.bfloat16)


def join_and_project(half, flip, me_ref, *refs):
    inner, across, (w_ref, out_ref, joined) = refs[:half], refs[half : 2 * half], refs[2 * half :]
    join_heads(half, me_ref, inner, across, joined)
    project(flip, me_ref, joined, w_ref, out_ref)


def project(flip, me_ref, joined, w_ref, out_ref):
    width = out_ref.shape[1]
    at = pl.multiple_of((me_ref[1] ^ flip) * width, width)
    out_ref[...] = jnp.dot(
        joined[...], w_ref[:, pl.ds(at, width)], preferred_element_type=jnp.float32
    ).astype(jnp.bfloat16)


def half_path(queries, keys_in, values_in, out_weight, spans, full_ids):
    n_seq = lax.axis_size("seq")
    half = n_seq // 2
    bf16, f32 = jnp.bfloat16, jnp.float32
    shape = jax.ShapeDtypeStruct
    where = jnp.stack([lax.axis_index("seq"), lax.axis_index("head")]).astype(jnp.int32)
    block = queries.shape[0]
    down = range(half - 1, -1, -1)
    piece = shape((block, HEAD_DIM), bf16)

    hbm = pl.BlockSpec(memory_space=pltpu.HBM)
    ours = [pltpu.with_memory_space_constraint(a, pltpu.HBM) for a in (queries, keys_in, values_in)]
    inner, cross = [], []
    for upper in range(2):
        dealt = own_kernel(
            functools.partial(deal, half, upper),
            [shape((3 * block, HEAD_DIM), bf16)] * half + [piece] * half,
            [SMEM] + [hbm] * 3,
            [pltpu.SemaphoreType.DMA((4 * half,))],
        )(where, *ours)
        inner.append(list(dealt[:half]))
        cross.append(list(dealt[half:]))
        for flip in range(half - 1, 0, -1):
            inner[upper][flip] = swap(inner[upper][flip], "seq", flip)
        for flip in down:
            pairs = [(i, i ^ half ^ flip) for i in range(half if upper else n_seq)]
            cross[upper][flip] = move(cross[upper][flip], "seq", pairs)
    w_held = held(out_weight)
    inner = [[held(a) for a in arrays] for arrays in inner]
    cross_qk, cross_v = [[held(a) for a in arrays] for arrays in cross]

    column = shape((half, block, 1), f32)
    own, weights = [], []
    for upper in range(2):
        states = [shape((half, STAT_ROWS, HEAD_DIM), bf16)]
        if upper:
            states = [shape((half, block, HEAD_DIM), f32), column, column]
        parts = own_kernel(
            functools.partial(attend_own_half, half, upper),
            [shape((half, block, HEAD_DIM), bf16)] + states,
            [SMEM] + in_vmem(half),
            [pltpu.VMEM((3, half * block, HEAD_DIM), bf16)],
            flops=10**9,
        )(where, *inner[upper])
        own += [held(a) for a in parts]
        parts = own_kernel(
            functools.partial(weigh_across, half, upper),
            [shape((half, block, half * block), bf16), column, column],
            [SMEM] * 3 + in_vmem(2 * half),
            flops=10**9,
        )(where, spans, full_ids, *inner[upper], *cross_qk)
        weights.append([held(a) for a in parts])
    across, own_half = [None] * half, [None] * half
    pairs = [(flip, flip - 1) for flip in range(half - 1, 0, -2)]
    for flips in pairs:
        lows = own_kernel(
            functools.partial(attend_low, half, flips),
            [shape((block + STAT_ROWS, HEAD_DIM), bf16)] * len(flips),
            [SMEM] + in_vmem(3 + half),
            [pltpu.VMEM((half * block, HEAD_DIM), bf16)],
            flops=5 * 10**8,
        )(where, *weights[0], *inner[0])
        for flip, low in zip(flips, lows):
            across[flip] = move(low, "seq", [(i, half + (i ^ flip)) for i in range(half)])
    for flips in pairs:
        ups = own_kernel(
            functools.partial(attend_up, half, flips),
            [shape((2 * block + STAT_ROWS, HEAD_DIM), bf16)] * len(flips),
            [SMEM] + in_vmem(9 + half),
            [pltpu.VMEM((half * block, HEAD_DIM), bf16)],
            flops=5 * 10**8,
        )(where, *own, *weights[1], *cross_v)
        for flip, up in zip(flips, ups):
            own_half[flip] = swap(up, "seq", flip) if flip else up
    came = [held(a) for a in own_half + across]
    width = out_weight.shape[1] // lax.axis_size("head")
    part = shape((block, width), bf16)
    sent, joined = own_kernel(
        functools.partial(join_and_project, half, 3),
        [part, shape((block, n_seq * HEAD_DIM), bf16)],
        [SMEM] + in_vmem(2 * half + 1),
        flops=10**9,
    )(where, *came, w_held)

    def columns_of(flip, rows):
        return own_kernel(
            functools.partial(project, flip), [part], [SMEM] + in_vmem(2), flops=10**9
        )(where, held(rows), w_held)[0]

    def summed(one, other):
        return (one.astype(f32) + other.astype(f32)).astype(bf16)

    far = summed(swap(sent, "head", 1), columns_of(2, joined))
    rows, far = lax.optimization_barrier((joined, far))
    far = swap(far, "head", 2)
    near = columns_of(1, rows)
    near = summed(swap(near, "head", 1), columns_of(0, rows))
    return summed(near, far)


def on_device(queries, keys_in, values_in, out_weight, spans, full_ids):
    n_seq, n_head = lax.axis_size("seq"), lax.axis_size("head")
    block = queries.shape[0]
    one_head_each = queries.shape[1] == n_seq * HEAD_DIM
    if one_head_each and n_head == 4 and n_seq == 8 and block == 256:
        return half_path(queries, keys_in, values_in, out_weight, spans, full_ids)
    return ring_path(queries, keys_in, values_in, out_weight, spans, full_ids)


def solution(mesh):
    placed = (
        P("seq", "head"),
        P("seq", "head"),
        P("seq", "head"),
        P("head", None),
        P("head"),
        P("head"),
    )
    return jax.shard_map(
        on_device, mesh=mesh, in_specs=placed, out_specs=P("seq", "head"), check_vma=False
    )
```

```python
import math

import functools

import jax
import jax.numpy as jnp
from jax import lax
from jax.experimental import pallas as pl
from jax.experimental.pallas import tpu as pltpu
from jax.sharding import PartitionSpec as P

HEAD_DIM = 128
SPAN_MAX = 4096


NEG_FILL = -1e30


def from_behind(block, axis, distance):
    devices = range(lax.axis_size(axis))
    route = [(i - distance, i) for i in devices if i - distance in devices]
    return lax.ppermute(block, axis, route)


def online_update(carry_state, scores, allowed, value_rows):
    old_peak, row_total, numerator = carry_state
    masked = jnp.where(allowed, scores, NEG_FILL)
    new_peak = jnp.maximum(old_peak, jnp.max(masked, axis=-1))
    weights = jnp.where(allowed, jnp.exp(masked - new_peak[..., None]), 0.0)
    rescale = jnp.exp(old_peak - new_peak)
    row_total = row_total * rescale + jnp.sum(weights, axis=-1)
    numerator = numerator * rescale[..., None] + jnp.einsum(
        "hqk,hkd->hqd", weights.astype(jnp.bfloat16), value_rows, preferred_element_type=jnp.float32
    )
    return (new_peak, row_total, numerator)


def empty_state(lead_count, row_count, head_width):
    return (
        jnp.full((lead_count, row_count), NEG_FILL, jnp.float32),
        jnp.zeros((lead_count, row_count), jnp.float32),
        jnp.zeros((lead_count, row_count, head_width), jnp.float32),
    )


def finish(carry_state):
    return (carry_state[2] / carry_state[1][..., None]).astype(jnp.bfloat16)


def ring_path(queries, keys_in, values_in, out_weight, spans, full_ids):
    score_scale = HEAD_DIM ** (-0.5)
    n_seq = lax.axis_size("seq")
    seq_index = lax.axis_index("seq")
    tok_rows = queries.shape[0]
    group_heads = queries.shape[1] // HEAD_DIM
    full_count = full_ids.shape[0]
    band_count = group_heads - full_count
    head_base = lax.axis_index("head") * group_heads
    local_range = jnp.arange(group_heads)
    marks = jnp.sum(
        (local_range[:, None] + head_base == full_ids[None, :]).astype(jnp.int32), axis=1
    )
    order_local = jnp.argsort(marks * group_heads + local_range)
    band_local = order_local[:band_count]
    full_local = order_local[band_count:]
    query_three = queries.reshape(tok_rows, group_heads, HEAD_DIM)
    key_three = keys_in.reshape(tok_rows, group_heads, HEAD_DIM)
    value_three = values_in.reshape(tok_rows, group_heads, HEAD_DIM)
    query_band = jnp.take(query_three, band_local, axis=1).transpose(1, 0, 2)
    kv_band = jnp.stack(
        [
            jnp.take(key_three, band_local, axis=1).transpose(1, 0, 2),
            jnp.take(value_three, band_local, axis=1).transpose(1, 0, 2),
        ]
    )
    band_reach = jnp.take(spans, band_local)
    query_pos = seq_index * tok_rows + jnp.arange(tok_rows)
    hop_count = min(max(1, SPAN_MAX // tok_rows), n_seq - 1)
    arrived = [(kv_band, 0)]
    moving = kv_band
    for distance in range(1, hop_count + 1):
        moving = from_behind(moving, "seq", 1)
        arrived.append((moving, distance))
    batch_size = max(1, 512 // tok_rows)
    band_state = empty_state(band_count, tok_rows, HEAD_DIM)
    for first_piece in range(0, len(arrived), batch_size):
        batch_pieces = arrived[first_piece : first_piece + batch_size]
        key_rows = jnp.concatenate([arrival[0][0] for arrival in batch_pieces], axis=1)
        value_rows = jnp.concatenate([arrival[0][1] for arrival in batch_pieces], axis=1)
        key_pos = jnp.concatenate(
            [(seq_index - arrival[1]) * tok_rows + jnp.arange(tok_rows) for arrival in batch_pieces]
        )
        scores = (
            jnp.einsum("hqd,hkd->hqk", query_band, key_rows, preferred_element_type=jnp.float32)
            * score_scale
        )
        gap_size = query_pos[None, :, None] - key_pos[None, None, :]
        allowed = (
            (gap_size >= 0) & (gap_size < band_reach[:, None, None]) & (key_pos >= 0)[None, None, :]
        )
        band_state = online_update(band_state, scores, allowed, value_rows)
    band_out = finish(band_state)
    query_full = jnp.take(query_three, full_local, axis=1).transpose(1, 0, 2)
    key_full = jnp.take(key_three, full_local, axis=1).transpose(1, 0, 2)
    value_full = jnp.take(value_three, full_local, axis=1).transpose(1, 0, 2)
    kv_full = jnp.stack([key_full, value_full])
    last_query = seq_index * tok_rows + tok_rows - 1
    key_piece = lax.all_gather(kv_full, "seq", axis=2, tiled=True)
    row_count = key_piece.shape[2]
    tile_rows = math.gcd(row_count, 512)

    def absorb_tile(tile_index, inner_state):
        key_tile = lax.dynamic_slice_in_dim(key_piece[0], tile_index * tile_rows, tile_rows, 1)
        value_tile = lax.dynamic_slice_in_dim(key_piece[1], tile_index * tile_rows, tile_rows, 1)
        key_pos = tile_index * tile_rows + jnp.arange(tile_rows)
        scores = (
            jnp.einsum("hqd,hkd->hqk", query_full, key_tile, preferred_element_type=jnp.float32)
            * score_scale
        )
        allowed = key_pos[None, None, :] <= query_pos[None, :, None]
        return online_update(inner_state, scores, allowed, value_tile)

    live_tiles = jnp.clip(last_query // tile_rows + 1, 0, row_count // tile_rows)
    full_state = lax.fori_loop(
        0, live_tiles, absorb_tile, empty_state(full_count, tok_rows, HEAD_DIM)
    )
    full_out = finish(full_state)
    combined = jnp.concatenate([band_out, full_out], axis=0)
    inverse = jnp.argsort(order_local)
    per_head = jnp.take(combined, inverse, axis=0)
    attended = per_head.transpose(1, 0, 2).reshape(tok_rows, group_heads * HEAD_DIM)
    projected = jnp.dot(attended, out_weight, preferred_element_type=jnp.float32)
    return lax.psum_scatter(projected.astype(jnp.bfloat16), "head", scatter_dimension=1, tiled=True)


def move(block, axis, pairs):
    return lax.ppermute(block, axis, pairs)


def swap(block, axis, flip):
    return move(block, axis, [(i, i ^ flip) for i in range(lax.axis_size(axis))])


def in_vmem(count):
    return [pl.BlockSpec(memory_space=pltpu.VMEM)] * count


def held(array):
    return pltpu.with_memory_space_constraint(array, pltpu.VMEM)


SMEM = pl.BlockSpec(memory_space=pltpu.SMEM)
FACTOR = HEAD_DIM**-0.5 * math.log2(math.e)
STAT_ROWS = 16


def own_kernel(body, out_shapes, in_specs, scratch=(), flops=10**8, limit=20 * 2**20):
    return pl.pallas_call(
        body,
        out_shape=out_shapes,
        in_specs=in_specs,
        out_specs=in_vmem(len(out_shapes)),
        scratch_shapes=list(scratch),
        compiler_params=pltpu.CompilerParams(vmem_limit_bytes=limit),
        cost_estimate=pl.CostEstimate(flops=flops, bytes_accessed=10**6, transcendentals=0),
    )


def deal(half, me_ref, spans_ref, full_ref, q_ref, k_ref, v_ref, *refs):
    reach_ref, sems, spans, full_ids = refs[4 * half :]
    me = me_ref[0]
    low = me % half
    tables = [
        pltpu.make_async_copy(spans_ref, spans, sems.at[8 * half]),
        pltpu.make_async_copy(full_ref, full_ids, sems.at[8 * half + 1]),
    ]
    for copy in tables:
        copy.start()
    rows = q_ref.shape[0]
    waits = []

    def fetch(source, head, out_ref, place):
        at = pl.multiple_of(head * HEAD_DIM, HEAD_DIM)
        return pltpu.make_async_copy(
            source.at[:, pl.ds(at, HEAD_DIM)],
            out_ref.at[pl.ds(place * rows, rows)],
            sems.at[len(waits)],
        )

    for upper in range(2):
        inner = refs[2 * upper * half : (2 * upper + 1) * half]
        cross = refs[(2 * upper + 1) * half : (2 * upper + 2) * half]
        for flip in range(half - 1, -1, -1):
            for place, source in enumerate((q_ref, k_ref, v_ref)):
                copy = fetch(source, (low ^ flip) + upper * half, inner[flip], place)
                copy.start()
                waits.append(copy)
        for flip in range(half - 1, -1, -1):
            target = low ^ flip
            if upper:
                copy = fetch(v_ref, target + half, cross[flip], 0)
                copy.start()
            else:
                below = fetch(k_ref, target + half, cross[flip], 0)
                copy = fetch(q_ref, target, cross[flip], 0)
                pl.when(me < half)(below.start)
                pl.when(me >= half)(copy.start)
            waits.append(copy)
    for copy in tables:
        copy.wait()
    for upper in range(2):
        local = low + upper * half
        reach = spans[local]
        for place in range(full_ids.shape[0]):
            is_full = full_ids[place] == me_ref[1] * 2 * half + local
            reach = jnp.where(is_full, 2 * half * rows, reach)
        reach_ref[upper : upper + 1] = jnp.full((1, reach_ref.shape[1]), reach, jnp.int32)
    for copy in waits:
        copy.wait()


def square_eye(size):
    row = lax.broadcasted_iota(jnp.int32, (size, size), 0)
    return row == lax.broadcasted_iota(jnp.int32, (size, size), 1)


def pack_stat(stat):
    eye = square_eye(HEAD_DIM)
    rows = []
    for first in range(0, stat.shape[0], HEAD_DIM):
        piece = jnp.where(eye, stat[first : first + HEAD_DIM], 0.0)
        left = jnp.sum(piece, axis=0, keepdims=True)
        for _ in range(3):
            part = left.astype(jnp.bfloat16).astype(jnp.float32)
            rows.append(part)
            left = left - part
    rows.append(jnp.zeros((STAT_ROWS - len(rows), HEAD_DIM), jnp.float32))
    return jnp.concatenate(rows, axis=0).astype(jnp.bfloat16)


def share_column(here, there, size):
    eye = square_eye(HEAD_DIM)
    apart = there.astype(jnp.float32) - here.astype(jnp.float32)
    columns = []
    for index in range(size // HEAD_DIM):
        row = apart[3 * index : 3 * index + 1]
        for more in (1, 2):
            row = row + apart[3 * index + more : 3 * index + more + 1]
        share = 1.0 / (1.0 + jnp.exp2(row))
        columns.append(jnp.sum(jnp.where(eye, share, 0.0), axis=1, keepdims=True))
    return jnp.concatenate(columns, axis=0)


def softmax_rows(pieces, value_tiles):
    peak = jnp.max(functools.reduce(jnp.maximum, pieces), axis=1, keepdims=True)
    total, numerator = None, None
    for scores, value_tile in zip(pieces, value_tiles):
        weights = jnp.exp2((scores - peak) * FACTOR)
        total = weights if total is None else total + weights
        product = jnp.dot(
            weights.astype(jnp.bfloat16), value_tile, preferred_element_type=jnp.float32
        )
        numerator = product if numerator is None else numerator + product
    return numerator, jnp.sum(total, axis=1, keepdims=True), peak


def score_tile(q_tile, k_tile):
    return lax.dot_general(
        q_tile, k_tile, (((1,), (1,)), ((), ())), preferred_element_type=jnp.float32
    )


def gaps(block):
    row = lax.broadcasted_iota(jnp.int32, (block, block), 0)
    return row - lax.broadcasted_iota(jnp.int32, (block, block), 1)


def attend_low(half, me_ref, reach_ref, *refs):
    inner, cross, out_refs = refs[:half], refs[half : 2 * half], refs[2 * half :]
    block = cross[0].shape[0]

    @pl.when(me_ref[0] < half)
    def _():
        low = me_ref[0]
        reach = reach_ref[0:1]
        gap = gaps(block)
        for flip in range(half - 1, -1, -1):
            pieces = []
            for other in range(half):
                offset = (half + (low ^ flip) - (low ^ other)) * block
                scores = score_tile(cross[flip][...], inner[other][block : 2 * block])
                pieces.append(jnp.where(gap < reach - offset, scores, NEG_FILL))
            value_tiles = [inner[other][2 * block :] for other in range(half)]
            numerator, total, peak = softmax_rows(pieces, value_tiles)
            out_refs[flip][:block] = (numerator / total).astype(jnp.bfloat16)
            out_refs[flip][block:] = pack_stat(peak * FACTOR + jnp.log2(total))


def attend_rest(half, me_ref, reach_ref, *refs):
    lower, upper = refs[:half], refs[half : 2 * half]
    cross_k, cross_v = refs[2 * half : 3 * half], refs[3 * half : 4 * half]
    out_refs = refs[4 * half : 5 * half]
    qkv, o_low, o_up, stats = refs[5 * half :]
    me = me_ref[0]
    low = me % half
    block = cross_k[0].shape[0]
    gap = gaps(block)
    for flip in range(half):
        at = pl.multiple_of((low ^ flip) * block, block)
        for place in range(3):
            rows = slice(place * block, (place + 1) * block)
            qkv[place, pl.ds(at, block)] = lower[flip][rows]
            qkv[3 + place, pl.ds(at, block)] = upper[flip][rows]

    def own_pieces(first, i):
        q_tile = qkv[first, i * block : (i + 1) * block]
        pieces, value_tiles = [], []
        for j in range(i + 1):
            scores = score_tile(q_tile, qkv[first + 1, j * block : (j + 1) * block])
            pieces.append(jnp.where(gap >= 0, scores, NEG_FILL) if i == j else scores)
            value_tiles.append(qkv[first + 2, j * block : (j + 1) * block])
        return q_tile, pieces, value_tiles

    for i in range(half):
        numerator, total, peak = softmax_rows(*own_pieces(0, i)[1:])
        o_low[i] = (numerator / total).astype(jnp.bfloat16)
        stats[i] = pack_stat(peak * FACTOR + jnp.log2(total))

    @pl.when(me < half)
    def _():
        for i in range(half):
            numerator, total, _ = softmax_rows(*own_pieces(3, i)[1:])
            o_up[i] = (numerator / total).astype(jnp.bfloat16)

    @pl.when(me >= half)
    def _():
        reach = reach_ref[1:2]
        for i in range(half):
            q_tile, pieces, value_tiles = own_pieces(3, i)
            for other in range(half):
                offset = (half + i - (low ^ other)) * block
                scores = score_tile(q_tile, cross_k[other][...])
                pieces.append(jnp.where(gap < reach - offset, scores, NEG_FILL))
                value_tiles.append(cross_v[other][...])
            numerator, total, _ = softmax_rows(pieces, value_tiles)
            o_up[i] = (numerator / total).astype(jnp.bfloat16)

    for flip in range(half):
        out_refs[flip][:block] = o_low[low ^ flip]
        out_refs[flip][block : 2 * block] = o_up[low ^ flip]
        out_refs[flip][2 * block :] = stats[low ^ flip]


def join_heads(half, me_ref, inner, across, joined):
    me = me_ref[0]
    low = me % half
    block = joined.shape[0]
    for flip in range(half):
        at = pl.multiple_of((low ^ flip) * HEAD_DIM, HEAD_DIM)
        up_at = pl.multiple_of((low ^ flip) * HEAD_DIM + half * HEAD_DIM, HEAD_DIM)
        joined[:, pl.ds(up_at, HEAD_DIM)] = inner[flip][block : 2 * block]

        @pl.when(me < half)
        def _():
            joined[:, pl.ds(at, HEAD_DIM)] = inner[flip][:block]

        @pl.when(me >= half)
        def _():
            share = share_column(inner[flip][2 * block :], across[flip][block:], block)
            mixed = inner[flip][:block].astype(jnp.float32) * share
            mixed = mixed + across[flip][:block].astype(jnp.float32) * (1.0 - share)
            joined[:, pl.ds(at, HEAD_DIM)] = mixed.astype(jnp.bfloat16)


def join_and_project(half, flip, me_ref, *refs):
    inner, across, (w_ref, out_ref, joined) = refs[:half], refs[half : 2 * half], refs[2 * half :]
    join_heads(half, me_ref, inner, across, joined)
    project(flip, me_ref, joined, w_ref, out_ref)


def project(flip, me_ref, joined, w_ref, out_ref):
    width = out_ref.shape[1]
    at = pl.multiple_of((me_ref[1] ^ flip) * width, width)
    out_ref[...] = jnp.dot(
        joined[...], w_ref[:, pl.ds(at, width)], preferred_element_type=jnp.float32
    ).astype(jnp.bfloat16)


def half_path(queries, keys_in, values_in, out_weight, spans, full_ids):
    n_seq = lax.axis_size("seq")
    half = n_seq // 2
    bf16, f32 = jnp.bfloat16, jnp.float32
    shape = jax.ShapeDtypeStruct
    where = jnp.stack([lax.axis_index("seq"), lax.axis_index("head")]).astype(jnp.int32)
    block = queries.shape[0]
    down = range(half - 1, -1, -1)
    piece = shape((block, HEAD_DIM), bf16)

    hbm = pl.BlockSpec(memory_space=pltpu.HBM)
    ours = (spans, full_ids, queries, keys_in, values_in)
    ours = [pltpu.with_memory_space_constraint(a, pltpu.HBM) for a in ours]
    dealt = own_kernel(
        functools.partial(deal, half),
        ([shape((3 * block, HEAD_DIM), bf16)] * half + [piece] * half) * 2
        + [shape((8, block), jnp.int32)],
        [SMEM] + [hbm] * 5,
        [
            pltpu.SemaphoreType.DMA((8 * half + 2,)),
            pltpu.SMEM(spans.shape, jnp.int32),
            pltpu.SMEM(full_ids.shape, jnp.int32),
        ],
    )(where, *ours)
    reach = held(dealt[4 * half])
    inner = [list(dealt[:half]), list(dealt[2 * half : 3 * half])]
    cross = [list(dealt[half : 2 * half]), list(dealt[3 * half : 4 * half])]
    for upper in range(2):
        for flip in range(half - 1, 0, -1):
            inner[upper][flip] = swap(inner[upper][flip], "seq", flip)
        for flip in down:
            pairs = [(i, i ^ half ^ flip) for i in range(half if upper else n_seq)]
            cross[upper][flip] = move(cross[upper][flip], "seq", pairs)
    w_held = held(out_weight)
    inner = [[held(a) for a in arrays] for arrays in inner]
    cross = [[held(a) for a in arrays] for arrays in cross]
    across, own_half = [None] * half, [None] * half
    lows = own_kernel(
        functools.partial(attend_low, half),
        [shape((block + STAT_ROWS, HEAD_DIM), bf16)] * half,
        [SMEM] + in_vmem(1 + 2 * half),
        flops=2 * 10**9,
    )(where, reach, *inner[0], *cross[0])
    for flip in down:
        pairs = [(i, half + (i ^ flip)) for i in range(half)]
        across[flip] = move(lows[flip], "seq", pairs)
    rest = own_kernel(
        functools.partial(attend_rest, half),
        [shape((2 * block + STAT_ROWS, HEAD_DIM), bf16)] * half,
        [SMEM] + in_vmem(1 + 4 * half),
        [
            pltpu.VMEM((6, half * block, HEAD_DIM), bf16),
            pltpu.VMEM((half, block, HEAD_DIM), bf16),
            pltpu.VMEM((half, block, HEAD_DIM), bf16),
            pltpu.VMEM((half, STAT_ROWS, HEAD_DIM), bf16),
        ],
        flops=4 * 10**9,
    )(where, reach, *inner[0], *inner[1], *cross[0], *cross[1])
    for flip in range(half):
        own_half[flip] = swap(rest[flip], "seq", flip) if flip else rest[flip]
    came = [held(a) for a in own_half + across]
    width = out_weight.shape[1] // lax.axis_size("head")
    part = shape((block, width), bf16)
    sent, joined = own_kernel(
        functools.partial(join_and_project, half, 3),
        [part, shape((block, n_seq * HEAD_DIM), bf16)],
        [SMEM] + in_vmem(2 * half + 1),
        flops=10**9,
    )(where, *came, w_held)

    def columns_of(flip, rows):
        return own_kernel(
            functools.partial(project, flip), [part], [SMEM] + in_vmem(2), flops=10**9
        )(where, held(rows), w_held)[0]

    def summed(one, other):
        return (one.astype(f32) + other.astype(f32)).astype(bf16)

    far = summed(swap(sent, "head", 1), columns_of(2, joined))
    rows, far = lax.optimization_barrier((joined, far))
    far = swap(far, "head", 2)
    near = columns_of(1, rows)
    near = summed(swap(near, "head", 1), columns_of(0, rows))
    return summed(near, far)


def on_device(queries, keys_in, values_in, out_weight, spans, full_ids):
    n_seq, n_head = lax.axis_size("seq"), lax.axis_size("head")
    block = queries.shape[0]
    one_head_each = queries.shape[1] == n_seq * HEAD_DIM
    if one_head_each and n_head == 4 and n_seq == 8 and block == 256:
        return half_path(queries, keys_in, values_in, out_weight, spans, full_ids)
    return ring_path(queries, keys_in, values_in, out_weight, spans, full_ids)


def solution(mesh):
    placed = (
        P("seq", "head"),
        P("seq", "head"),
        P("seq", "head"),
        P("head", None),
        P("head"),
        P("head"),
    )
    return jax.shard_map(
        on_device, mesh=mesh, in_specs=placed, out_specs=P("seq", "head"), check_vma=False
    )
```

```python
import math

import functools

import jax
import jax.numpy as jnp
from jax import lax
from jax.experimental import pallas as pl
from jax.experimental.pallas import tpu as pltpu
from jax.sharding import PartitionSpec as P

HEAD_DIM = 128
SPAN_MAX = 4096


NEG_FILL = -1e30


def from_behind(block, axis, distance):
    devices = range(lax.axis_size(axis))
    route = [(i - distance, i) for i in devices if i - distance in devices]
    return lax.ppermute(block, axis, route)


def online_update(carry_state, scores, allowed, value_rows):
    old_peak, row_total, numerator = carry_state
    masked = jnp.where(allowed, scores, NEG_FILL)
    new_peak = jnp.maximum(old_peak, jnp.max(masked, axis=-1))
    weights = jnp.where(allowed, jnp.exp(masked - new_peak[..., None]), 0.0)
    rescale = jnp.exp(old_peak - new_peak)
    row_total = row_total * rescale + jnp.sum(weights, axis=-1)
    numerator = numerator * rescale[..., None] + jnp.einsum(
        "hqk,hkd->hqd", weights.astype(jnp.bfloat16), value_rows, preferred_element_type=jnp.float32
    )
    return (new_peak, row_total, numerator)


def empty_state(lead_count, row_count, head_width):
    return (
        jnp.full((lead_count, row_count), NEG_FILL, jnp.float32),
        jnp.zeros((lead_count, row_count), jnp.float32),
        jnp.zeros((lead_count, row_count, head_width), jnp.float32),
    )


def finish(carry_state):
    return (carry_state[2] / carry_state[1][..., None]).astype(jnp.bfloat16)


def ring_path(queries, keys_in, values_in, out_weight, spans, full_ids):
    score_scale = HEAD_DIM ** (-0.5)
    n_seq = lax.axis_size("seq")
    seq_index = lax.axis_index("seq")
    tok_rows = queries.shape[0]
    group_heads = queries.shape[1] // HEAD_DIM
    full_count = full_ids.shape[0]
    band_count = group_heads - full_count
    head_base = lax.axis_index("head") * group_heads
    local_range = jnp.arange(group_heads)
    marks = jnp.sum(
        (local_range[:, None] + head_base == full_ids[None, :]).astype(jnp.int32), axis=1
    )
    order_local = jnp.argsort(marks * group_heads + local_range)
    band_local = order_local[:band_count]
    full_local = order_local[band_count:]
    query_three = queries.reshape(tok_rows, group_heads, HEAD_DIM)
    key_three = keys_in.reshape(tok_rows, group_heads, HEAD_DIM)
    value_three = values_in.reshape(tok_rows, group_heads, HEAD_DIM)
    query_band = jnp.take(query_three, band_local, axis=1).transpose(1, 0, 2)
    kv_band = jnp.stack(
        [
            jnp.take(key_three, band_local, axis=1).transpose(1, 0, 2),
            jnp.take(value_three, band_local, axis=1).transpose(1, 0, 2),
        ]
    )
    band_reach = jnp.take(spans, band_local)
    query_pos = seq_index * tok_rows + jnp.arange(tok_rows)
    hop_count = min(max(1, SPAN_MAX // tok_rows), n_seq - 1)
    arrived = [(kv_band, 0)]
    moving = kv_band
    for distance in range(1, hop_count + 1):
        moving = from_behind(moving, "seq", 1)
        arrived.append((moving, distance))
    batch_size = max(1, 512 // tok_rows)
    band_state = empty_state(band_count, tok_rows, HEAD_DIM)
    for first_piece in range(0, len(arrived), batch_size):
        batch_pieces = arrived[first_piece : first_piece + batch_size]
        key_rows = jnp.concatenate([arrival[0][0] for arrival in batch_pieces], axis=1)
        value_rows = jnp.concatenate([arrival[0][1] for arrival in batch_pieces], axis=1)
        key_pos = jnp.concatenate(
            [(seq_index - arrival[1]) * tok_rows + jnp.arange(tok_rows) for arrival in batch_pieces]
        )
        scores = (
            jnp.einsum("hqd,hkd->hqk", query_band, key_rows, preferred_element_type=jnp.float32)
            * score_scale
        )
        gap_size = query_pos[None, :, None] - key_pos[None, None, :]
        allowed = (
            (gap_size >= 0) & (gap_size < band_reach[:, None, None]) & (key_pos >= 0)[None, None, :]
        )
        band_state = online_update(band_state, scores, allowed, value_rows)
    band_out = finish(band_state)
    query_full = jnp.take(query_three, full_local, axis=1).transpose(1, 0, 2)
    key_full = jnp.take(key_three, full_local, axis=1).transpose(1, 0, 2)
    value_full = jnp.take(value_three, full_local, axis=1).transpose(1, 0, 2)
    kv_full = jnp.stack([key_full, value_full])
    last_query = seq_index * tok_rows + tok_rows - 1
    key_piece = lax.all_gather(kv_full, "seq", axis=2, tiled=True)
    row_count = key_piece.shape[2]
    tile_rows = math.gcd(row_count, 512)

    def absorb_tile(tile_index, inner_state):
        key_tile = lax.dynamic_slice_in_dim(key_piece[0], tile_index * tile_rows, tile_rows, 1)
        value_tile = lax.dynamic_slice_in_dim(key_piece[1], tile_index * tile_rows, tile_rows, 1)
        key_pos = tile_index * tile_rows + jnp.arange(tile_rows)
        scores = (
            jnp.einsum("hqd,hkd->hqk", query_full, key_tile, preferred_element_type=jnp.float32)
            * score_scale
        )
        allowed = key_pos[None, None, :] <= query_pos[None, :, None]
        return online_update(inner_state, scores, allowed, value_tile)

    live_tiles = jnp.clip(last_query // tile_rows + 1, 0, row_count // tile_rows)
    full_state = lax.fori_loop(
        0, live_tiles, absorb_tile, empty_state(full_count, tok_rows, HEAD_DIM)
    )
    full_out = finish(full_state)
    combined = jnp.concatenate([band_out, full_out], axis=0)
    inverse = jnp.argsort(order_local)
    per_head = jnp.take(combined, inverse, axis=0)
    attended = per_head.transpose(1, 0, 2).reshape(tok_rows, group_heads * HEAD_DIM)
    projected = jnp.dot(attended, out_weight, preferred_element_type=jnp.float32)
    return lax.psum_scatter(projected.astype(jnp.bfloat16), "head", scatter_dimension=1, tiled=True)


def move(block, axis, pairs):
    return lax.ppermute(block, axis, pairs)


def swap(block, axis, flip):
    return move(block, axis, [(i, i ^ flip) for i in range(lax.axis_size(axis))])


def in_vmem(count):
    return [pl.BlockSpec(memory_space=pltpu.VMEM)] * count


def held(array):
    return pltpu.with_memory_space_constraint(array, pltpu.VMEM)


SMEM = pl.BlockSpec(memory_space=pltpu.SMEM)
FACTOR = HEAD_DIM**-0.5 * math.log2(math.e)
STAT_ROWS = 16


def own_kernel(body, out_shapes, in_specs, scratch=(), flops=10**8, limit=20 * 2**20):
    return pl.pallas_call(
        body,
        out_shape=out_shapes,
        in_specs=in_specs,
        out_specs=in_vmem(len(out_shapes)),
        scratch_shapes=list(scratch),
        compiler_params=pltpu.CompilerParams(vmem_limit_bytes=limit),
        cost_estimate=pl.CostEstimate(flops=flops, bytes_accessed=10**6, transcendentals=0),
    )


def deal(half, me_ref, spans_ref, full_ref, q_ref, k_ref, v_ref, *refs):
    reach_ref, sems, spans, full_ids = refs[4 * half :]
    me = me_ref[0]
    low = me % half
    tables = [
        pltpu.make_async_copy(spans_ref, spans, sems.at[8 * half]),
        pltpu.make_async_copy(full_ref, full_ids, sems.at[8 * half + 1]),
    ]
    for copy in tables:
        copy.start()
    rows = q_ref.shape[0]
    waits = []

    def fetch(source, head, out_ref, place):
        at = pl.multiple_of(head * HEAD_DIM, HEAD_DIM)
        return pltpu.make_async_copy(
            source.at[:, pl.ds(at, HEAD_DIM)],
            out_ref.at[pl.ds(place * rows, rows)],
            sems.at[len(waits)],
        )

    for upper in range(2):
        inner = refs[2 * upper * half : (2 * upper + 1) * half]
        cross = refs[(2 * upper + 1) * half : (2 * upper + 2) * half]
        for flip in range(half - 1, -1, -1):
            for place, source in enumerate((q_ref, k_ref, v_ref)):
                copy = fetch(source, (low ^ flip) + upper * half, inner[flip], place)
                copy.start()
                waits.append(copy)
        for flip in range(half - 1, -1, -1):
            target = low ^ flip
            if upper:
                copy = fetch(v_ref, target + half, cross[flip], 0)
                copy.start()
            else:
                below = fetch(k_ref, target + half, cross[flip], 0)
                copy = fetch(q_ref, target, cross[flip], 0)
                pl.when(me < half)(below.start)
                pl.when(me >= half)(copy.start)
            waits.append(copy)
    for copy in tables:
        copy.wait()
    for upper in range(2):
        local = low + upper * half
        reach = spans[local]
        for place in range(full_ids.shape[0]):
            is_full = full_ids[place] == me_ref[1] * 2 * half + local
            reach = jnp.where(is_full, 2 * half * rows, reach)
        reach_ref[upper : upper + 1] = jnp.full((1, reach_ref.shape[1]), reach, jnp.int32)
    for copy in waits:
        copy.wait()


def square_eye(size):
    row = lax.broadcasted_iota(jnp.int32, (size, size), 0)
    return row == lax.broadcasted_iota(jnp.int32, (size, size), 1)


def pack_stat(stat):
    eye = square_eye(HEAD_DIM)
    rows = []
    for first in range(0, stat.shape[0], HEAD_DIM):
        piece = jnp.where(eye, stat[first : first + HEAD_DIM], 0.0)
        left = jnp.sum(piece, axis=0, keepdims=True)
        for _ in range(3):
            part = left.astype(jnp.bfloat16).astype(jnp.float32)
            rows.append(part)
            left = left - part
    rows.append(jnp.zeros((STAT_ROWS - len(rows), HEAD_DIM), jnp.float32))
    return jnp.concatenate(rows, axis=0).astype(jnp.bfloat16)


def share_column(here, there, size):
    eye = square_eye(HEAD_DIM)
    apart = there.astype(jnp.float32) - here.astype(jnp.float32)
    columns = []
    for index in range(size // HEAD_DIM):
        row = apart[3 * index : 3 * index + 1]
        for more in (1, 2):
            row = row + apart[3 * index + more : 3 * index + more + 1]
        share = 1.0 / (1.0 + jnp.exp2(row))
        columns.append(jnp.sum(jnp.where(eye, share, 0.0), axis=1, keepdims=True))
    return jnp.concatenate(columns, axis=0)


def softmax_rows(pieces, value_tiles):
    peak = jnp.max(functools.reduce(jnp.maximum, pieces), axis=1, keepdims=True)
    total, numerator = None, None
    for scores, value_tile in zip(pieces, value_tiles):
        weights = jnp.exp2((scores - peak) * FACTOR)
        total = weights if total is None else total + weights
        product = jnp.dot(
            weights.astype(jnp.bfloat16), value_tile, preferred_element_type=jnp.float32
        )
        numerator = product if numerator is None else numerator + product
    return numerator, jnp.sum(total, axis=1, keepdims=True), peak


def score_tile(q_tile, k_tile):
    return lax.dot_general(
        q_tile, k_tile, (((1,), (1,)), ((), ())), preferred_element_type=jnp.float32
    )


def gaps(block):
    row = lax.broadcasted_iota(jnp.int32, (block, block), 0)
    return row - lax.broadcasted_iota(jnp.int32, (block, block), 1)


def gather_rows(half, low, inner, qkv, first):
    block = inner[0].shape[0] // 3
    for flip in range(half):
        at = pl.multiple_of((low ^ flip) * block, block)
        for place in range(3):
            rows = slice(place * block, (place + 1) * block)
            qkv[first + place, pl.ds(at, block)] = inner[flip][rows]


def own_pieces(qkv, first, i, gap):
    block = gap.shape[0]
    q_tile = qkv[first, i * block : (i + 1) * block]
    pieces, value_tiles = [], []
    for j in range(i + 1):
        scores = score_tile(q_tile, qkv[first + 1, j * block : (j + 1) * block])
        pieces.append(jnp.where(gap >= 0, scores, NEG_FILL) if i == j else scores)
        value_tiles.append(qkv[first + 2, j * block : (j + 1) * block])
    return q_tile, pieces, value_tiles


def attend_lower_own(half, qkv, gap, o_low, stats):
    for i in range(half):
        numerator, total, peak = softmax_rows(*own_pieces(qkv, 0, i, gap)[1:])
        o_low[i] = (numerator / total).astype(jnp.bfloat16)
        stats[i] = pack_stat(peak * FACTOR + jnp.log2(total))


def attend_low(half, me_ref, reach_ref, *refs):
    inner, cross, out_refs = refs[:half], refs[half : 2 * half], refs[2 * half : 3 * half]
    o_low, stats, qkv = refs[3 * half :]
    block = cross[0].shape[0]
    low = me_ref[0] % half
    gap = gaps(block)

    @pl.when(me_ref[0] < half)
    def _():
        reach = reach_ref[0:1]
        for flip in range(half - 1, -1, -1):
            pieces = []
            for other in range(half):
                offset = (half + (low ^ flip) - (low ^ other)) * block
                scores = score_tile(cross[flip][...], inner[other][block : 2 * block])
                pieces.append(jnp.where(gap < reach - offset, scores, NEG_FILL))
            value_tiles = [inner[other][2 * block :] for other in range(half)]
            numerator, total, peak = softmax_rows(pieces, value_tiles)
            out_refs[flip][:block] = (numerator / total).astype(jnp.bfloat16)
            out_refs[flip][block:] = pack_stat(peak * FACTOR + jnp.log2(total))

    @pl.when(me_ref[0] >= half)
    def _():
        gather_rows(half, low, inner, qkv, 0)
        attend_lower_own(half, qkv, gap, o_low, stats)


def attend_rest(half, me_ref, reach_ref, low_ref, stat_ref, *refs):
    lower, upper = refs[:half], refs[half : 2 * half]
    cross_k, cross_v = refs[2 * half : 3 * half], refs[3 * half : 4 * half]
    out_refs = refs[4 * half : 5 * half]
    qkv, o_low, o_up, stats = refs[5 * half :]
    me = me_ref[0]
    low = me % half
    block = cross_k[0].shape[0]
    gap = gaps(block)
    gather_rows(half, low, upper, qkv, 3)

    @pl.when(me < half)
    def _():
        gather_rows(half, low, lower, qkv, 0)
        attend_lower_own(half, qkv, gap, o_low, stats)
        for i in range(half):
            numerator, total, _ = softmax_rows(*own_pieces(qkv, 3, i, gap)[1:])
            o_up[i] = (numerator / total).astype(jnp.bfloat16)
        for flip in range(half):
            out_refs[flip][:block] = o_low[low ^ flip]
            out_refs[flip][2 * block :] = stats[low ^ flip]

    @pl.when(me >= half)
    def _():
        reach = reach_ref[1:2]
        for i in range(half):
            q_tile, pieces, value_tiles = own_pieces(qkv, 3, i, gap)
            for other in range(half):
                offset = (half + i - (low ^ other)) * block
                scores = score_tile(q_tile, cross_k[other][...])
                pieces.append(jnp.where(gap < reach - offset, scores, NEG_FILL))
                value_tiles.append(cross_v[other][...])
            numerator, total, _ = softmax_rows(pieces, value_tiles)
            o_up[i] = (numerator / total).astype(jnp.bfloat16)
        for flip in range(half):
            out_refs[flip][:block] = low_ref[low ^ flip]
            out_refs[flip][2 * block :] = stat_ref[low ^ flip]

    for flip in range(half):
        out_refs[flip][block : 2 * block] = o_up[low ^ flip]


def join_heads(half, me_ref, inner, across, joined):
    me = me_ref[0]
    low = me % half
    block = joined.shape[0]
    for flip in range(half):
        at = pl.multiple_of((low ^ flip) * HEAD_DIM, HEAD_DIM)
        up_at = pl.multiple_of((low ^ flip) * HEAD_DIM + half * HEAD_DIM, HEAD_DIM)
        joined[:, pl.ds(up_at, HEAD_DIM)] = inner[flip][block : 2 * block]

        @pl.when(me < half)
        def _():
            joined[:, pl.ds(at, HEAD_DIM)] = inner[flip][:block]

        @pl.when(me >= half)
        def _():
            share = share_column(inner[flip][2 * block :], across[flip][block:], block)
            mixed = inner[flip][:block].astype(jnp.float32) * share
            mixed = mixed + across[flip][:block].astype(jnp.float32) * (1.0 - share)
            joined[:, pl.ds(at, HEAD_DIM)] = mixed.astype(jnp.bfloat16)


def join_and_project(half, flip, part, parts, me_ref, *refs):
    inner, across, (w_ref, out_ref, joined) = refs[:half], refs[half : 2 * half], refs[2 * half :]
    join_heads(half, me_ref, inner, across, joined)
    project(flip, part, parts, me_ref, joined, w_ref, out_ref)


def project(flip, part, parts, me_ref, joined, w_ref, *refs):
    *other, out_ref = refs
    width = out_ref.shape[1]
    at = pl.multiple_of(((me_ref[1] ^ flip) * parts + part) * width, width)
    product = jnp.dot(
        joined[...], w_ref[:, pl.ds(at, width)], preferred_element_type=jnp.float32
    ).astype(jnp.bfloat16)
    if other:
        total = product.astype(jnp.float32) + other[0][...].astype(jnp.float32)
        product = total.astype(jnp.bfloat16)
    out_ref[...] = product


def half_path(queries, keys_in, values_in, out_weight, spans, full_ids):
    n_seq = lax.axis_size("seq")
    half = n_seq // 2
    bf16, f32 = jnp.bfloat16, jnp.float32
    shape = jax.ShapeDtypeStruct
    where = jnp.stack([lax.axis_index("seq"), lax.axis_index("head")]).astype(jnp.int32)
    block = queries.shape[0]
    down = range(half - 1, -1, -1)
    piece = shape((block, HEAD_DIM), bf16)

    hbm = pl.BlockSpec(memory_space=pltpu.HBM)
    ours = (spans, full_ids, queries, keys_in, values_in)
    ours = [pltpu.with_memory_space_constraint(a, pltpu.HBM) for a in ours]
    dealt = own_kernel(
        functools.partial(deal, half),
        ([shape((3 * block, HEAD_DIM), bf16)] * half + [piece] * half) * 2
        + [shape((8, block), jnp.int32)],
        [SMEM] + [hbm] * 5,
        [
            pltpu.SemaphoreType.DMA((8 * half + 2,)),
            pltpu.SMEM(spans.shape, jnp.int32),
            pltpu.SMEM(full_ids.shape, jnp.int32),
        ],
    )(where, *ours)
    reach = held(dealt[4 * half])
    inner = [list(dealt[:half]), list(dealt[2 * half : 3 * half])]
    cross = [list(dealt[half : 2 * half]), list(dealt[3 * half : 4 * half])]
    for upper in range(2):
        for flip in range(half - 1, 0, -1):
            inner[upper][flip] = swap(inner[upper][flip], "seq", flip)
        for flip in down:
            pairs = [(i, i ^ half ^ flip) for i in range(half if upper else n_seq)]
            cross[upper][flip] = move(cross[upper][flip], "seq", pairs)
    w_held = held(out_weight)
    inner = [[held(a) for a in arrays] for arrays in inner]
    cross = [[held(a) for a in arrays] for arrays in cross]
    across, own_half = [None] * half, [None] * half
    *lows, o_low, stats = own_kernel(
        functools.partial(attend_low, half),
        [shape((block + STAT_ROWS, HEAD_DIM), bf16)] * half
        + [shape((half, block, HEAD_DIM), bf16), shape((half, STAT_ROWS, HEAD_DIM), bf16)],
        [SMEM] + in_vmem(1 + 2 * half),
        [pltpu.VMEM((3, half * block, HEAD_DIM), bf16)],
        flops=2 * 10**9,
    )(where, reach, *inner[0], *cross[0])
    for flip in range(half):
        pairs = [(i, half + (i ^ flip)) for i in range(half)]
        across[flip] = move(lows[flip], "seq", pairs)
    rest = own_kernel(
        functools.partial(attend_rest, half),
        [shape((2 * block + STAT_ROWS, HEAD_DIM), bf16)] * half,
        [SMEM] + in_vmem(3 + 4 * half),
        [
            pltpu.VMEM((6, half * block, HEAD_DIM), bf16),
            pltpu.VMEM((half, block, HEAD_DIM), bf16),
            pltpu.VMEM((half, block, HEAD_DIM), bf16),
            pltpu.VMEM((half, STAT_ROWS, HEAD_DIM), bf16),
        ],
        flops=4 * 10**9,
    )(where, reach, held(o_low), held(stats), *inner[0], *inner[1], *cross[0], *cross[1])
    for flip in range(half):
        own_half[flip] = swap(rest[flip], "seq", flip) if flip else rest[flip]
    came = [held(a) for a in own_half + across]
    width = out_weight.shape[1] // lax.axis_size("head")
    parts = 2
    slab = shape((block, width // parts), bf16)

    def columns_of(flip, part, parts, rows, *other):
        return own_kernel(
            functools.partial(project, flip, part, parts),
            [shape((block, width // parts), bf16)],
            [SMEM] + in_vmem(2 + len(other)),
            flops=10**9 // parts,
        )(where, held(rows), w_held, *[held(a) for a in other])[0]

    first, joined = own_kernel(
        functools.partial(join_and_project, half, 3, 0, parts),
        [slab, shape((block, n_seq * HEAD_DIM), bf16)],
        [SMEM] + in_vmem(2 * half + 1),
        flops=10**9,
    )(where, *came, w_held)
    first = swap(first, "head", 1)
    second = columns_of(3, 1, parts, joined)
    second = swap(second, "head", 1)
    far = [first, second]
    for part in range(parts):
        far[part] = columns_of(2, part, parts, joined, far[part])
    rows, _ = lax.optimization_barrier((joined, far[1]))
    for part in range(parts):
        far[part] = swap(far[part], "head", 2)
    near = columns_of(1, 0, 1, rows)
    near = columns_of(0, 0, 1, rows, swap(near, "head", 1))
    return (near.astype(f32) + jnp.concatenate(far, axis=1).astype(f32)).astype(bf16)


def on_device(queries, keys_in, values_in, out_weight, spans, full_ids):
    n_seq, n_head = lax.axis_size("seq"), lax.axis_size("head")
    block = queries.shape[0]
    one_head_each = queries.shape[1] == n_seq * HEAD_DIM
    if one_head_each and n_head == 4 and n_seq == 8 and block == 256:
        return half_path(queries, keys_in, values_in, out_weight, spans, full_ids)
    return ring_path(queries, keys_in, values_in, out_weight, spans, full_ids)


def solution(mesh):
    placed = (
        P("seq", "head"),
        P("seq", "head"),
        P("seq", "head"),
        P("head", None),
        P("head"),
        P("head"),
    )
    return jax.shard_map(
        on_device, mesh=mesh, in_specs=placed, out_specs=P("seq", "head"), check_vma=False
    )
```

```python
import math

import functools

import jax
import jax.numpy as jnp
from jax import lax
from jax.experimental import pallas as pl
from jax.experimental.pallas import tpu as pltpu
from jax.sharding import PartitionSpec as P

HEAD_DIM = 128
SPAN_MAX = 4096


NEG_FILL = -1e30


def from_behind(block, axis, distance):
    devices = range(lax.axis_size(axis))
    route = [(i - distance, i) for i in devices if i - distance in devices]
    return lax.ppermute(block, axis, route)


def online_update(carry_state, scores, allowed, value_rows):
    old_peak, row_total, numerator = carry_state
    masked = jnp.where(allowed, scores, NEG_FILL)
    new_peak = jnp.maximum(old_peak, jnp.max(masked, axis=-1))
    weights = jnp.where(allowed, jnp.exp(masked - new_peak[..., None]), 0.0)
    rescale = jnp.exp(old_peak - new_peak)
    row_total = row_total * rescale + jnp.sum(weights, axis=-1)
    numerator = numerator * rescale[..., None] + jnp.einsum(
        "hqk,hkd->hqd", weights.astype(jnp.bfloat16), value_rows, preferred_element_type=jnp.float32
    )
    return (new_peak, row_total, numerator)


def empty_state(lead_count, row_count, head_width):
    return (
        jnp.full((lead_count, row_count), NEG_FILL, jnp.float32),
        jnp.zeros((lead_count, row_count), jnp.float32),
        jnp.zeros((lead_count, row_count, head_width), jnp.float32),
    )


def finish(carry_state):
    return (carry_state[2] / carry_state[1][..., None]).astype(jnp.bfloat16)


def ring_path(queries, keys_in, values_in, out_weight, spans, full_ids):
    score_scale = HEAD_DIM ** (-0.5)
    n_seq = lax.axis_size("seq")
    seq_index = lax.axis_index("seq")
    tok_rows = queries.shape[0]
    group_heads = queries.shape[1] // HEAD_DIM
    full_count = full_ids.shape[0]
    band_count = group_heads - full_count
    head_base = lax.axis_index("head") * group_heads
    local_range = jnp.arange(group_heads)
    marks = jnp.sum(
        (local_range[:, None] + head_base == full_ids[None, :]).astype(jnp.int32), axis=1
    )
    order_local = jnp.argsort(marks * group_heads + local_range)
    band_local = order_local[:band_count]
    full_local = order_local[band_count:]
    query_three = queries.reshape(tok_rows, group_heads, HEAD_DIM)
    key_three = keys_in.reshape(tok_rows, group_heads, HEAD_DIM)
    value_three = values_in.reshape(tok_rows, group_heads, HEAD_DIM)
    query_band = jnp.take(query_three, band_local, axis=1).transpose(1, 0, 2)
    kv_band = jnp.stack(
        [
            jnp.take(key_three, band_local, axis=1).transpose(1, 0, 2),
            jnp.take(value_three, band_local, axis=1).transpose(1, 0, 2),
        ]
    )
    band_reach = jnp.take(spans, band_local)
    query_pos = seq_index * tok_rows + jnp.arange(tok_rows)
    hop_count = min(max(1, SPAN_MAX // tok_rows), n_seq - 1)
    arrived = [(kv_band, 0)]
    moving = kv_band
    for distance in range(1, hop_count + 1):
        moving = from_behind(moving, "seq", 1)
        arrived.append((moving, distance))
    batch_size = max(1, 512 // tok_rows)
    band_state = empty_state(band_count, tok_rows, HEAD_DIM)
    for first_piece in range(0, len(arrived), batch_size):
        batch_pieces = arrived[first_piece : first_piece + batch_size]
        key_rows = jnp.concatenate([arrival[0][0] for arrival in batch_pieces], axis=1)
        value_rows = jnp.concatenate([arrival[0][1] for arrival in batch_pieces], axis=1)
        key_pos = jnp.concatenate(
            [(seq_index - arrival[1]) * tok_rows + jnp.arange(tok_rows) for arrival in batch_pieces]
        )
        scores = (
            jnp.einsum("hqd,hkd->hqk", query_band, key_rows, preferred_element_type=jnp.float32)
            * score_scale
        )
        gap_size = query_pos[None, :, None] - key_pos[None, None, :]
        allowed = (
            (gap_size >= 0) & (gap_size < band_reach[:, None, None]) & (key_pos >= 0)[None, None, :]
        )
        band_state = online_update(band_state, scores, allowed, value_rows)
    band_out = finish(band_state)
    query_full = jnp.take(query_three, full_local, axis=1).transpose(1, 0, 2)
    key_full = jnp.take(key_three, full_local, axis=1).transpose(1, 0, 2)
    value_full = jnp.take(value_three, full_local, axis=1).transpose(1, 0, 2)
    kv_full = jnp.stack([key_full, value_full])
    last_query = seq_index * tok_rows + tok_rows - 1
    key_piece = lax.all_gather(kv_full, "seq", axis=2, tiled=True)
    row_count = key_piece.shape[2]
    tile_rows = math.gcd(row_count, 512)

    def absorb_tile(tile_index, inner_state):
        key_tile = lax.dynamic_slice_in_dim(key_piece[0], tile_index * tile_rows, tile_rows, 1)
        value_tile = lax.dynamic_slice_in_dim(key_piece[1], tile_index * tile_rows, tile_rows, 1)
        key_pos = tile_index * tile_rows + jnp.arange(tile_rows)
        scores = (
            jnp.einsum("hqd,hkd->hqk", query_full, key_tile, preferred_element_type=jnp.float32)
            * score_scale
        )
        allowed = key_pos[None, None, :] <= query_pos[None, :, None]
        return online_update(inner_state, scores, allowed, value_tile)

    live_tiles = jnp.clip(last_query // tile_rows + 1, 0, row_count // tile_rows)
    full_state = lax.fori_loop(
        0, live_tiles, absorb_tile, empty_state(full_count, tok_rows, HEAD_DIM)
    )
    full_out = finish(full_state)
    combined = jnp.concatenate([band_out, full_out], axis=0)
    inverse = jnp.argsort(order_local)
    per_head = jnp.take(combined, inverse, axis=0)
    attended = per_head.transpose(1, 0, 2).reshape(tok_rows, group_heads * HEAD_DIM)
    projected = jnp.dot(attended, out_weight, preferred_element_type=jnp.float32)
    return lax.psum_scatter(projected.astype(jnp.bfloat16), "head", scatter_dimension=1, tiled=True)


def move(block, axis, pairs):
    return lax.ppermute(block, axis, pairs)


def swap(block, axis, flip):
    return move(block, axis, [(i, i ^ flip) for i in range(lax.axis_size(axis))])


def in_vmem(count):
    return [pl.BlockSpec(memory_space=pltpu.VMEM)] * count


def held(array):
    return pltpu.with_memory_space_constraint(array, pltpu.VMEM)


SMEM = pl.BlockSpec(memory_space=pltpu.SMEM)
FACTOR = HEAD_DIM**-0.5 * math.log2(math.e)
STAT_ROWS = 16


def own_kernel(body, out_shapes, in_specs, scratch=(), flops=10**8, limit=20 * 2**20):
    return pl.pallas_call(
        body,
        out_shape=out_shapes,
        in_specs=in_specs,
        out_specs=in_vmem(len(out_shapes)),
        scratch_shapes=list(scratch),
        compiler_params=pltpu.CompilerParams(vmem_limit_bytes=limit),
        cost_estimate=pl.CostEstimate(flops=flops, bytes_accessed=10**6, transcendentals=0),
    )


def deal(half, me_ref, spans_ref, full_ref, q_ref, k_ref, v_ref, *refs):
    reach_ref, sems, spans, full_ids = refs[4 * half :]
    me = me_ref[0]
    low = me % half
    tables = [
        pltpu.make_async_copy(spans_ref, spans, sems.at[8 * half]),
        pltpu.make_async_copy(full_ref, full_ids, sems.at[8 * half + 1]),
    ]
    for copy in tables:
        copy.start()
    rows = q_ref.shape[0]
    waits = []

    def fetch(source, head, out_ref, place):
        at = pl.multiple_of(head * HEAD_DIM, HEAD_DIM)
        return pltpu.make_async_copy(
            source.at[:, pl.ds(at, HEAD_DIM)],
            out_ref.at[pl.ds(place * rows, rows)],
            sems.at[len(waits)],
        )

    for upper in range(2):
        inner = refs[2 * upper * half : (2 * upper + 1) * half]
        cross = refs[(2 * upper + 1) * half : (2 * upper + 2) * half]
        for flip in range(half - 1, -1, -1):
            for place, source in enumerate((q_ref, k_ref, v_ref)):
                copy = fetch(source, (low ^ flip) + upper * half, inner[flip], place)
                copy.start()
                waits.append(copy)
        for flip in range(half - 1, -1, -1):
            target = low ^ flip
            if upper:
                copy = fetch(v_ref, target + half, cross[flip], 0)
                copy.start()
            else:
                below = fetch(k_ref, target + half, cross[flip], 0)
                copy = fetch(q_ref, target, cross[flip], 0)
                pl.when(me < half)(below.start)
                pl.when(me >= half)(copy.start)
            waits.append(copy)
    for copy in tables:
        copy.wait()
    for upper in range(2):
        local = low + upper * half
        reach = spans[local]
        for place in range(full_ids.shape[0]):
            is_full = full_ids[place] == me_ref[1] * 2 * half + local
            reach = jnp.where(is_full, 2 * half * rows, reach)
        reach_ref[upper : upper + 1] = jnp.full((1, reach_ref.shape[1]), reach, jnp.int32)
    for copy in waits:
        copy.wait()


def square_eye(size):
    row = lax.broadcasted_iota(jnp.int32, (size, size), 0)
    return row == lax.broadcasted_iota(jnp.int32, (size, size), 1)


def pack_stat(stat):
    eye = square_eye(HEAD_DIM)
    rows = []
    for first in range(0, stat.shape[0], HEAD_DIM):
        piece = jnp.where(eye, stat[first : first + HEAD_DIM], 0.0)
        left = jnp.sum(piece, axis=0, keepdims=True)
        for _ in range(3):
            part = left.astype(jnp.bfloat16).astype(jnp.float32)
            rows.append(part)
            left = left - part
    rows.append(jnp.zeros((STAT_ROWS - len(rows), HEAD_DIM), jnp.float32))
    return jnp.concatenate(rows, axis=0).astype(jnp.bfloat16)


def share_column(here, there, size):
    eye = square_eye(HEAD_DIM)
    apart = there.astype(jnp.float32) - here.astype(jnp.float32)
    columns = []
    for index in range(size // HEAD_DIM):
        row = apart[3 * index : 3 * index + 1]
        for more in (1, 2):
            row = row + apart[3 * index + more : 3 * index + more + 1]
        share = 1.0 / (1.0 + jnp.exp2(row))
        columns.append(jnp.sum(jnp.where(eye, share, 0.0), axis=1, keepdims=True))
    return jnp.concatenate(columns, axis=0)


def softmax_rows(pieces, value_tiles):
    peak = jnp.max(functools.reduce(jnp.maximum, pieces), axis=1, keepdims=True)
    total, numerator = None, None
    for scores, value_tile in zip(pieces, value_tiles):
        weights = jnp.exp2((scores - peak) * FACTOR)
        total = weights if total is None else total + weights
        product = jnp.dot(
            weights.astype(jnp.bfloat16), value_tile, preferred_element_type=jnp.float32
        )
        numerator = product if numerator is None else numerator + product
    return numerator, jnp.sum(total, axis=1, keepdims=True), peak


def score_tile(q_tile, k_tile):
    return lax.dot_general(
        q_tile, k_tile, (((1,), (1,)), ((), ())), preferred_element_type=jnp.float32
    )


def gaps(block):
    row = lax.broadcasted_iota(jnp.int32, (block, block), 0)
    return row - lax.broadcasted_iota(jnp.int32, (block, block), 1)


def gather_rows(half, low, inner, qkv, first):
    block = inner[0].shape[0] // 3
    for flip in range(half):
        at = pl.multiple_of((low ^ flip) * block, block)
        for place in range(3):
            rows = slice(place * block, (place + 1) * block)
            qkv[first + place, pl.ds(at, block)] = inner[flip][rows]


def own_pieces(qkv, first, i, gap):
    block = gap.shape[0]
    q_tile = qkv[first, i * block : (i + 1) * block]
    pieces, value_tiles = [], []
    for j in range(i + 1):
        scores = score_tile(q_tile, qkv[first + 1, j * block : (j + 1) * block])
        pieces.append(jnp.where(gap >= 0, scores, NEG_FILL) if i == j else scores)
        value_tiles.append(qkv[first + 2, j * block : (j + 1) * block])
    return q_tile, pieces, value_tiles


def attend_lower_own(half, qkv, gap, o_low, stats):
    for i in range(half):
        numerator, total, peak = softmax_rows(*own_pieces(qkv, 0, i, gap)[1:])
        o_low[i] = (numerator / total).astype(jnp.bfloat16)
        stats[i] = pack_stat(peak * FACTOR + jnp.log2(total))


def attend_low(half, me_ref, reach_ref, *refs):
    inner, cross, out_refs = refs[:half], refs[half : 2 * half], refs[2 * half : 3 * half]
    o_low, stats, qkv = refs[3 * half :]
    block = cross[0].shape[0]
    low = me_ref[0] % half
    gap = gaps(block)

    @pl.when(me_ref[0] < half)
    def _():
        reach = reach_ref[0:1]
        for flip in range(half - 1, -1, -1):
            pieces = []
            for other in range(half):
                offset = (half + (low ^ flip) - (low ^ other)) * block
                scores = score_tile(cross[flip][...], inner[other][block : 2 * block])
                pieces.append(jnp.where(gap < reach - offset, scores, NEG_FILL))
            value_tiles = [inner[other][2 * block :] for other in range(half)]
            numerator, total, peak = softmax_rows(pieces, value_tiles)
            out_refs[flip][:block] = (numerator / total).astype(jnp.bfloat16)
            out_refs[flip][block:] = pack_stat(peak * FACTOR + jnp.log2(total))

    @pl.when(me_ref[0] >= half)
    def _():
        gather_rows(half, low, inner, qkv, 0)
        attend_lower_own(half, qkv, gap, o_low, stats)


def attend_rest(half, me_ref, reach_ref, low_ref, stat_ref, *refs):
    lower, upper = refs[:half], refs[half : 2 * half]
    cross_k, cross_v = refs[2 * half : 3 * half], refs[3 * half : 4 * half]
    out_refs = refs[4 * half : 5 * half]
    qkv, o_low, o_up, stats = refs[5 * half :]
    me = me_ref[0]
    low = me % half
    block = cross_k[0].shape[0]
    gap = gaps(block)
    gather_rows(half, low, upper, qkv, 3)

    @pl.when(me < half)
    def _():
        gather_rows(half, low, lower, qkv, 0)
        attend_lower_own(half, qkv, gap, o_low, stats)
        for i in range(half):
            numerator, total, _ = softmax_rows(*own_pieces(qkv, 3, i, gap)[1:])
            o_up[i] = (numerator / total).astype(jnp.bfloat16)
        for flip in range(half):
            out_refs[flip][:block] = o_low[low ^ flip]
            out_refs[flip][2 * block :] = stats[low ^ flip]

    @pl.when(me >= half)
    def _():
        reach = reach_ref[1:2]
        for i in range(half):
            q_tile, pieces, value_tiles = own_pieces(qkv, 3, i, gap)
            for other in range(half):
                offset = (half + i - (low ^ other)) * block
                scores = score_tile(q_tile, cross_k[other][...])
                pieces.append(jnp.where(gap < reach - offset, scores, NEG_FILL))
                value_tiles.append(cross_v[other][...])
            numerator, total, _ = softmax_rows(pieces, value_tiles)
            o_up[i] = (numerator / total).astype(jnp.bfloat16)
        for flip in range(half):
            out_refs[flip][:block] = low_ref[low ^ flip]
            out_refs[flip][2 * block :] = stat_ref[low ^ flip]

    for flip in range(half):
        out_refs[flip][block : 2 * block] = o_up[low ^ flip]


def join_heads(half, me_ref, inner, across, joined):
    me = me_ref[0]
    low = me % half
    block = joined.shape[0]

    def place(flip, upper, value):
        at = pl.multiple_of((low ^ flip) * HEAD_DIM + upper * half * HEAD_DIM, HEAD_DIM)
        joined[:, pl.ds(at, HEAD_DIM)] = value

    @pl.when(me < half)
    def _():
        for flip in range(half):
            place(flip, 0, inner[flip][:block])
            place(flip, 1, inner[flip][block : 2 * block])

    @pl.when(me >= half)
    def _():
        merged = []
        for flip in range(half):
            share = share_column(inner[flip][2 * block :], across[flip][block:], block)
            value = inner[flip][:block].astype(jnp.float32) * share
            value = value + across[flip][:block].astype(jnp.float32) * (1.0 - share)
            merged.append(value.astype(jnp.bfloat16))
        for flip in range(half):
            place(flip, 0, merged[flip])
            place(flip, 1, inner[flip][block : 2 * block])


def join_and_project(half, flip, part, parts, me_ref, *refs):
    inner, across, (w_ref, out_ref, joined) = refs[:half], refs[half : 2 * half], refs[2 * half :]
    join_heads(half, me_ref, inner, across, joined)
    project(flip, part, parts, me_ref, joined, w_ref, out_ref)


def project(flip, part, parts, me_ref, joined, w_ref, *refs):
    *other, out_ref = refs
    width = out_ref.shape[1]
    at = pl.multiple_of(((me_ref[1] ^ flip) * parts + part) * width, width)
    product = jnp.dot(
        joined[...], w_ref[:, pl.ds(at, width)], preferred_element_type=jnp.float32
    ).astype(jnp.bfloat16)
    if other:
        total = product.astype(jnp.float32) + other[0][...].astype(jnp.float32)
        product = total.astype(jnp.bfloat16)
    out_ref[...] = product


def half_path(queries, keys_in, values_in, out_weight, spans, full_ids):
    n_seq = lax.axis_size("seq")
    half = n_seq // 2
    bf16, f32 = jnp.bfloat16, jnp.float32
    shape = jax.ShapeDtypeStruct
    where = jnp.stack([lax.axis_index("seq"), lax.axis_index("head")]).astype(jnp.int32)
    block = queries.shape[0]
    down = range(half - 1, -1, -1)
    piece = shape((block, HEAD_DIM), bf16)

    hbm = pl.BlockSpec(memory_space=pltpu.HBM)
    ours = (spans, full_ids, queries, keys_in, values_in)
    ours = [pltpu.with_memory_space_constraint(a, pltpu.HBM) for a in ours]
    dealt = own_kernel(
        functools.partial(deal, half),
        ([shape((3 * block, HEAD_DIM), bf16)] * half + [piece] * half) * 2
        + [shape((8, block), jnp.int32)],
        [SMEM] + [hbm] * 5,
        [
            pltpu.SemaphoreType.DMA((8 * half + 2,)),
            pltpu.SMEM(spans.shape, jnp.int32),
            pltpu.SMEM(full_ids.shape, jnp.int32),
        ],
    )(where, *ours)
    reach = held(dealt[4 * half])
    inner = [list(dealt[:half]), list(dealt[2 * half : 3 * half])]
    cross = [list(dealt[half : 2 * half]), list(dealt[3 * half : 4 * half])]
    for upper in range(2):
        for flip in range(half - 1, 0, -1):
            inner[upper][flip] = swap(inner[upper][flip], "seq", flip)
        for flip in down:
            pairs = [(i, i ^ half ^ flip) for i in range(half if upper else n_seq)]
            cross[upper][flip] = move(cross[upper][flip], "seq", pairs)
    w_held = held(out_weight)
    inner = [[held(a) for a in arrays] for arrays in inner]
    cross = [[held(a) for a in arrays] for arrays in cross]
    across, own_half = [None] * half, [None] * half
    *lows, o_low, stats = own_kernel(
        functools.partial(attend_low, half),
        [shape((block + STAT_ROWS, HEAD_DIM), bf16)] * half
        + [shape((half, block, HEAD_DIM), bf16), shape((half, STAT_ROWS, HEAD_DIM), bf16)],
        [SMEM] + in_vmem(1 + 2 * half),
        [pltpu.VMEM((3, half * block, HEAD_DIM), bf16)],
        flops=2 * 10**9,
    )(where, reach, *inner[0], *cross[0])
    for flip in range(half):
        pairs = [(i, half + (i ^ flip)) for i in range(half)]
        across[flip] = move(lows[flip], "seq", pairs)
    rest = own_kernel(
        functools.partial(attend_rest, half),
        [shape((2 * block + STAT_ROWS, HEAD_DIM), bf16)] * half,
        [SMEM] + in_vmem(3 + 4 * half),
        [
            pltpu.VMEM((6, half * block, HEAD_DIM), bf16),
            pltpu.VMEM((half, block, HEAD_DIM), bf16),
            pltpu.VMEM((half, block, HEAD_DIM), bf16),
            pltpu.VMEM((half, STAT_ROWS, HEAD_DIM), bf16),
        ],
        flops=4 * 10**9,
    )(where, reach, held(o_low), held(stats), *inner[0], *inner[1], *cross[0], *cross[1])
    for flip in range(half):
        own_half[flip] = swap(rest[flip], "seq", flip) if flip else rest[flip]
    came = [held(a) for a in own_half + across]
    width = out_weight.shape[1] // lax.axis_size("head")
    parts = 2
    slab = shape((block, width // parts), bf16)

    def columns_of(flip, part, parts, rows, *other):
        return own_kernel(
            functools.partial(project, flip, part, parts),
            [shape((block, width // parts), bf16)],
            [SMEM] + in_vmem(2 + len(other)),
            flops=10**9 // parts,
        )(where, held(rows), w_held, *[held(a) for a in other])[0]

    first, joined = own_kernel(
        functools.partial(join_and_project, half, 3, 0, parts),
        [slab, shape((block, n_seq * HEAD_DIM), bf16)],
        [SMEM] + in_vmem(2 * half + 1),
        flops=10**9,
    )(where, *came, w_held)
    first = swap(first, "head", 1)
    second = columns_of(3, 1, parts, joined)
    second = swap(second, "head", 1)
    kept = columns_of(2, 0, parts, joined)
    kept = (first.astype(f32) + kept.astype(f32)).astype(bf16)
    far = [kept, columns_of(2, 1, parts, joined, second)]
    rows, _ = lax.optimization_barrier((joined, far[1]))
    for part in range(parts):
        far[part] = swap(far[part], "head", 2)
    near = columns_of(1, 0, 1, rows)
    near = columns_of(0, 0, 1, rows, swap(near, "head", 1))
    return (near.astype(f32) + jnp.concatenate(far, axis=1).astype(f32)).astype(bf16)


def on_device(queries, keys_in, values_in, out_weight, spans, full_ids):
    n_seq, n_head = lax.axis_size("seq"), lax.axis_size("head")
    block = queries.shape[0]
    one_head_each = queries.shape[1] == n_seq * HEAD_DIM
    if one_head_each and n_head == 4 and n_seq == 8 and block == 256:
        return half_path(queries, keys_in, values_in, out_weight, spans, full_ids)
    return ring_path(queries, keys_in, values_in, out_weight, spans, full_ids)


def solution(mesh):
    placed = (
        P("seq", "head"),
        P("seq", "head"),
        P("seq", "head"),
        P("head", None),
        P("head"),
        P("head"),
    )
    return jax.shard_map(
        on_device, mesh=mesh, in_specs=placed, out_specs=P("seq", "head"), check_vma=False
    )
```

```python
import functools
import math

import jax
import jax.numpy as jnp
from jax import lax
from jax.experimental import pallas as pl
from jax.experimental.pallas import tpu as pltpu
from jax.sharding import PartitionSpec as P

HEAD_DIM = 128
SPAN_MAX = 4096
SPAN_MIN = 1024


NEG_FILL = -1e30


def from_behind(block, axis, distance):
    devices = range(lax.axis_size(axis))
    route = [(i - distance, i) for i in devices if i - distance in devices]
    return lax.ppermute(block, axis, route)


def online_update(carry_state, scores, allowed, value_rows):
    old_peak, row_total, numerator = carry_state
    masked = jnp.where(allowed, scores, NEG_FILL)
    new_peak = jnp.maximum(old_peak, jnp.max(masked, axis=-1))
    weights = jnp.where(allowed, jnp.exp(masked - new_peak[..., None]), 0.0)
    rescale = jnp.exp(old_peak - new_peak)
    row_total = row_total * rescale + jnp.sum(weights, axis=-1)
    numerator = numerator * rescale[..., None] + jnp.einsum(
        "hqk,hkd->hqd", weights.astype(jnp.bfloat16), value_rows, preferred_element_type=jnp.float32
    )
    return (new_peak, row_total, numerator)


def empty_state(lead_count, row_count, head_width):
    return (
        jnp.full((lead_count, row_count), NEG_FILL, jnp.float32),
        jnp.zeros((lead_count, row_count), jnp.float32),
        jnp.zeros((lead_count, row_count, head_width), jnp.float32),
    )


def finish(carry_state):
    return (carry_state[2] / carry_state[1][..., None]).astype(jnp.bfloat16)


def ring_path(queries, keys_in, values_in, out_weight, spans, full_ids):
    score_scale = HEAD_DIM ** (-0.5)
    n_seq = lax.axis_size("seq")
    seq_index = lax.axis_index("seq")
    tok_rows = queries.shape[0]
    group_heads = queries.shape[1] // HEAD_DIM
    full_count = full_ids.shape[0]
    band_count = group_heads - full_count
    head_base = lax.axis_index("head") * group_heads
    local_range = jnp.arange(group_heads)
    marks = jnp.sum(
        (local_range[:, None] + head_base == full_ids[None, :]).astype(jnp.int32), axis=1
    )
    order_local = jnp.argsort(marks * group_heads + local_range)
    band_local = order_local[:band_count]
    full_local = order_local[band_count:]
    query_three = queries.reshape(tok_rows, group_heads, HEAD_DIM)
    key_three = keys_in.reshape(tok_rows, group_heads, HEAD_DIM)
    value_three = values_in.reshape(tok_rows, group_heads, HEAD_DIM)
    query_band = jnp.take(query_three, band_local, axis=1).transpose(1, 0, 2)
    kv_band = jnp.stack(
        [
            jnp.take(key_three, band_local, axis=1).transpose(1, 0, 2),
            jnp.take(value_three, band_local, axis=1).transpose(1, 0, 2),
        ]
    )
    band_reach = jnp.take(spans, band_local)
    query_pos = seq_index * tok_rows + jnp.arange(tok_rows)
    hop_count = min(max(1, SPAN_MAX // tok_rows), n_seq - 1)
    arrived = [(kv_band, 0)]
    moving = kv_band
    for distance in range(1, hop_count + 1):
        moving = from_behind(moving, "seq", 1)
        arrived.append((moving, distance))
    batch_size = max(1, 512 // tok_rows)
    band_state = empty_state(band_count, tok_rows, HEAD_DIM)
    for first_piece in range(0, len(arrived), batch_size):
        batch_pieces = arrived[first_piece : first_piece + batch_size]
        key_rows = jnp.concatenate([arrival[0][0] for arrival in batch_pieces], axis=1)
        value_rows = jnp.concatenate([arrival[0][1] for arrival in batch_pieces], axis=1)
        key_pos = jnp.concatenate(
            [(seq_index - arrival[1]) * tok_rows + jnp.arange(tok_rows) for arrival in batch_pieces]
        )
        scores = (
            jnp.einsum("hqd,hkd->hqk", query_band, key_rows, preferred_element_type=jnp.float32)
            * score_scale
        )
        gap_size = query_pos[None, :, None] - key_pos[None, None, :]
        allowed = (
            (gap_size >= 0) & (gap_size < band_reach[:, None, None]) & (key_pos >= 0)[None, None, :]
        )
        band_state = online_update(band_state, scores, allowed, value_rows)
    band_out = finish(band_state)
    query_full = jnp.take(query_three, full_local, axis=1).transpose(1, 0, 2)
    key_full = jnp.take(key_three, full_local, axis=1).transpose(1, 0, 2)
    value_full = jnp.take(value_three, full_local, axis=1).transpose(1, 0, 2)
    kv_full = jnp.stack([key_full, value_full])
    last_query = seq_index * tok_rows + tok_rows - 1
    key_piece = lax.all_gather(kv_full, "seq", axis=2, tiled=True)
    row_count = key_piece.shape[2]
    tile_rows = math.gcd(row_count, 512)

    def absorb_tile(tile_index, inner_state):
        key_tile = lax.dynamic_slice_in_dim(key_piece[0], tile_index * tile_rows, tile_rows, 1)
        value_tile = lax.dynamic_slice_in_dim(key_piece[1], tile_index * tile_rows, tile_rows, 1)
        key_pos = tile_index * tile_rows + jnp.arange(tile_rows)
        scores = (
            jnp.einsum("hqd,hkd->hqk", query_full, key_tile, preferred_element_type=jnp.float32)
            * score_scale
        )
        allowed = key_pos[None, None, :] <= query_pos[None, :, None]
        return online_update(inner_state, scores, allowed, value_tile)

    live_tiles = jnp.clip(last_query // tile_rows + 1, 0, row_count // tile_rows)
    full_state = lax.fori_loop(
        0, live_tiles, absorb_tile, empty_state(full_count, tok_rows, HEAD_DIM)
    )
    full_out = finish(full_state)
    combined = jnp.concatenate([band_out, full_out], axis=0)
    inverse = jnp.argsort(order_local)
    per_head = jnp.take(combined, inverse, axis=0)
    attended = per_head.transpose(1, 0, 2).reshape(tok_rows, group_heads * HEAD_DIM)
    projected = jnp.dot(attended, out_weight, preferred_element_type=jnp.float32)
    return lax.psum_scatter(projected.astype(jnp.bfloat16), "head", scatter_dimension=1, tiled=True)


def move(block, axis, pairs):
    return lax.ppermute(block, axis, pairs)


def swap(block, axis, flip):
    return move(block, axis, [(i, i ^ flip) for i in range(lax.axis_size(axis))])


def in_vmem(count):
    return [pl.BlockSpec(memory_space=pltpu.VMEM)] * count


def held(array):
    return pltpu.with_memory_space_constraint(array, pltpu.VMEM)


SMEM = pl.BlockSpec(memory_space=pltpu.SMEM)
FACTOR = HEAD_DIM**-0.5 * math.log2(math.e)
STAT_ROWS = 16


def own_kernel(body, out_shapes, in_specs, scratch=(), flops=10**8, limit=20 * 2**20):
    return pl.pallas_call(
        body,
        out_shape=out_shapes,
        in_specs=in_specs,
        out_specs=in_vmem(len(out_shapes)),
        scratch_shapes=list(scratch),
        compiler_params=pltpu.CompilerParams(vmem_limit_bytes=limit),
        cost_estimate=pl.CostEstimate(flops=flops, bytes_accessed=10**6, transcendentals=0),
    )


def deal(half, me_ref, spans_ref, full_ref, q_ref, k_ref, v_ref, *refs):
    reach_ref, sems, spans, full_ids = refs[4 * half :]
    me = me_ref[0]
    low = me % half
    tables = [
        pltpu.make_async_copy(spans_ref, spans, sems.at[8 * half]),
        pltpu.make_async_copy(full_ref, full_ids, sems.at[8 * half + 1]),
    ]
    for copy in tables:
        copy.start()
    rows = q_ref.shape[0]
    waits = []

    def fetch(source, head, out_ref, place):
        at = pl.multiple_of(head * HEAD_DIM, HEAD_DIM)
        return pltpu.make_async_copy(
            source.at[:, pl.ds(at, HEAD_DIM)],
            out_ref.at[pl.ds(place * rows, rows)],
            sems.at[len(waits)],
        )

    for upper in range(2):
        inner = refs[2 * upper * half : (2 * upper + 1) * half]
        cross = refs[(2 * upper + 1) * half : (2 * upper + 2) * half]
        for flip in range(half - 1, -1, -1):
            for place, source in enumerate((q_ref, k_ref, v_ref)):
                copy = fetch(source, (low ^ flip) + upper * half, inner[flip], place)
                copy.start()
                waits.append(copy)
        for flip in range(half - 1, -1, -1):
            target = low ^ flip
            if upper:
                copy = fetch(v_ref, target + half, cross[flip], 0)
                copy.start()
            else:
                below = fetch(k_ref, target + half, cross[flip], 0)
                copy = fetch(q_ref, target, cross[flip], 0)
                pl.when(me < half)(below.start)
                pl.when(me >= half)(copy.start)
            waits.append(copy)
    for copy in tables:
        copy.wait()
    for upper in range(2):
        local = low + upper * half
        reach = spans[local]
        for place in range(full_ids.shape[0]):
            is_full = full_ids[place] == me_ref[1] * 2 * half + local
            reach = jnp.where(is_full, 2 * half * rows, reach)
        reach_ref[upper : upper + 1] = jnp.full((1, reach_ref.shape[1]), reach, jnp.int32)
    for copy in waits:
        copy.wait()


def square_eye(size):
    row = lax.broadcasted_iota(jnp.int32, (size, size), 0)
    return row == lax.broadcasted_iota(jnp.int32, (size, size), 1)


def pack_stat(stat):
    eye = square_eye(HEAD_DIM)
    rows = []
    for first in range(0, stat.shape[0], HEAD_DIM):
        piece = jnp.where(eye, stat[first : first + HEAD_DIM], 0.0)
        left = jnp.sum(piece, axis=0, keepdims=True)
        for _ in range(3):
            part = left.astype(jnp.bfloat16).astype(jnp.float32)
            rows.append(part)
            left = left - part
    rows.append(jnp.zeros((STAT_ROWS - len(rows), HEAD_DIM), jnp.float32))
    return jnp.concatenate(rows, axis=0).astype(jnp.bfloat16)


def share_column(here, there, size):
    eye = square_eye(HEAD_DIM)
    apart = there.astype(jnp.float32) - here.astype(jnp.float32)
    columns = []
    for index in range(size // HEAD_DIM):
        row = apart[3 * index : 3 * index + 1]
        for more in (1, 2):
            row = row + apart[3 * index + more : 3 * index + more + 1]
        share = 1.0 / (1.0 + jnp.exp2(row))
        columns.append(jnp.sum(jnp.where(eye, share, 0.0), axis=1, keepdims=True))
    return jnp.concatenate(columns, axis=0)


def softmax_rows(pieces, value_tiles):
    peak = jnp.max(functools.reduce(jnp.maximum, pieces), axis=1, keepdims=True)
    total, numerator = None, None
    for scores, value_tile in zip(pieces, value_tiles):
        weights = jnp.exp2((scores - peak) * FACTOR)
        total = weights if total is None else total + weights
        product = jnp.dot(
            weights.astype(jnp.bfloat16), value_tile, preferred_element_type=jnp.float32
        )
        numerator = product if numerator is None else numerator + product
    return numerator, jnp.sum(total, axis=1, keepdims=True), peak


def score_tile(q_tile, k_tile):
    return lax.dot_general(
        q_tile, k_tile, (((1,), (1,)), ((), ())), preferred_element_type=jnp.float32
    )


def gaps(block):
    row = lax.broadcasted_iota(jnp.int32, (block, block), 0)
    return row - lax.broadcasted_iota(jnp.int32, (block, block), 1)


def gather_rows(half, low, inner, qkv, first):
    block = inner[0].shape[0] // 3
    for flip in range(half):
        at = pl.multiple_of((low ^ flip) * block, block)
        for place in range(3):
            rows = slice(place * block, (place + 1) * block)
            qkv[first + place, pl.ds(at, block)] = inner[flip][rows]


def own_pieces(qkv, first, i, gap):
    block = gap.shape[0]
    q_tile = qkv[first, i * block : (i + 1) * block]
    pieces, value_tiles = [], []
    for j in range(i + 1):
        scores = score_tile(q_tile, qkv[first + 1, j * block : (j + 1) * block])
        pieces.append(jnp.where(gap >= 0, scores, NEG_FILL) if i == j else scores)
        value_tiles.append(qkv[first + 2, j * block : (j + 1) * block])
    return q_tile, pieces, value_tiles


def attend_lower_own(half, qkv, gap, o_low, stats):
    for i in range(half):
        numerator, total, peak = softmax_rows(*own_pieces(qkv, 0, i, gap)[1:])
        o_low[i] = (numerator / total).astype(jnp.bfloat16)
        stats[i] = pack_stat(peak * FACTOR + jnp.log2(total))


def attend_low(half, me_ref, reach_ref, *refs):
    inner, cross, out_refs = refs[:half], refs[half : 2 * half], refs[2 * half : 3 * half]
    o_low, stats, qkv = refs[3 * half :]
    block = cross[0].shape[0]
    low = me_ref[0] % half
    gap = gaps(block)

    @pl.when(me_ref[0] < half)
    def _():
        reach = reach_ref[0:1]
        for flip in range(half - 1, -1, -1):
            pieces = []
            for other in range(half):
                offset = (half + (low ^ flip) - (low ^ other)) * block
                scores = score_tile(cross[flip][...], inner[other][block : 2 * block])
                pieces.append(jnp.where(gap < reach - offset, scores, NEG_FILL))
            value_tiles = [inner[other][2 * block :] for other in range(half)]
            numerator, total, peak = softmax_rows(pieces, value_tiles)
            out_refs[flip][:block] = (numerator / total).astype(jnp.bfloat16)
            out_refs[flip][block:] = pack_stat(peak * FACTOR + jnp.log2(total))

    @pl.when(me_ref[0] >= half)
    def _():
        gather_rows(half, low, inner, qkv, 0)
        attend_lower_own(half, qkv, gap, o_low, stats)


def attend_rest(half, me_ref, reach_ref, low_ref, stat_ref, *refs):
    lower, upper = refs[:half], refs[half : 2 * half]
    cross_k, cross_v = refs[2 * half : 3 * half], refs[3 * half : 4 * half]
    out_refs = refs[4 * half : 5 * half]
    qkv, o_low, o_up, stats = refs[5 * half :]
    me = me_ref[0]
    low = me % half
    block = cross_k[0].shape[0]
    gap = gaps(block)
    gather_rows(half, low, upper, qkv, 3)

    @pl.when(me < half)
    def _():
        gather_rows(half, low, lower, qkv, 0)
        attend_lower_own(half, qkv, gap, o_low, stats)
        for i in range(half):
            numerator, total, _ = softmax_rows(*own_pieces(qkv, 3, i, gap)[1:])
            o_up[i] = (numerator / total).astype(jnp.bfloat16)
        for flip in range(half):
            out_refs[flip][:block] = o_low[low ^ flip]
            out_refs[flip][2 * block :] = stats[low ^ flip]

    @pl.when(me >= half)
    def _():
        reach = reach_ref[1:2]
        for i in range(half):
            q_tile, pieces, value_tiles = own_pieces(qkv, 3, i, gap)
            for other in range(half):
                offset = (half + i - (low ^ other)) * block
                scores = score_tile(q_tile, cross_k[other][...])
                pieces.append(jnp.where(gap < reach - offset, scores, NEG_FILL))
                value_tiles.append(cross_v[other][...])
            numerator, total, _ = softmax_rows(pieces, value_tiles)
            o_up[i] = (numerator / total).astype(jnp.bfloat16)
        for flip in range(half):
            out_refs[flip][:block] = low_ref[low ^ flip]
            out_refs[flip][2 * block :] = stat_ref[low ^ flip]

    for flip in range(half):
        out_refs[flip][block : 2 * block] = o_up[low ^ flip]


def join_heads(half, me_ref, inner, across, joined):
    me = me_ref[0]
    low = me % half
    block = joined.shape[0]

    def place(flip, upper, value):
        at = pl.multiple_of((low ^ flip) * HEAD_DIM + upper * half * HEAD_DIM, HEAD_DIM)
        joined[:, pl.ds(at, HEAD_DIM)] = value

    @pl.when(me < half)
    def _():
        for flip in range(half):
            place(flip, 0, inner[flip][:block])
            place(flip, 1, inner[flip][block : 2 * block])

    @pl.when(me >= half)
    def _():
        merged = []
        for flip in range(half):
            share = share_column(inner[flip][2 * block :], across[flip][block:], block)
            value = inner[flip][:block].astype(jnp.float32) * share
            value = value + across[flip][:block].astype(jnp.float32) * (1.0 - share)
            merged.append(value.astype(jnp.bfloat16))
        for flip in range(half):
            place(flip, 0, merged[flip])
            place(flip, 1, inner[flip][block : 2 * block])


def join_and_project(half, flip, part, parts, me_ref, *refs):
    inner, across, (w_ref, out_ref, joined) = refs[:half], refs[half : 2 * half], refs[2 * half :]
    join_heads(half, me_ref, inner, across, joined)
    project(flip, part, parts, me_ref, joined, w_ref, out_ref)


def project(flip, part, parts, me_ref, joined, w_ref, *refs):
    *other, out_ref = refs
    width = out_ref.shape[1]
    at = pl.multiple_of(((me_ref[1] ^ flip) * parts + part) * width, width)
    product = jnp.dot(
        joined[...], w_ref[:, pl.ds(at, width)], preferred_element_type=jnp.float32
    ).astype(jnp.bfloat16)
    if other:
        total = product.astype(jnp.float32) + other[0][...].astype(jnp.float32)
        product = total.astype(jnp.bfloat16)
    out_ref[...] = product


def half_path(queries, keys_in, values_in, out_weight, spans, full_ids):
    n_seq = lax.axis_size("seq")
    half = n_seq // 2
    bf16, f32 = jnp.bfloat16, jnp.float32
    shape = jax.ShapeDtypeStruct
    where = jnp.stack([lax.axis_index("seq"), lax.axis_index("head")]).astype(jnp.int32)
    block = queries.shape[0]
    down = range(half - 1, -1, -1)
    piece = shape((block, HEAD_DIM), bf16)

    hbm = pl.BlockSpec(memory_space=pltpu.HBM)
    ours = (spans, full_ids, queries, keys_in, values_in)
    ours = [pltpu.with_memory_space_constraint(a, pltpu.HBM) for a in ours]
    dealt = own_kernel(
        functools.partial(deal, half),
        ([shape((3 * block, HEAD_DIM), bf16)] * half + [piece] * half) * 2
        + [shape((8, block), jnp.int32)],
        [SMEM] + [hbm] * 5,
        [
            pltpu.SemaphoreType.DMA((8 * half + 2,)),
            pltpu.SMEM(spans.shape, jnp.int32),
            pltpu.SMEM(full_ids.shape, jnp.int32),
        ],
    )(where, *ours)
    reach = held(dealt[4 * half])
    inner = [list(dealt[:half]), list(dealt[2 * half : 3 * half])]
    cross = [list(dealt[half : 2 * half]), list(dealt[3 * half : 4 * half])]
    for upper in range(2):
        for flip in range(half - 1, 0, -1):
            inner[upper][flip] = swap(inner[upper][flip], "seq", flip)
        for flip in down:
            pairs = [(i, i ^ half ^ flip) for i in range(half if upper else n_seq)]
            cross[upper][flip] = move(cross[upper][flip], "seq", pairs)
    w_held = held(out_weight)
    inner = [[held(a) for a in arrays] for arrays in inner]
    cross = [[held(a) for a in arrays] for arrays in cross]
    across, own_half = [None] * half, [None] * half
    *lows, o_low, stats = own_kernel(
        functools.partial(attend_low, half),
        [shape((block + STAT_ROWS, HEAD_DIM), bf16)] * half
        + [shape((half, block, HEAD_DIM), bf16), shape((half, STAT_ROWS, HEAD_DIM), bf16)],
        [SMEM] + in_vmem(1 + 2 * half),
        [pltpu.VMEM((3, half * block, HEAD_DIM), bf16)],
        flops=2 * 10**9,
    )(where, reach, *inner[0], *cross[0])
    for flip in range(half):
        pairs = [(i, half + (i ^ flip)) for i in range(half)]
        across[flip] = move(lows[flip], "seq", pairs)
    rest = own_kernel(
        functools.partial(attend_rest, half),
        [shape((2 * block + STAT_ROWS, HEAD_DIM), bf16)] * half,
        [SMEM] + in_vmem(3 + 4 * half),
        [
            pltpu.VMEM((6, half * block, HEAD_DIM), bf16),
            pltpu.VMEM((half, block, HEAD_DIM), bf16),
            pltpu.VMEM((half, block, HEAD_DIM), bf16),
            pltpu.VMEM((half, STAT_ROWS, HEAD_DIM), bf16),
        ],
        flops=4 * 10**9,
    )(where, reach, held(o_low), held(stats), *inner[0], *inner[1], *cross[0], *cross[1])
    for flip in range(half):
        own_half[flip] = swap(rest[flip], "seq", flip) if flip else rest[flip]
    came = [held(a) for a in own_half + across]
    width = out_weight.shape[1] // lax.axis_size("head")
    parts = 2
    slab = shape((block, width // parts), bf16)

    def columns_of(flip, part, parts, rows, *other):
        return own_kernel(
            functools.partial(project, flip, part, parts),
            [shape((block, width // parts), bf16)],
            [SMEM] + in_vmem(2 + len(other)),
            flops=10**9 // parts,
        )(where, held(rows), w_held, *[held(a) for a in other])[0]

    first, joined = own_kernel(
        functools.partial(join_and_project, half, 3, 0, parts),
        [slab, shape((block, n_seq * HEAD_DIM), bf16)],
        [SMEM] + in_vmem(2 * half + 1),
        flops=10**9,
    )(where, *came, w_held)
    first = swap(first, "head", 1)
    second = columns_of(3, 1, parts, joined)
    second = swap(second, "head", 1)
    kept = columns_of(2, 0, parts, joined)
    kept = (first.astype(f32) + kept.astype(f32)).astype(bf16)
    far = [kept, columns_of(2, 1, parts, joined, second)]
    rows, _ = lax.optimization_barrier((joined, far[1]))
    for part in range(parts):
        far[part] = swap(far[part], "head", 2)
    near = columns_of(1, 0, 1, rows)
    near = columns_of(0, 0, 1, rows, swap(near, "head", 1))
    return (near.astype(f32) + jnp.concatenate(far, axis=1).astype(f32)).astype(bf16)


def on_device(queries, keys_in, values_in, out_weight, spans, full_ids):
    n_seq, n_head = lax.axis_size("seq"), lax.axis_size("head")
    block = queries.shape[0]
    fits = queries.shape[1] == n_seq * HEAD_DIM and n_seq > 2 and n_seq & (n_seq - 1) == 0
    fits = fits and block % HEAD_DIM == 0 and n_seq // 2 * block <= SPAN_MIN
    fits = fits and 3 * block <= STAT_ROWS * HEAD_DIM and n_head == 4
    if fits:
        return half_path(queries, keys_in, values_in, out_weight, spans, full_ids)
    return ring_path(queries, keys_in, values_in, out_weight, spans, full_ids)


def solution(mesh):
    placed = (
        P("seq", "head"),
        P("seq", "head"),
        P("seq", "head"),
        P("head", None),
        P("head"),
        P("head"),
    )
    return jax.shard_map(
        on_device, mesh=mesh, in_specs=placed, out_specs=P("seq", "head"), check_vma=False
    )
```
